32 devices in a mesh: col: 8 (over y, x, core), row: 4 (over z).
Axes of the slice: x: 2, y: 2, z: 4, core: 2. Of those that a mesh axis runs over, the one named last changes fastest.
Arguments:
- trace_start: float32 [32, 32768], P(None, ('col', 'row')), may hold values from -6 to 6
- surface_load: float32 [32, 32768], P(None, ('col', 'row')), may hold values from -6 to 6
- panel_tiles: bfloat16 [704, 512, 512], P(('col', 'row')), may hold values from -0.03125 to 0.03125
- tile_list: int32 [704], P(('col', 'row')), may hold values from -1 to 4095, as said below
- surf_map: int32 [8], replicated, may hold values from 0 to 7, as said below
- coef_index: int32 [2, 4, 16384], P(None, None, 'row'), may hold values from 0 to 15
- coef_table: float32 [16], replicated, may hold values from 0.2 to 2
- vol_source: float32 [2, 4, 16384], P(None, None, 'row'), may hold values from -6 to 6
Outputs:
- traces: float32 [32, 32768], P(None, ('col', 'row'))
- response: float32 [32, 32768], P(None, ('col', 'row'))
The draws below stay inside these ranges and needn't reach their ends.
Inputs may be any that keep to these rules, and one draw needn't show every extreme that they name: `tile_list`: each device has 22 slots, ordered by col index, then row index, then slot. A value i * 64 + j names the tile of rows i * 512 to (i + 1) * 512 - 1 and columns j * 512 to (j + 1) * 512 - 1 of the boundary matrix, with j <= i and j < 8; each such tile is named exactly once. A device of col index c and row index r names only tiles whose rows lie in shards of row index r (i * 512 // 1024 leaves remainder r modulo 4), and none if c >= 6; its named tiles fill its first slots and the rest hold -1. Some device names 22 tiles. surf_map[r * 2 + q] leaves remainder r modulo 4; each volume tile lies under exactly one surface tile.
All inputs are finite; a program needn't handle non-finite values.
Results may differ from the reference program's by a relative error of at most 0.0041.
Values may be sent and summed in bfloat16 or wider, within the bound.
A program may use at most 128 MiB of HBM per device.

```python
import math
import jax
import jax.numpy as jnp
import numpy as np
from jax import lax

RHS = 32
NODES = 4096
TILE = 512
LAYERS = 4
ITERS = 2
SWEEPS = 4
COEFS = 16
VOL_COLS = 2
DENSE_COLS = 6
SURFACE = 32768
SHARD = 1024
WIN_TILES = 8
SIDE = 64
SLOTS_DEV = 22
SLOTS = 704
SURF_TILES = 8
LINE = 16384
N_COL = 8
N_ROW = 4


def draw_tile_list(key, part):
    per_shard = SHARD // TILE
    slot_table = jnp.full((N_COL, N_ROW, SLOTS_DEV), -1, jnp.int32)
    for row_block in range(N_ROW):
        tile_names = []
        for tile_row in range(SIDE):
            if tile_row // per_shard % N_ROW == row_block:
                for tile_col in range(min(tile_row + 1, WIN_TILES)):
                    tile_names.append(tile_row * SIDE + tile_col)
        name_table = jnp.asarray(np.array(tile_names, dtype=np.int32))
        name_count = len(tile_names)
        key_order = jax.random.fold_in(key, 2 * row_block + 11)
        key_columns = jax.random.fold_in(key, 2 * row_block + 12)
        tile_order = jax.random.permutation(key_order, name_count)
        column_order = jax.random.permutation(key_columns, DENSE_COLS)
        placing = np.arange(name_count)
        slot_table = slot_table.at[column_order[placing % DENSE_COLS], row_block, placing // DENSE_COLS].set(name_table[tile_order])
    return slot_table.reshape(-1)


def draw_surf_map(key, part):
    pieces = []
    for row_block in range(N_ROW):
        order = jax.random.permutation(jax.random.fold_in(key, 101 + row_block), VOL_COLS).astype(jnp.int32)
        pieces.append(order * N_ROW + row_block)
    return jnp.concatenate(pieces)


def plant(values, rng, smallest, largest):
    spot = [jax.random.randint(jax.random.fold_in(rng, axis), (), 0, length) for axis, length in enumerate(values.shape)]
    longest = values.shape.index(max(values.shape))
    neighbour = spot[:longest] + [(spot[longest] + 1) % values.shape[longest]] + spot[longest + 1:]
    return values.at[tuple(spot)].set(smallest).at[tuple(neighbour)].set(largest)


def level_of(own_key, extent, split, low, high):
    def one(dim, parts):
        steps = jax.random.uniform(jax.random.fold_in(jax.random.fold_in(own_key, 6), dim), (parts,), jnp.float32, low / len(split), high / len(split))
        return jnp.repeat(jnp.exp(steps), extent[dim] // parts).reshape((-1,) + (1,) * (len(extent) - dim - 1))

    gain = one(*split[0])
    for cut in split[1:]:
        gain = gain * one(*cut)
    return gain


def scatter_about(own_key, extent, scale, bound, shards=(), held_as=jnp.bfloat16):
    factor_of = level_of(own_key, extent, shards, -0.22, 0.18) if shards else 1.0
    values = jax.random.normal(own_key, extent, jnp.float32) * scale * factor_of
    return jnp.minimum(jnp.maximum(values, -bound), bound).astype(held_as)


def setup_inputs(seed: int = 0) -> dict:
    key_list = jax.random.split(jax.random.key(seed), 9)
    trace_start = scatter_about(key_list[0], (RHS, SURFACE), 1.0, 6.0, ((1, 32),), jnp.float32)
    surface_load = scatter_about(key_list[1], (RHS, SURFACE), 1.0, 6.0, ((1, 32),), jnp.float32)
    panel_tiles = scatter_about(key_list[2], (SLOTS, TILE, TILE), SURFACE ** -0.5, 0.03125, ((0, 32),))
    tile_list = draw_tile_list(jax.random.fold_in(key_list[8], 71), 0)
    surf_map = draw_surf_map(jax.random.fold_in(key_list[8], 71), 0)
    coef_index = plant(jax.random.randint(key_list[5], (VOL_COLS, LAYERS, LINE), 0, COEFS), jax.random.fold_in(key_list[5], 1), 0, COEFS - 1).astype(jnp.int32)
    coef_table = jnp.clip(jnp.exp(jax.random.uniform(key_list[6], (COEFS,), jnp.float32, math.log(0.2), math.log(2.0))), 0.2, 2.0)
    vol_source = scatter_about(key_list[7], (VOL_COLS, LAYERS, LINE), 1.0, 6.0, ((2, 4),), jnp.float32)
    return {"trace_start": trace_start, "surface_load": surface_load, "panel_tiles": panel_tiles, "tile_list": tile_list, "surf_map": surf_map, "coef_index": coef_index, "coef_table": coef_table, "vol_source": vol_source}


COUPLING_STEP = 0.3
JACOBI_WEIGHT = 0.8
CELL_MASS = 0.05


def lookup_coefs(indices, coef_values):
    levels = jnp.arange(coef_values.shape[0], dtype=jnp.int32)
    return jnp.sum(jnp.where(indices[..., None] == levels, coef_values, 0.0), axis=-1)


def relax_line(padded_values, coefs_pad, source, top_trace):
    centre_coef = coefs_pad[:, 1:-1]
    left_weight = 0.5 * (centre_coef + coefs_pad[:, :-2])
    right_weight = 0.5 * (centre_coef + coefs_pad[:, 2:])
    layer_weight = 0.5 * (centre_coef[:-1] + centre_coef[1:])
    upper_weight = jnp.concatenate([centre_coef[:1], layer_weight], 0)
    lower_weight = jnp.concatenate([layer_weight, jnp.zeros_like(centre_coef[:1])], 0)
    centre = padded_values[:, :, 1:-1]
    upper_values = jnp.concatenate([top_trace[:, None, :], centre[:, :-1]], 1)
    lower_values = jnp.concatenate([centre[:, 1:], jnp.zeros_like(centre[:, :1])], 1)
    gathered = (left_weight * padded_values[:, :, :-2] + right_weight * padded_values[:, :, 2:]
                + upper_weight * upper_values + lower_weight * lower_values + source)
    diagonal = left_weight + right_weight + upper_weight + lower_weight + CELL_MASS
    return (1.0 - JACOBI_WEIGHT) * centre + JACOBI_WEIGHT * gathered / diagonal


def add_block(partial_value, block_sum, block_start):
    current = lax.dynamic_slice_in_dim(partial_value, block_start, TILE, 1)
    return lax.dynamic_update_slice_in_dim(partial_value, current + block_sum, block_start, 1)


def to_bands(values):
    return values.reshape(RHS, N_COL, N_ROW, SHARD).transpose(0, 2, 1, 3).reshape(RHS, SURFACE)


def from_bands(values):
    return values.reshape(RHS, N_ROW, N_COL, SHARD).transpose(0, 2, 1, 3).reshape(RHS, SURFACE)


def panel_product(whole_traces, panel_tiles, tile_list):
    def advance(partial_value, item):
        panel_block, tile_ident = item

        def accumulate(current):
            row_start = ((tile_ident // SIDE) * TILE).astype(jnp.int32)
            col_start = ((tile_ident % SIDE) * TILE).astype(jnp.int32)
            row_part = lax.dynamic_slice_in_dim(whole_traces, row_start, TILE, 1)
            col_part = lax.dynamic_slice_in_dim(whole_traces, col_start, TILE, 1)
            into_rows = lax.dot_general(col_part, panel_block, (((1,), (1,)), ((), ())),
                                        preferred_element_type=jnp.float32)
            into_cols = jnp.dot(row_part, panel_block, preferred_element_type=jnp.float32)
            current = add_block(current, into_rows, row_start)
            return add_block(current, into_cols, col_start)

        partial_value = lax.cond(tile_ident >= 0, accumulate, lambda current: current, partial_value)
        return partial_value, None

    start_sum = jnp.zeros((RHS, SURFACE), jnp.float32)
    result, _ = lax.scan(advance, start_sum, (panel_tiles, tile_list))
    return result


def reference(trace_start, surface_load, panel_tiles, tile_list, surf_map, coef_index, coef_table, vol_source):
    coef_lines = lookup_coefs(coef_index, coef_table)
    coef_padded = jnp.pad(coef_lines, ((0, 0), (0, 0), (1, 1)))
    inverse_map = jnp.zeros((SURF_TILES,), jnp.int32).at[surf_map].set(jnp.arange(SURF_TILES, dtype=jnp.int32))
    volume_states = [jnp.zeros((RHS, LAYERS, LINE), jnp.float32) for line_index in range(VOL_COLS)]
    traces = trace_start
    response = trace_start
    for iteration in range(ITERS):
        whole_traces = traces.astype(jnp.bfloat16)
        products = panel_product(whole_traces, panel_tiles, tile_list)
        surface_tiles = to_bands(whole_traces.astype(jnp.float32)).reshape(RHS, SURF_TILES, NODES)
        line_traces = surface_tiles[:, inverse_map].reshape(RHS, VOL_COLS, LINE)
        fluxes = []
        for line_index in range(VOL_COLS):
            top_trace = line_traces[:, line_index]
            volume_state = volume_states[line_index]
            for sweep_index in range(SWEEPS):
                padded_state = jnp.pad(volume_state, ((0, 0), (0, 0), (1, 1)))
                volume_state = relax_line(padded_state, coef_padded[line_index], vol_source[line_index], top_trace)
            volume_states[line_index] = volume_state
            fluxes.append(coef_lines[line_index, 0] * (top_trace - volume_state[:, 0]))
        flux_lines = jnp.stack(fluxes, 1).reshape(RHS, SURF_TILES, NODES)
        flux_surface = from_bands(flux_lines[:, surf_map].reshape(RHS, SURFACE))
        response = products + flux_surface
        traces = traces + COUPLING_STEP * (surface_load - traces - response)
    return traces, response
```

```python
import functools

import jax
import jax.numpy as jnp
from jax import lax
from jax.experimental import pallas as pl
from jax.experimental.pallas import tpu as pltpu
from jax.sharding import PartitionSpec as P

ITERS = 2
SWEEPS = 4

COUPLING_STEP = 0.3
JACOBI_WEIGHT = 0.8
CELL_MASS = 0.05

LANES = 128
SUB = 8
CORES = 2
F32 = jnp.float32
BF16 = jnp.bfloat16
I32 = jnp.int32


def quotient(x, n):
    return x >> (n.bit_length() - 1) if n & (n - 1) == 0 else lax.div(x, n)


def remainder(x, n):
    return x & (n - 1) if n & (n - 1) == 0 else lax.rem(x, n)


def kernel(
    cfg,
    list_ref,
    surf_ref,
    table_ref,
    start_hbm,
    load_hbm,
    index_hbm,
    source_hbm,
    panel_hbm,
    traces_ref,
    response_ref,
    panel,
    load_ref,
    index_ref,
    source_ref,
    tab,
    order,
    band0,
    band1,
    window0,
    window1,
    edge_left,
    edge_right,
    halo_index,
    halo_source,
    product,
    mix_out,
    mix_in,
    zone_own,
    zone_out,
    zone_in,
    total_out,
    total_in,
    pair_out,
    pair_in,
    row_own,
    row_out,
    row_in,
    index_ext,
    coef_ext,
    source_ext,
    weights,
    state,
    top,
    flux,
    panel_sem,
    input_sem,
    tab_sem,
    band_send,
    pass_send,
    band_recv,
    win_send,
    win_pass,
    win_recv,
    edge_send,
    edge_recv,
    halo_send,
    halo_recv,
    mix_send,
    mix_recv,
    zone_send,
    zone_recv,
    total_send,
    total_recv,
    pair_send,
    pair_recv,
    row_send,
    row_recv,
):
    cols, rows, lines, per_shard, tile, slots, nodes, layers, rhs, levels = cfg
    dense = cols - lines
    group = cols // lines
    shard = per_shard * tile
    half = per_shard // CORES
    chips = cols // CORES
    dense_chips = dense // CORES
    win_tiles = rows * per_shard
    band_tiles = cols * per_shard
    side = cols * rows * per_shard
    span = shard + 2 * LANES
    bands = (band0, band1)
    windows = (window0, window1)
    c = lax.axis_index("col")
    r = lax.axis_index("row")
    core = lax.rem(c, CORES)
    chip = lax.div(c, CORES)
    other = 1 - core
    partner = chip * CORES + other
    q = lax.div(c, group)
    m = lax.rem(c, group)
    is_dense = c < dense
    row_up = jnp.minimum(r + 1, rows - 1)
    row_down = jnp.maximum(r - 1, 0)
    first_of_tile = m == 0
    last_of_tile = m == group - 1
    cross_left = first_of_tile & (r > 0)
    cross_right = last_of_tile & (r < rows - 1)

    def copy(src, dst, send, recv, to_col, to_row):
        return pltpu.make_async_remote_copy(
            src_ref=src,
            dst_ref=dst,
            send_sem=send,
            recv_sem=recv,
            device_id=(to_col, to_row),
            device_id_type=pl.DeviceIdType.MESH,
        )

    def panel_copy(s):
        return pltpu.make_async_copy(panel_hbm.at[s], panel.at[s], panel_sem.at[s])

    inputs = (
        (start_hbm, traces_ref),
        (index_hbm, index_ref),
        (source_hbm, source_ref),
        (load_hbm, load_ref),
    )

    def input_copy(i):
        return pltpu.make_async_copy(inputs[i][0], inputs[i][1], input_sem.at[i])

    for i in range(len(inputs)):
        input_copy(i).start()

    barrier = pltpu.get_barrier_semaphore()

    def greet(to_col, to_row):
        pl.semaphore_signal(
            barrier, inc=1, device_id=(to_col, to_row), device_id_type=pl.DeviceIdType.MESH
        )

    for k in range(1, rows):
        greet(c, lax.rem(r + k, rows))
    for k in range(1, cols):
        greet(lax.rem(c + k, cols), r)

    @pl.when(cross_right)
    def _():
        for z in range(lines):
            greet(z * group, row_up)

    @pl.when(cross_left)
    def _():
        for z in range(lines):
            greet(z * group + group - 1, row_down)

    @pl.when(is_dense)
    def _():
        def start(s, _):
            panel_copy(s).start()
            return 0

        lax.fori_loop(0, slots, start, 0)


    padded_slots = -(-slots // SUB) * SUB
    lane = lax.broadcasted_iota(I32, (SUB, LANES), 1)

    def sort_slots():
        slot = lax.broadcasted_iota(I32, (padded_slots, LANES), 0)
        lanes = lax.broadcasted_iota(I32, (padded_slots, LANES), 1)
        row_key = jnp.full((padded_slots, LANES), band_tiles, I32)
        col_key = jnp.full((padded_slots, LANES), win_tiles, I32)
        keys = []
        for s in range(slots):
            name = list_ref[s]
            safe = jnp.maximum(name, 0)
            row = quotient(safe, side)
            row = quotient(quotient(row, per_shard), rows) * per_shard + remainder(row, per_shard)
            row = jnp.where(name >= 0, row, band_tiles)
            col = jnp.where(name >= 0, remainder(safe, side), win_tiles)
            keys.append((col, row))
            row_key = jnp.where(slot == s, row, row_key)
            col_key = jnp.where(slot == s, col, col_key)

        def fold(x):
            x = functools.reduce(jnp.add, [x[i : i + SUB] for i in range(0, padded_slots, SUB)])
            for shift in (4, 2, 1):
                x = x + pltpu.roll(x, shift, 0)
            return x

        for which, key, source, count in (
            (0, col_key, row_key, win_tiles),
            (1, row_key, col_key, band_tiles),
        ):
            rank = jnp.zeros((padded_slots, LANES), I32)
            upto = jnp.zeros((SUB, LANES), I32)
            equal = jnp.zeros((SUB, LANES), I32)
            for s in range(slots):
                value = keys[s][which]
                ahead = (key > value) | ((key == value) & (slot > s))
                rank = rank + jnp.where(ahead, 1, 0)
                upto = upto + jnp.where(lane >= value, 1, 0)
                equal = equal + jnp.where(lane == value, 1, 0)
            rank = jnp.where(slot < slots, rank, LANES)
            here = rank == lanes
            place = fold(jnp.where(here, slot, 0))
            origin = fold(jnp.where(here, jnp.where(key < count, source, 0), 0))
            value = fold(jnp.where(here, key, 0))
            keep = (value == pltpu.roll(value, 1, 1)) & (lane > 0)
            last = jnp.where(equal > 0, upto - 1, slots)
            for i, x in enumerate((place, origin, jnp.where(keep, 1, 0), last)):
                tab[4 * which + i : 4 * which + i + 1, :] = x[0:1, :]

    @pl.when(is_dense)
    def _():
        sort_slots()
        pltpu.make_async_copy(tab, order, tab_sem).start()
        product[slots] = jnp.zeros((rhs, tile), F32)

    input_copy(0).wait()
    input_copy(1).wait()
    input_copy(2).wait()

    expected = (
        cols - 1 + rows - 1 + jnp.where(cross_right, lines, 0) + jnp.where(cross_left, lines, 0)
    )
    pl.semaphore_wait(barrier, expected)


    def halo_copy(kind, side_of, arrival=False):
        ref = (index_ref, source_ref)[kind]
        dst = (halo_index, halo_source)[kind]
        at = nodes - LANES if side_of == 0 else 0
        to = row_up if (side_of == 0) != arrival else row_down
        return copy(
            ref.at[:, :, pl.ds(at, LANES)],
            dst.at[side_of],
            halo_send.at[kind, side_of],
            halo_recv.at[kind, side_of],
            c,
            to,
        )

    halo_sends = (first_of_tile & (r < rows - 1), last_of_tile & (r > 0))
    halo_receives = (cross_left, cross_right)


    def edge_source(it, side_of):
        if side_of == 0:
            return bands[it].at[c * per_shard + per_shard - 1, :, pl.ds(tile - LANES, LANES)]
        return bands[it].at[c * per_shard, :, pl.ds(0, LANES)]

    def edge_near(it, side_of, arrival=False):
        dst = (edge_left, edge_right)[side_of]
        to = c + 1 if (side_of == 0) != arrival else c - 1
        return copy(
            edge_source(it, side_of),
            dst.at[it, lines],
            edge_send.at[it, side_of, lines],
            edge_recv.at[it, side_of, lines],
            to,
            r,
        )

    def edge_far(it, side_of, z):
        dst = (edge_left, edge_right)[side_of]
        to = (z * group, row_up) if side_of == 0 else (z * group + group - 1, row_down)
        return copy(
            edge_source(it, side_of),
            dst.at[it, q],
            edge_send.at[it, side_of, z],
            edge_recv.at[it, side_of, q],
            *to,
        )

    def edge_far_arrival(it, side_of, z):
        dst = (edge_left, edge_right)[side_of]
        at = (z * group + group - 1, row_down) if side_of == 0 else (z * group, row_up)
        return copy(
            edge_source(it, side_of),
            dst.at[it, z],
            edge_send.at[it, side_of, z],
            edge_recv.at[it, side_of, z],
            *at,
        )


    def shard_of(ref, col):
        return ref.at[pl.ds(col * per_shard, per_shard)]

    def peer_chip(k):
        return lax.rem(chip + k, chips)

    def band_copy(it, k, arrival=False):
        peer = peer_chip(k) * CORES + core
        at = peer if arrival else c
        return copy(
            shard_of(bands[it], at),
            shard_of(bands[it], at),
            band_send.at[it, k],
            band_recv.at[it, at],
            peer,
            r,
        )

    def band_pass(it, k, arrival=False):
        at = peer_chip(k) * CORES + (other if arrival else core)
        return copy(
            shard_of(bands[it], at),
            shard_of(bands[it], at),
            pass_send.at[it, k],
            band_recv.at[it, at],
            partner,
            r,
        )

    def window_copy(it, k, arrival=False):
        peer = lax.rem(r + k, rows)
        at = peer if arrival else r
        return copy(
            shard_of(bands[it], 0),
            shard_of(windows[it], at),
            win_send.at[it, k],
            win_recv.at[it, at],
            c,
            peer,
        )

    def window_pass(it, k):
        at = lax.rem(r + k, rows)
        return copy(
            shard_of(windows[it], at),
            shard_of(windows[it], at),
            win_pass.at[it, k],
            win_recv.at[it, at],
            partner,
            r,
        )


    def mix_copy(it):
        return copy(
            mix_out.at[it], mix_in.at[it], mix_send.at[it], mix_recv.at[it], partner, r
        )

    def zone_copy(it, k, arrival=False):
        peer = lax.rem(r + k, rows)
        return copy(
            zone_out.at[it, peer],
            zone_in.at[it, peer if arrival else r],
            zone_send.at[it, k],
            zone_recv.at[it, peer if arrival else r],
            c,
            peer,
        )

    def total_copy(it, col, to):
        return copy(
            total_out.at[it], total_in.at[it, col], total_send.at[it], total_recv.at[it, col], to, r
        )


    def pair_copy(it, k):
        return copy(
            pair_out.at[it, k],
            pair_in.at[it, k],
            pair_send.at[it, k],
            pair_recv.at[it, k],
            partner,
            r,
        )

    def row_copy(it, k):
        peer = peer_chip(k)
        return copy(
            row_out.at[it, peer],
            row_in.at[it, chip],
            row_send.at[it, k],
            row_recv.at[it, chip],
            peer * CORES + core,
            r,
        )

    def row_arrival(it, src):
        return copy(
            row_out.at[it, src],
            row_in.at[it, src],
            row_send.at[it, 0],
            row_recv.at[it, src],
            src * CORES + core,
            r,
        )

    def prepare_volume():
        line = lax.div(surf_ref[r * lines + q], rows)
        for side_of, edge_of_tile in ((0, first_of_tile), (1, last_of_tile)):
            to = pl.ds(0 if side_of == 0 else LANES + shard, LANES)
            at = m * shard - LANES if side_of == 0 else m * shard + shard
            at = pl.multiple_of(jnp.clip(at, 0, nodes - LANES), LANES)
            receives = halo_receives[side_of]

            @pl.when(jnp.logical_not(edge_of_tile))
            def _():
                index_ext[:, to] = index_ref[line, :, pl.ds(at, LANES)]
                source_ext[:, to] = source_ref[line, :, pl.ds(at, LANES)]

            @pl.when(receives)
            def _():
                for kind in range(2):
                    halo_copy(kind, side_of, True).wait_recv()
                index_ext[:, to] = halo_index[side_of, line]
                source_ext[:, to] = halo_source[side_of, line]

            @pl.when(edge_of_tile & jnp.logical_not(receives))
            def _():
                index_ext[:, to] = jnp.full((layers, LANES), levels, I32)
                source_ext[:, to] = jnp.zeros((layers, LANES), F32)

        at = pl.multiple_of(m * shard, LANES)
        index_ext[:, LANES : LANES + shard] = index_ref[line, :, pl.ds(at, shard)]
        source_ext[:, LANES : LANES + shard] = source_ref[line, :, pl.ds(at, shard)]
        indices = index_ext[...]
        coefs = jnp.zeros((layers, span), F32)
        for level in range(levels):
            coefs = jnp.where(indices == level, table_ref[level], coefs)
        coef_ext[...] = coefs
        inside = index_ext[0:1, :] < levels
        for layer in range(layers):
            k = coef_ext[layer : layer + 1, :]
            left = 0.5 * (k + pltpu.roll(k, 1, 1))
            right = 0.5 * (k + pltpu.roll(k, span - 1, 1))
            up = 0.5 * (k + coef_ext[layer - 1 : layer, :]) if layer else k
            diagonal = left + right + up + CELL_MASS
            parts = [left, right, up]
            if layer < layers - 1:
                down = 0.5 * (k + coef_ext[layer + 1 : layer + 2, :])
                diagonal = diagonal + down
                parts.append(down)
            else:
                parts.append(None)
            parts.append(source_ext[layer : layer + 1, :])
            scale = jnp.where(inside, JACOBI_WEIGHT / diagonal, 0.0)
            for kind, part in enumerate(parts):
                if part is not None:
                    weights[kind, layer] = jnp.broadcast_to(part * scale, (SUB, span))

    def relax(now, g, first):
        at = pl.ds(g * SUB, SUB)
        for layer in range(layers):
            value = weights[4, layer]
            if first:
                if layer == 0:
                    value = value + weights[2, layer] * top[at, :]
            else:
                centre = state[now, layer, at, :]
                value = value + (1.0 - JACOBI_WEIGHT) * centre
                value = value + weights[0, layer] * pltpu.roll(centre, 1, 1)
                value = value + weights[1, layer] * pltpu.roll(centre, span - 1, 1)
                above = state[now, layer - 1, at, :] if layer else top[at, :]
                value = value + weights[2, layer] * above
                if layer < layers - 1:
                    value = value + weights[3, layer] * state[now, layer + 1, at, :]
            state[1 - now, layer, at, :] = value

    def volume(it):
        line = lax.div(surf_ref[r * lines + q], rows)
        for side_of, edge_of_tile in ((0, first_of_tile), (1, last_of_tile)):
            dst = (edge_left, edge_right)[side_of]
            to = slice(0, LANES) if side_of == 0 else slice(LANES + shard, span)
            base = row_down if side_of == 0 else row_up
            place = 0
            for z in range(lines):
                place = jnp.where(surf_ref[base * lines + z] == line * rows + base, z, place)
            receives = halo_receives[side_of]

            @pl.when(jnp.logical_not(edge_of_tile))
            def _():
                edge_near(it, side_of, True).wait_recv()
                top[:, to] = dst[it, lines].astype(F32)

            @pl.when(receives)
            def _():
                for z in range(lines):
                    edge_far_arrival(it, side_of, z).wait_recv()
                value = dst[it, 0]
                for z in range(1, lines):
                    value = jnp.where(place == z, dst[it, z], value)
                top[:, to] = value.astype(F32)

            @pl.when(edge_of_tile & jnp.logical_not(receives))
            def _():
                top[:, to] = jnp.zeros((rhs, LANES), F32)

        def rows_of(g, _):
            for i in range(SWEEPS):
                relax(i % 2, g, it == 0 and i == 0)
            at = pl.ds(g * SUB, SUB)
            k = jnp.broadcast_to(coef_ext[0:1, LANES : LANES + shard], (SUB, shard))
            flux[at, :] = k * (
                top[at, LANES : LANES + shard]
                - state[SWEEPS % 2, 0, at, LANES : LANES + shard]
            )
            return 0

        lax.fori_loop(0, rhs // SUB, rows_of, 0)

    def segments(which, traces_of, contract):
        def step(k, acc):
            s = order[4 * which, k]
            keep = order[4 * which + 2, k].astype(F32)
            acc = acc * keep + lax.dot_general(
                traces_of[order[4 * which + 1, k]],
                panel[s],
                (((1,), (contract,)), ((), ())),
                preferred_element_type=F32,
            )
            product[k] = acc
            return acc

        acc = jnp.zeros((rhs, tile), F32)
        for k in range(slots):
            acc = step(k, acc)

    def last_of(which, at):
        return product[order[4 * which + 3, at]]

    def dense_part(it):
        @pl.when(is_dense & (core == 0) & (c == 0))
        def _():
            for k in range(1, rows):
                window_copy(it, k).start()

        for k in range(1, chips):
            band_copy(it, k, True).wait_recv()
            band_pass(it, k).start()

            @pl.when((core == 0) & (peer_chip(k) == 0))
            def _():
                for j in range(1, rows):
                    window_copy(it, j).start()

        for k in range(chips):
            band_pass(it, k, True).wait_recv()
        windows[it][pl.ds(r * per_shard, per_shard)] = bands[it][0:per_shard]
        if it == 0:
            pltpu.make_async_copy(tab, order, tab_sem).wait()

            def landed(s, _):
                panel_copy(s).wait()
                return 0

            lax.fori_loop(0, slots, landed, 0)

        segments(0, bands[it], 0)
        for z in range(rows):
            for p in range(half):
                value = last_of(0, z * per_shard + other * half + p)
                mix_out[it, z, p] = value.astype(BF16)
        mix_copy(it).start()

        @pl.when(core == 0)
        def _():
            for k in range(1, rows):
                window_copy(it, k, True).wait_recv()
                window_pass(it, k).start()

        mix_copy(it).wait_recv()
        for z in range(rows):
            for p in range(half):
                value = last_of(0, z * per_shard + core * half + p) + mix_in[it, z, p].astype(F32)
                zone_out[it, z, p] = value.astype(BF16)
        for p in range(half):
            zone_own[p] = last_of(0, r * per_shard + core * half + p) + mix_in[it, r, p].astype(F32)
        for k in range(1, rows):
            zone_copy(it, k).start()

        @pl.when(core == 1)
        def _():
            for k in range(1, rows):
                window_copy(it, k, True).wait_recv()

        segments(1, windows[it], 1)
        for k in range(chips):
            for p in range(per_shard):
                value = last_of(1, (k * CORES + other) * per_shard + p)
                pair_out[it, k, p] = value.astype(BF16)
            pair_copy(it, k).start()
        for k in range(chips):
            pair_copy(it, k).wait_recv()
        for k in range(1, chips):
            peer = peer_chip(k)
            for p in range(per_shard):
                value = last_of(1, (peer * CORES + core) * per_shard + p)
                value = value + pair_in[it, peer, p].astype(F32)
                row_out[it, peer, p] = value.astype(BF16)
            row_copy(it, k).start()
        for p in range(per_shard):
            row_own[p] = last_of(1, c * per_shard + p) + pair_in[it, chip, p].astype(F32)
        for k in range(1, rows):
            zone_copy(it, k, True).wait_recv()
        for p in range(half):
            value = zone_own[p]
            for k in range(1, rows):
                value = value + zone_in[it, lax.rem(r + k, rows), p].astype(F32)
            zone_own[p] = value
            total_out[it, p] = value.astype(BF16)

        @pl.when(c != 0)
        def _():
            total_copy(it, c, 0).start()

    for it in range(ITERS):
        for p in range(per_shard):
            rounded = traces_ref[:, p * tile : (p + 1) * tile].astype(BF16)
            bands[it][c * per_shard + p] = rounded
            top[:, LANES + p * tile : LANES + (p + 1) * tile] = rounded.astype(F32)

        @pl.when(jnp.logical_not(last_of_tile))
        def _():
            edge_near(it, 0).start()

        @pl.when(jnp.logical_not(first_of_tile))
        def _():
            edge_near(it, 1).start()

        @pl.when(cross_right)
        def _():
            for z in range(lines):
                edge_far(it, 0, z).start()

        @pl.when(cross_left)
        def _():
            for z in range(lines):
                edge_far(it, 1, z).start()

        if it == 0:
            for side_of in range(2):

                @pl.when(halo_sends[side_of])
                def _():
                    for kind in range(2):
                        halo_copy(kind, side_of).start()

        for k in range(1, chips):

            @pl.when(peer_chip(k) < dense_chips)
            def _():
                band_copy(it, k).start()

        @pl.when(is_dense)
        def _():
            band_pass(it, 0).start()

        if it == 0:
            prepare_volume()
        volume(it)

        @pl.when(is_dense)
        def _():
            dense_part(it)

        if it == 0:
            input_copy(3).wait()

        response_ref[...] = flux[...]
        for src in range(dense_chips):

            @pl.when(src != chip)
            def _():
                row_arrival(it, src).wait_recv()
                for p in range(per_shard):
                    at = slice(p * tile, (p + 1) * tile)
                    response_ref[:, at] += row_in[it, src, p].astype(F32)

        @pl.when(is_dense)
        def _():
            for p in range(per_shard):
                at = slice(p * tile, (p + 1) * tile)
                response_ref[:, at] += row_own[p]

        @pl.when(c == 0)
        def _():
            for p in range(half):
                at = slice(p * tile, (p + 1) * tile)
                response_ref[:, at] += zone_own[p]
            for src in range(1, dense):
                total_copy(it, src, src).wait_recv()
                for p in range(half):
                    at = (src % CORES) * half + p
                    at = slice(at * tile, (at + 1) * tile)
                    response_ref[:, at] += total_in[it, src, p].astype(F32)

        t = traces_ref[...]
        traces_ref[...] = t + COUPLING_STEP * (load_ref[...] - t - response_ref[...])

    for it in range(ITERS):

        @pl.when(jnp.logical_not(last_of_tile))
        def _():
            edge_near(it, 0).wait_send()

        @pl.when(jnp.logical_not(first_of_tile))
        def _():
            edge_near(it, 1).wait_send()

        @pl.when(cross_right)
        def _():
            for z in range(lines):
                edge_far(it, 0, z).wait_send()

        @pl.when(cross_left)
        def _():
            for z in range(lines):
                edge_far(it, 1, z).wait_send()

        if it == 0:
            for side_of in range(2):

                @pl.when(halo_sends[side_of])
                def _():
                    for kind in range(2):
                        halo_copy(kind, side_of).wait_send()

        for k in range(1, chips):

            @pl.when(peer_chip(k) < dense_chips)
            def _():
                band_copy(it, k).wait_send()

        @pl.when(is_dense)
        def _():
            for k in range(chips):
                band_pass(it, k).wait_send()
                pair_copy(it, k).wait_send()
            for k in range(1, chips):
                row_copy(it, k).wait_send()
            mix_copy(it).wait_send()
            for k in range(1, rows):
                zone_copy(it, k).wait_send()

            @pl.when(core == 0)
            def _():
                for k in range(1, rows):
                    window_copy(it, k).wait_send()
                    window_pass(it, k).wait_send()

            @pl.when(c != 0)
            def _():
                total_copy(it, c, 0).wait_send()


def local(
    trace_start, surface_load, panel_tiles, tile_list, surf_map, coef_index, coef_table, vol_source
):
    cols = lax.axis_size("col")
    rows = lax.axis_size("row")
    lines, layers, nodes = coef_index.shape
    slots, tile, _ = panel_tiles.shape
    rhs, shard = trace_start.shape
    per_shard = shard // tile
    levels = coef_table.shape[0]
    half = per_shard // CORES
    chips = cols // CORES
    span = shard + 2 * LANES
    cfg = (cols, rows, lines, per_shard, tile, slots, nodes, layers, rhs, levels)
    smem = pl.BlockSpec(memory_space=pltpu.SMEM)
    vmem = pl.BlockSpec(memory_space=pltpu.VMEM)
    hbm = pl.BlockSpec(memory_space=pl.ANY)
    block = (rhs, tile)
    dma = pltpu.SemaphoreType.DMA
    out = jax.ShapeDtypeStruct((rhs, shard), F32)
    return pl.pallas_call(
        functools.partial(kernel, cfg),
        out_shape=(out, out),
        in_specs=[smem] * 3 + [hbm] * 5,
        out_specs=(vmem, vmem),
        scratch_shapes=[
            pltpu.VMEM((slots, tile, tile), BF16),
            pltpu.VMEM((rhs, shard), F32),
            pltpu.VMEM((lines, layers, nodes), I32),
            pltpu.VMEM((lines, layers, nodes), F32),
            pltpu.VMEM((SUB, LANES), I32),
            pltpu.SMEM((SUB, LANES), I32),
            pltpu.VMEM((cols * per_shard,) + block, BF16),
            pltpu.VMEM((cols * per_shard,) + block, BF16),
            pltpu.VMEM((rows * per_shard,) + block, BF16),
            pltpu.VMEM((rows * per_shard,) + block, BF16),
            pltpu.VMEM((ITERS, lines + 1, rhs, LANES), BF16),
            pltpu.VMEM((ITERS, lines + 1, rhs, LANES), BF16),
            pltpu.VMEM((2, lines, layers, LANES), I32),
            pltpu.VMEM((2, lines, layers, LANES), F32),
            pltpu.VMEM((slots + 1,) + block, F32),
            pltpu.VMEM((ITERS, rows, half) + block, BF16),
            pltpu.VMEM((ITERS, rows, half) + block, BF16),
            pltpu.VMEM((half,) + block, F32),
            pltpu.VMEM((ITERS, rows, half) + block, BF16),
            pltpu.VMEM((ITERS, rows, half) + block, BF16),
            pltpu.VMEM((ITERS, half) + block, BF16),
            pltpu.VMEM((ITERS, cols, half) + block, BF16),
            pltpu.VMEM((ITERS, chips, per_shard) + block, BF16),
            pltpu.VMEM((ITERS, chips, per_shard) + block, BF16),
            pltpu.VMEM((per_shard,) + block, F32),
            pltpu.VMEM((ITERS, chips, per_shard) + block, BF16),
            pltpu.VMEM((ITERS, chips, per_shard) + block, BF16),
            pltpu.VMEM((layers, span), I32),
            pltpu.VMEM((layers, span), F32),
            pltpu.VMEM((layers, span), F32),
            pltpu.VMEM((5, layers, SUB, span), F32),
            pltpu.VMEM((2, layers, rhs, span), F32),
            pltpu.VMEM((rhs, span), F32),
            pltpu.VMEM((rhs, shard), F32),
            dma((slots,)),
            dma((4,)),
            dma,
            dma((ITERS, chips)),
            dma((ITERS, chips)),
            dma((ITERS, cols)),
            dma((ITERS, rows)),
            dma((ITERS, rows)),
            dma((ITERS, rows)),
            dma((ITERS, 2, lines + 1)),
            dma((ITERS, 2, lines + 1)),
            dma((2, 2)),
            dma((2, 2)),
            dma((ITERS,)),
            dma((ITERS,)),
            dma((ITERS, rows)),
            dma((ITERS, rows)),
            dma((ITERS,)),
            dma((ITERS, cols)),
            dma((ITERS, chips)),
            dma((ITERS, chips)),
            dma((ITERS, chips)),
            dma((ITERS, chips)),
        ],
        compiler_params=pltpu.CompilerParams(
            collective_id=0, has_side_effects=True, vmem_limit_bytes=60 * 1024 * 1024
        ),
        name="coupled",
    )(
        tile_list,
        surf_map,
        coef_table,
        trace_start,
        surface_load,
        coef_index,
        vol_source,
        panel_tiles,
    )


def solution(mesh):
    return jax.shard_map(
        local,
        mesh=mesh,
        in_specs=(
            P(None, ("col", "row")),
            P(None, ("col", "row")),
            P(("col", "row"), None, None),
            P(("col", "row")),
            P(),
            P(None, None, "row"),
            P(),
            P(None, None, "row"),
        ),
        out_specs=(P(None, ("col", "row")), P(None, ("col", "row"))),
        check_vma=False,
    )
```

```python
import functools

import jax
import jax.numpy as jnp
from jax import lax
from jax.experimental import pallas as pl
from jax.experimental.pallas import tpu as pltpu
from jax.sharding import PartitionSpec as P

ITERS = 2
SWEEPS = 4

COUPLING_STEP = 0.3
JACOBI_WEIGHT = 0.8
CELL_MASS = 0.05

LANES = 128
SUB = 8
CORES = 2
TURNED_BYTES = 36 * 1024 * 1024
F32 = jnp.float32
BF16 = jnp.bfloat16
I32 = jnp.int32


def quotient(x, n):
    return x >> (n.bit_length() - 1) if n & (n - 1) == 0 else lax.div(x, n)


def remainder(x, n):
    return x & (n - 1) if n & (n - 1) == 0 else lax.rem(x, n)


def kernel(
    cfg,
    list_hbm,
    surf_hbm,
    table_hbm,
    start_hbm,
    load_hbm,
    index_hbm,
    source_hbm,
    panel_hbm,
    middle_hbm,
    product_hbm,
    flux_hbm,
    middle_ref,
    product_ref,
    flux,
    list_ref,
    surf_ref,
    table_ref,
    panel,
    turned,
    traces_ref,
    load_ref,
    index_ref,
    source_ref,
    tab,
    order,
    near_band0,
    near_band1,
    far_band0,
    far_band1,
    near_window0,
    near_window1,
    far_window0,
    far_window1,
    edge_out,
    edge_left,
    edge_right,
    halo_index,
    halo_source,
    product,
    mix_out,
    mix_in,
    zone_own,
    zone_out,
    zone_in,
    total_own,
    total_out,
    total_in,
    pair_out,
    pair_in,
    row_own,
    row_out,
    row_in,
    index_ext,
    coef_ext,
    source_ext,
    weights,
    state,
    top,
    panel_sem,
    input_sem,
    output_sem,
    tab_sem,
    band_send,
    pass_send,
    near_recv,
    far_recv,
    win_send,
    win_pass,
    win_recv,
    win_far,
    edge_send,
    edge_recv,
    halo_send,
    halo_recv,
    mix_send,
    mix_recv,
    zone_send,
    zone_recv,
    total_send,
    total_recv,
    pair_send,
    pair_recv,
    row_send,
    row_recv,
):
    cols, rows, lines, per_shard, tile, slots, nodes, layers, rhs, levels, turns = cfg
    dense = cols - lines
    group = cols // lines
    shard = per_shard * tile
    half = per_shard // CORES
    chips = cols // CORES
    dense_chips = dense // CORES
    win_tiles = rows * per_shard
    band_tiles = cols * per_shard
    side = cols * rows * per_shard
    span = shard + 2 * LANES
    wide = tile // 2
    near_bands = (near_band0, near_band1)
    far_bands = (far_band0, far_band1)
    near_windows = (near_window0, near_window1)
    far_windows = (far_window0, far_window1)
    c = lax.axis_index("col")
    r = lax.axis_index("row")
    core = lax.rem(c, CORES)
    chip = lax.div(c, CORES)
    other = 1 - core
    partner = chip * CORES + other
    q = lax.div(c, group)
    m = lax.rem(c, group)
    is_dense = c < dense
    row_up = jnp.minimum(r + 1, rows - 1)
    row_down = jnp.maximum(r - 1, 0)
    first_of_tile = m == 0
    last_of_tile = m == group - 1
    cross_left = first_of_tile & (r > 0)
    cross_right = last_of_tile & (r < rows - 1)

    def copy(src, dst, send, recv, to_col, to_row):
        return pltpu.make_async_remote_copy(
            src_ref=src,
            dst_ref=dst,
            send_sem=send,
            recv_sem=recv,
            device_id=(to_col, to_row),
            device_id_type=pl.DeviceIdType.MESH,
        )

    stops = sorted({0, slots // 4, slots // 2 // 2 * 2, slots})

    def panel_copy(i):
        part = pl.ds(stops[i], stops[i + 1] - stops[i])
        return pltpu.make_async_copy(panel_hbm.at[part], panel.at[part], panel_sem.at[i])

    inputs = (
        (start_hbm, traces_ref),
        (index_hbm, index_ref),
        (source_hbm, source_ref),
        (load_hbm, load_ref),
        (list_hbm, list_ref),
        (surf_hbm, surf_ref),
        (table_hbm, table_ref),
    )

    def input_copy(i):
        return pltpu.make_async_copy(inputs[i][0], inputs[i][1], input_sem.at[i])

    outputs = ((middle_ref, middle_hbm), (product_ref, product_hbm), (flux, flux_hbm))

    def output_copy(i):
        return pltpu.make_async_copy(outputs[i][0], outputs[i][1], output_sem.at[i])

    barrier = pltpu.get_barrier_semaphore()

    def greet(to_col, to_row):
        pl.semaphore_signal(
            barrier, inc=1, device_id=(to_col, to_row), device_id_type=pl.DeviceIdType.MESH
        )

    for k in range(1, rows):
        greet(c, lax.rem(r + k, rows))
    for k in range(1, cols):
        greet(lax.rem(c + k, cols), r)

    @pl.when(cross_right)
    def _():
        for z in range(lines):
            greet(z * group, row_up)

    @pl.when(cross_left)
    def _():
        for z in range(lines):
            greet(z * group + group - 1, row_down)

    for i in (4, 0, 1, 2, 5, 6, 3):
        input_copy(i).start()

    @pl.when(is_dense)
    def _():
        for i in range(len(stops) - 1):
            panel_copy(i).start()


    padded_slots = -(-slots // SUB) * SUB
    lane = lax.broadcasted_iota(I32, (SUB, LANES), 1)

    def sort_slots():
        slot = lax.broadcasted_iota(I32, (padded_slots, LANES), 0)
        lanes = lax.broadcasted_iota(I32, (padded_slots, LANES), 1)
        row_key = jnp.full((padded_slots, LANES), band_tiles, I32)
        col_key = jnp.full((padded_slots, LANES), win_tiles, I32)
        keys = []
        for s in range(slots):
            name = list_ref[s]
            safe = jnp.maximum(name, 0)
            row = quotient(safe, side)
            row = quotient(quotient(row, per_shard), rows) * per_shard + remainder(row, per_shard)
            row = jnp.where(name >= 0, row, band_tiles)
            col = jnp.where(name >= 0, remainder(safe, side), win_tiles)
            keys.append((col, row))
            row_key = jnp.where(slot == s, row, row_key)
            col_key = jnp.where(slot == s, col, col_key)

        def fold(x):
            x = functools.reduce(jnp.add, [x[i : i + SUB] for i in range(0, padded_slots, SUB)])
            for shift in (4, 2, 1):
                x = x + pltpu.roll(x, shift, 0)
            return x

        for which, key, source, count in (
            (0, col_key, row_key, win_tiles),
            (1, row_key, col_key, band_tiles),
        ):
            rank = jnp.zeros((padded_slots, LANES), I32)
            upto = jnp.zeros((SUB, LANES), I32)
            equal = jnp.zeros((SUB, LANES), I32)
            for s in range(slots):
                value = keys[s][which]
                ahead = (key > value) | ((key == value) & (slot > s))
                rank = rank + jnp.where(ahead, 1, 0)
                upto = upto + jnp.where(lane >= value, 1, 0)
                equal = equal + jnp.where(lane == value, 1, 0)
            rank = jnp.where(slot < slots, rank, LANES)
            here = rank == lanes
            place = fold(jnp.where(here, slot, 0))
            origin = fold(jnp.where(here, jnp.where(key < count, source, 0), 0))
            value = fold(jnp.where(here, key, 0))
            keep = (value == pltpu.roll(value, 1, 1)) & (lane > 0)
            last = jnp.where(equal > 0, upto - 1, slots)
            for i, x in enumerate((place, origin, jnp.where(keep, 1, 0), last)):
                tab[4 * which + i : 4 * which + i + 1, :] = x[0:1, :]

    input_copy(4).wait()

    @pl.when(is_dense)
    def _():
        sort_slots()
        pltpu.make_async_copy(tab, order, tab_sem).start()
        product[slots] = jnp.zeros((rhs, tile), F32)

    input_copy(0).wait()
    input_copy(1).wait()
    input_copy(2).wait()
    input_copy(5).wait()
    input_copy(6).wait()

    expected = (
        cols - 1 + rows - 1 + jnp.where(cross_right, lines, 0) + jnp.where(cross_left, lines, 0)
    )
    pl.semaphore_wait(barrier, expected)

    def settle(ref, sem):
        copy(ref, ref, sem, sem, partner, r).wait_recv()

    def settle_send(ref, sem):
        copy(ref, ref, sem, sem, partner, r).wait_send()


    def halo_copy(kind, side_of, arrival=False):
        ref = (index_ref, source_ref)[kind]
        dst = (halo_index, halo_source)[kind]
        at = nodes - LANES if side_of == 0 else 0
        to = row_up if (side_of == 0) != arrival else row_down
        return copy(
            ref.at[:, :, pl.ds(at, LANES)],
            dst.at[side_of],
            halo_send.at[side_of],
            halo_recv.at[side_of],
            c,
            to,
        )

    halo_sends = (first_of_tile & (r < rows - 1), last_of_tile & (r > 0))
    halo_receives = (cross_left, cross_right)


    def edge_near(it, side_of):
        dst = (edge_left, edge_right)[side_of]
        return copy(
            edge_out.at[it, side_of],
            dst.at[it, lines],
            edge_send.at[it, side_of],
            edge_recv.at[it, side_of],
            c + 1 if side_of == 0 else c - 1,
            r,
        )

    def edge_far(it, side_of, z):
        dst = (edge_left, edge_right)[side_of]
        to = (z * group, row_up) if side_of == 0 else (z * group + group - 1, row_down)
        return copy(
            edge_out.at[it, side_of],
            dst.at[it, q],
            edge_send.at[it, side_of],
            edge_recv.at[it, side_of],
            *to,
        )


    def shards(ref, col, count=1):
        return ref.at[pl.ds(col * per_shard, count * per_shard)]

    bits = chips.bit_length() - 1
    power = chips == 1 << bits
    near_first = sorted(range(1, chips), key=lambda k: k.bit_count() if power else k)
    far_first = near_first[::-1]

    def peer_chip(k):
        if not power:
            return lax.rem(chip + k, chips)
        digits = [remainder(quotient(chip, 1 << b), 2) for b in range(bits)]
        return sum((1 - d if k >> b & 1 else d) * (1 << b) for b, d in enumerate(digits))

    def band_copies(it, k):
        peer = peer_chip(k) * CORES
        send, recv = band_send.at[it], near_recv.at[it, chip]
        near, far = shards(near_bands[it], c), shards(far_bands[it], c)
        return copy(near, near, send, recv, peer + core, r), copy(far, near, send, recv, peer + other, r)

    def partner_copies(it):
        near, far = shards(near_bands[it], c), shards(far_bands[it], c)
        return (
            copy(far, near, band_send.at[it], near_recv.at[it, chip], partner, r),
            copy(near, far, pass_send.at[it], far_recv.at[it], partner, r),
        )

    def band_pass(it, k):
        at = peer_chip(k) * CORES
        return copy(
            shards(near_bands[it], at, CORES),
            shards(far_bands[it], at, CORES),
            pass_send.at[it],
            far_recv.at[it],
            partner,
            r,
        )

    def to_rows(send):
        for d in range(rows - 1, 0, -1):

            @pl.when(r + d < rows)
            def _():
                send(r + d)

            @pl.when(r >= d)
            def _():
                send(r - d)

    def window_copy(it, peer):
        return copy(
            shards(near_bands[it], 0),
            shards(near_windows[it], r),
            win_send.at[it],
            win_recv.at[it, r],
            c,
            peer,
        )

    def window_pass(it, at):
        return copy(
            shards(near_windows[it], at),
            shards(far_windows[it], at),
            win_pass.at[it],
            win_far.at[it],
            partner,
            r,
        )

    def send_window(it):
        to_rows(lambda peer: window_copy(it, peer).start())


    def mix_copy(it, h):
        return copy(
            mix_out.at[it, h], mix_in.at[it, h], mix_send.at[it], mix_recv.at[it, h], partner, r
        )

    def zone_copy(it, h, peer):
        return copy(
            zone_out.at[it, h, peer],
            zone_in.at[it, h, r],
            zone_send.at[it],
            zone_recv.at[it],
            c,
            peer,
        )

    def total_copy(it):
        return copy(
            total_out.at[it], total_in.at[it, c], total_send.at[it], total_recv.at[it], 0, r
        )


    def pair_copy(it, h):
        return copy(
            pair_out.at[it, h],
            pair_in.at[it, h],
            pair_send.at[it],
            pair_recv.at[it, h],
            partner,
            r,
        )

    def row_copy(it, h, k):
        peer = peer_chip(k)
        return copy(
            row_out.at[it, h, peer],
            row_in.at[it, h, chip],
            row_send.at[it],
            row_recv.at[it],
            peer * CORES + core,
            r,
        )

    def prepare_volume():
        line = lax.div(surf_ref[r * lines + q], rows)
        for side_of, edge_of_tile in ((0, first_of_tile), (1, last_of_tile)):
            to = pl.ds(0 if side_of == 0 else LANES + shard, LANES)
            at = m * shard - LANES if side_of == 0 else m * shard + shard
            at = pl.multiple_of(jnp.clip(at, 0, nodes - LANES), LANES)
            receives = halo_receives[side_of]

            @pl.when(jnp.logical_not(edge_of_tile))
            def _():
                index_ext[:, to] = index_ref[line, :, pl.ds(at, LANES)]
                source_ext[:, to] = source_ref[line, :, pl.ds(at, LANES)]

            @pl.when(receives)
            def _():
                settle(halo_source, halo_recv.at[side_of])
                index_ext[:, to] = halo_index[side_of, line]
                source_ext[:, to] = halo_source[side_of, line]

            @pl.when(edge_of_tile & jnp.logical_not(receives))
            def _():
                index_ext[:, to] = jnp.full((layers, LANES), levels, I32)
                source_ext[:, to] = jnp.zeros((layers, LANES), F32)

        at = pl.multiple_of(m * shard, LANES)
        index_ext[:, LANES : LANES + shard] = index_ref[line, :, pl.ds(at, shard)]
        source_ext[:, LANES : LANES + shard] = source_ref[line, :, pl.ds(at, shard)]
        indices = index_ext[...]
        coefs = jnp.zeros((layers, span), F32)
        for level in range(levels):
            coefs = jnp.where(indices == level, table_ref[level], coefs)
        coef_ext[...] = coefs
        inside = index_ext[0:1, :] < levels
        for layer in range(layers):
            k = coef_ext[layer : layer + 1, :]
            left = 0.5 * (k + pltpu.roll(k, 1, 1))
            right = 0.5 * (k + pltpu.roll(k, span - 1, 1))
            up = 0.5 * (k + coef_ext[layer - 1 : layer, :]) if layer else k
            diagonal = left + right + up + CELL_MASS
            parts = [left, right, up]
            if layer < layers - 1:
                down = 0.5 * (k + coef_ext[layer + 1 : layer + 2, :])
                diagonal = diagonal + down
                parts.append(down)
            else:
                parts.append(None)
            parts.append(source_ext[layer : layer + 1, :])
            scale = jnp.where(inside, JACOBI_WEIGHT / diagonal, 0.0)
            for kind, part in enumerate(parts):
                if part is not None:
                    weights[kind, layer] = jnp.broadcast_to(part * scale, (SUB, span))

    def relax(now, g, first):
        at = pl.ds(g * SUB, SUB)
        for layer in range(layers):
            value = weights[4, layer]
            if first:
                if layer == 0:
                    value = value + weights[2, layer] * top[at, :]
            else:
                centre = state[now, layer, at, :]
                value = value + (1.0 - JACOBI_WEIGHT) * centre
                value = value + weights[0, layer] * pltpu.roll(centre, 1, 1)
                value = value + weights[1, layer] * pltpu.roll(centre, span - 1, 1)
                above = state[now, layer - 1, at, :] if layer else top[at, :]
                value = value + weights[2, layer] * above
                if layer < layers - 1:
                    value = value + weights[3, layer] * state[now, layer + 1, at, :]
            state[1 - now, layer, at, :] = value

    def gather_top(it):
        line = lax.div(surf_ref[r * lines + q], rows)
        for side_of, edge_of_tile in ((0, first_of_tile), (1, last_of_tile)):
            dst = (edge_left, edge_right)[side_of]
            to = slice(0, LANES) if side_of == 0 else slice(LANES + shard, span)
            base = row_down if side_of == 0 else row_up
            place = 0
            for z in range(lines):
                place = jnp.where(surf_ref[base * lines + z] == line * rows + base, z, place)
            receives = halo_receives[side_of]

            @pl.when(jnp.logical_not(edge_of_tile))
            def _():
                settle(dst.at[it, lines], edge_recv.at[it, side_of])
                top[:, to] = dst[it, lines].astype(F32)

            @pl.when(receives)
            def _():
                settle(dst.at[it, pl.ds(0, lines)], edge_recv.at[it, side_of])
                value = dst[it, 0]
                for z in range(1, lines):
                    value = jnp.where(place == z, dst[it, z], value)
                top[:, to] = value.astype(F32)

            @pl.when(edge_of_tile & jnp.logical_not(receives))
            def _():
                top[:, to] = jnp.zeros((rhs, LANES), F32)

    def relax_groups(it, begin, end):
        def rows_of(g, _):
            for i in range(SWEEPS):
                relax(i % 2, g, it == 0 and i == 0)
            at = pl.ds(g * SUB, SUB)
            k = jnp.broadcast_to(coef_ext[0:1, LANES : LANES + shard], (SUB, shard))
            flux[at, :] = k * (
                top[at, LANES : LANES + shard]
                - state[SWEEPS % 2, 0, at, LANES : LANES + shard]
            )
            return 0

        lax.fori_loop(begin, end, rows_of, 0)

    def lanes_of(h):
        return slice(h * wide, (h + 1) * wide)

    def segments(which, traces_of, part, h=None):
        at = slice(None) if h is None else lanes_of(h)
        part = pl.ds(pl.multiple_of(part * wide, wide), wide)
        acc = jnp.zeros((rhs, tile if h is None else wide), F32)
        for k in range(slots):
            s = order[4 * which, k]
            traces = traces_of[order[4 * which + 1, k]]
            keep = order[4 * which + 2, k].astype(F32)
            if which == 0:
                term = jnp.dot(traces, panel[s, part, at], preferred_element_type=F32)
            elif turns == slots or k < turns:
                block = turned[s if turns == slots else k, part, at]
                term = jnp.dot(traces, block, preferred_element_type=F32)
            else:
                block = panel[s, at, part]
                contract = (((1,), (1,)), ((), ()))
                term = lax.dot_general(traces, block, contract, preferred_element_type=F32)
            acc = acc * keep + term
            product[k, :, at] = acc if h is None else product[k, :, at] + acc

    def last_of(which, h, at):
        return product[order[4 * which + 3, at], :, lanes_of(h)]

    def send_mix(it, h):
        for z in range(rows):
            for p in range(half):
                value = last_of(0, h, z * per_shard + other * half + p)
                mix_out[it, h, z, p] = value.astype(BF16)
                zone_own[h, z, p] = last_of(0, h, z * per_shard + core * half + p)
        mix_copy(it, h).start()

    def send_zone(it, h):
        settle(mix_in.at[it, h], mix_recv.at[it, h])
        for z in range(rows):
            for p in range(half):
                value = zone_own[h, z, p] + mix_in[it, h, z, p].astype(F32)
                zone_own[h, z, p] = value
                zone_out[it, h, z, p] = value.astype(BF16)
        to_rows(lambda peer: zone_copy(it, h, peer).start())

    def send_pair(it, h):
        for k in range(chips):
            for p in range(per_shard):
                value = last_of(1, h, (k * CORES + other) * per_shard + p)
                pair_out[it, h, k, p] = value.astype(BF16)
                row_own[h, k, p] = last_of(1, h, (k * CORES + core) * per_shard + p)
        pair_copy(it, h).start()

    def send_rows(it, h):
        settle(pair_in.at[it, h], pair_recv.at[it, h])
        for k in range(chips):
            for p in range(per_shard):
                value = row_own[h, k, p] + pair_in[it, h, k, p].astype(F32)
                row_own[h, k, p] = value
                row_out[it, h, k, p] = value.astype(BF16)
        for k in far_first:
            row_copy(it, h, k).start()

    def wait_panel():
        for i in range(len(stops) - 1):
            panel_copy(i).wait()


    def turn(i):
        begin, end = min(stops[i], turns), min(stops[i + 1], turns)
        if turns == slots:
            panel_copy(i).wait()

        def one(k):
            turned[k] = panel[k if turns == slots else order[4, k]].T

        def two(j, _):
            one(begin + 2 * j)
            one(begin + 2 * j + 1)
            return 0

        lax.fori_loop(0, (end - begin) // 2, two, 0)
        if (end - begin) % 2:
            one(end - 1)

    def dense_part(it):
        near_band, far_band = near_bands[it], far_bands[it]
        near_window, far_window = near_windows[it], far_windows[it]
        if it == 0:
            if turns < slots:
                pltpu.make_async_copy(tab, order, tab_sem).wait()
                wait_panel()
            for i in range(len(stops) - 2):
                turn(i)
        settle(shards(near_band, partner), near_recv.at[it, chip])

        @pl.when(c == 1)
        def _():
            send_window(it)

        for i, k in enumerate(near_first):
            settle(shards(near_band, peer_chip(k) * CORES, CORES), near_recv.at[it, peer_chip(k)])
            band_pass(it, k).start()

            @pl.when(peer_chip(k) == 0)
            def _():
                send_window(it)

            if it == 0 and i == min(1, len(near_first) - 1):
                turn(len(stops) - 2)

        if it == 0 and turns == slots:
            pltpu.make_async_copy(tab, order, tab_sem).wait()
        segments(0, near_band, core)
        settle(shards(far_band, 0, cols - 1), far_recv.at[it])
        near_window[pl.ds(r * per_shard, per_shard)] = near_band[0:per_shard]
        far_window[pl.ds(r * per_shard, per_shard)] = far_band[0:per_shard]
        segments(0, far_band, other, 0)
        send_mix(it, 0)
        segments(0, far_band, other, 1)
        send_mix(it, 1)
        send_zone(it, 0)
        send_zone(it, 1)
        for k in range(1, rows):
            at = lax.rem(r + k, rows)
            settle(shards(near_window, at), win_recv.at[it, at])
            window_pass(it, at).start()
        segments(1, near_window, core)
        settle(shards(far_window, 0, rows - 1), win_far.at[it])
        segments(1, far_window, other, 0)
        send_pair(it, 0)
        segments(1, far_window, other, 1)
        send_pair(it, 1)
        groups = rhs // SUB
        gather_top(it)
        relax_groups(it, 0, groups // 4)
        send_rows(it, 0)
        relax_groups(it, groups // 4, groups // 2)
        send_rows(it, 1)
        settle(zone_in.at[it, :, pl.ds(0, rows - 1)], zone_recv.at[it])
        for p in range(half):
            for h in range(2):
                value = zone_own[h, r, p]
                for k in range(1, rows):
                    value = value + zone_in[it, h, lax.rem(r + k, rows), p].astype(F32)
                total_own[p, :, lanes_of(h)] = value
                total_out[it, p, :, lanes_of(h)] = value.astype(BF16)

        @pl.when(c != 0)
        def _():
            total_copy(it).start()

        relax_groups(it, groups // 2, groups)

    def drain(it):
        for side_of, near, far in (
            (0, jnp.logical_not(last_of_tile), cross_right),
            (1, jnp.logical_not(first_of_tile), cross_left),
        ):

            @pl.when(near)
            def _():
                settle_send(edge_left.at[it, 0], edge_send.at[it, side_of])

            @pl.when(far)
            def _():
                settle_send(edge_left.at[it, pl.ds(0, lines)], edge_send.at[it, side_of])

        if it == 0:
            for side_of in range(2):

                @pl.when(halo_sends[side_of])
                def _():
                    settle_send(halo_source, halo_send.at[side_of])

        @pl.when(jnp.logical_not(is_dense))
        def _():
            settle_send(shards(near_bands[it], 0, dense_chips * CORES), band_send.at[it])

        @pl.when(is_dense)
        def _():
            settle_send(shards(near_bands[it], 0, (dense_chips - 1) * CORES + 1), band_send.at[it])
            settle_send(shards(near_bands[it], 0, cols - 1), pass_send.at[it])
            settle_send(shards(near_windows[it], 0, rows - 1), win_send.at[it])
            settle_send(shards(near_windows[it], 0, rows - 1), win_pass.at[it])
            settle_send(mix_out.at[it], mix_send.at[it])
            settle_send(zone_out.at[it, :, pl.ds(0, rows - 1)], zone_send.at[it])
            settle_send(pair_out.at[it], pair_send.at[it])
            settle_send(row_out.at[it, :, pl.ds(0, chips - 1)], row_send.at[it])

            @pl.when(c != 0)
            def _():
                settle_send(total_out.at[it], total_send.at[it])

    for it in range(ITERS):
        for p in range(per_shard):
            rounded = traces_ref[:, p * tile : (p + 1) * tile].astype(BF16)
            low, high = rounded[:, :wide], rounded[:, wide:]
            near_bands[it][c * per_shard + p] = jnp.where(core == 0, low, high)
            far_bands[it][c * per_shard + p] = jnp.where(core == 0, high, low)
            top[:, LANES + p * tile : LANES + (p + 1) * tile] = rounded.astype(F32)
            if p == per_shard - 1:
                edge_out[it, 0] = rounded[:, tile - LANES :]
            if p == 0:
                edge_out[it, 1] = rounded[:, :LANES]

        @pl.when(jnp.logical_not(last_of_tile))
        def _():
            edge_near(it, 0).start()

        @pl.when(jnp.logical_not(first_of_tile))
        def _():
            edge_near(it, 1).start()

        @pl.when(cross_right)
        def _():
            for z in range(lines):
                edge_far(it, 0, z).start()

        @pl.when(cross_left)
        def _():
            for z in range(lines):
                edge_far(it, 1, z).start()

        if it == 0:
            for side_of in range(2):

                @pl.when(halo_sends[side_of])
                def _():
                    for kind in range(2):
                        halo_copy(kind, side_of).start()

        for k in near_first:

            @pl.when(peer_chip(k) < dense_chips)
            def _():
                for part in band_copies(it, k):
                    part.start()

        @pl.when(is_dense)
        def _():
            for part in partner_copies(it):
                part.start()

        @pl.when(c == 0)
        def _():
            send_window(it)

        if it == 0:
            prepare_volume()

        @pl.when(is_dense)
        def _():
            dense_part(it)

        @pl.when(jnp.logical_not(is_dense))
        def _():
            gather_top(it)
            relax_groups(it, 0, rhs // SUB)

        if it == 0:
            input_copy(3).wait()
        middle_ref[...] = traces_ref[...] + COUPLING_STEP * (load_ref[...] - traces_ref[...])
        if it == ITERS - 1:
            output_copy(0).start()
            output_copy(2).start()
            for done in range(ITERS):
                drain(done)

        def own(h, p):
            return slice(p * tile + h * wide, p * tile + (h + 1) * wide)

        @pl.when(is_dense)
        def _():
            for h in range(2):
                for p in range(per_shard):
                    product_ref[:, own(h, p)] = row_own[h, chip, p]

        @pl.when(jnp.logical_not(is_dense))
        def _():
            product_ref[...] = jnp.zeros((rhs, shard), F32)

        @pl.when(is_dense)
        def _():
            settle(row_in.at[it, :, pl.ds(0, dense_chips - 1)], row_recv.at[it])

        @pl.when(jnp.logical_not(is_dense))
        def _():
            settle(row_in.at[it, :, pl.ds(0, dense_chips)], row_recv.at[it])

        for src in range(dense_chips):

            @pl.when(src != chip)
            def _():
                for h in range(2):
                    for p in range(per_shard):
                        product_ref[:, own(h, p)] += row_in[it, h, src, p].astype(F32)

        @pl.when(c == 0)
        def _():
            settle(total_in.at[it, pl.ds(0, dense - 1)], total_recv.at[it])
            for p in range(half):
                at = slice(p * tile, (p + 1) * tile)
                product_ref[:, at] += total_own[p]
            for src in range(1, dense):
                for p in range(half):
                    at = (src % CORES) * half + p
                    at = slice(at * tile, (at + 1) * tile)
                    product_ref[:, at] += total_in[it, src, p].astype(F32)

        if it < ITERS - 1:
            change = COUPLING_STEP * (product_ref[...] + flux[...])
            traces_ref[...] = middle_ref[...] - change

    output_copy(1).start()
    for i in range(len(outputs)):
        output_copy(i).wait()


def local(
    trace_start, surface_load, panel_tiles, tile_list, surf_map, coef_index, coef_table, vol_source
):
    cols = lax.axis_size("col")
    rows = lax.axis_size("row")
    lines, layers, nodes = coef_index.shape
    slots, tile, _ = panel_tiles.shape
    rhs, shard = trace_start.shape
    per_shard = shard // tile
    levels = coef_table.shape[0]
    half = per_shard // CORES
    chips = cols // CORES
    span = shard + 2 * LANES
    turns = min(slots, TURNED_BYTES // (2 * tile * tile) - slots)
    cfg = (cols, rows, lines, per_shard, tile, slots, nodes, layers, rhs, levels, turns)
    hbm = pl.BlockSpec(memory_space=pl.ANY)
    block = (rhs, tile)
    piece = (rhs, tile // 2)
    dma = pltpu.SemaphoreType.DMA
    out = jax.ShapeDtypeStruct((rhs, shard), F32)
    middle, product, flux = pl.pallas_call(
        functools.partial(kernel, cfg),
        out_shape=(out,) * 3,
        in_specs=[hbm] * 8,
        out_specs=(hbm,) * 3,
        scratch_shapes=[
            pltpu.VMEM((rhs, shard), F32),
            pltpu.VMEM((rhs, shard), F32),
            pltpu.VMEM((rhs, shard), F32),
            pltpu.SMEM(tile_list.shape, I32),
            pltpu.SMEM(surf_map.shape, I32),
            pltpu.SMEM(coef_table.shape, F32),
            pltpu.VMEM((slots, tile, tile), BF16),
            pltpu.VMEM((turns, tile, tile), BF16),
            pltpu.VMEM((rhs, shard), F32),
            pltpu.VMEM((rhs, shard), F32),
            pltpu.VMEM((lines, layers, nodes), I32),
            pltpu.VMEM((lines, layers, nodes), F32),
            pltpu.VMEM((SUB, LANES), I32),
            pltpu.SMEM((SUB, LANES), I32),
            pltpu.VMEM((cols * per_shard,) + piece, BF16),
            pltpu.VMEM((cols * per_shard,) + piece, BF16),
            pltpu.VMEM((cols * per_shard,) + piece, BF16),
            pltpu.VMEM((cols * per_shard,) + piece, BF16),
            pltpu.VMEM((rows * per_shard,) + piece, BF16),
            pltpu.VMEM((rows * per_shard,) + piece, BF16),
            pltpu.VMEM((rows * per_shard,) + piece, BF16),
            pltpu.VMEM((rows * per_shard,) + piece, BF16),
            pltpu.VMEM((ITERS, 2, rhs, LANES), BF16),
            pltpu.VMEM((ITERS, lines + 1, rhs, LANES), BF16),
            pltpu.VMEM((ITERS, lines + 1, rhs, LANES), BF16),
            pltpu.VMEM((2, lines, layers, LANES), I32),
            pltpu.VMEM((2, lines, layers, LANES), F32),
            pltpu.VMEM((slots + 1,) + block, F32),
            pltpu.VMEM((ITERS, 2, rows, half) + piece, BF16),
            pltpu.VMEM((ITERS, 2, rows, half) + piece, BF16),
            pltpu.VMEM((2, rows, half) + piece, F32),
            pltpu.VMEM((ITERS, 2, rows, half) + piece, BF16),
            pltpu.VMEM((ITERS, 2, rows, half) + piece, BF16),
            pltpu.VMEM((half,) + block, F32),
            pltpu.VMEM((ITERS, half) + block, BF16),
            pltpu.VMEM((ITERS, cols, half) + block, BF16),
            pltpu.VMEM((ITERS, 2, chips, per_shard) + piece, BF16),
            pltpu.VMEM((ITERS, 2, chips, per_shard) + piece, BF16),
            pltpu.VMEM((2, chips, per_shard) + piece, F32),
            pltpu.VMEM((ITERS, 2, chips, per_shard) + piece, BF16),
            pltpu.VMEM((ITERS, 2, chips, per_shard) + piece, BF16),
            pltpu.VMEM((layers, span), I32),
            pltpu.VMEM((layers, span), F32),
            pltpu.VMEM((layers, span), F32),
            pltpu.VMEM((5, layers, SUB, span), F32),
            pltpu.VMEM((2, layers, rhs, span), F32),
            pltpu.VMEM((rhs, span), F32),
            dma((3,)),
            dma((7,)),
            dma((3,)),
            dma,
            dma((ITERS,)),
            dma((ITERS,)),
            dma((ITERS, chips)),
            dma((ITERS,)),
            dma((ITERS,)),
            dma((ITERS,)),
            dma((ITERS, rows)),
            dma((ITERS,)),
            dma((ITERS, 2)),
            dma((ITERS, 2)),
            dma((2,)),
            dma((2,)),
            dma((ITERS,)),
            dma((ITERS, 2)),
            dma((ITERS,)),
            dma((ITERS,)),
            dma((ITERS,)),
            dma((ITERS,)),
            dma((ITERS,)),
            dma((ITERS, 2)),
            dma((ITERS,)),
            dma((ITERS,)),
        ],
        compiler_params=pltpu.CompilerParams(
            collective_id=0, has_side_effects=True, vmem_limit_bytes=60 * 1024 * 1024
        ),
        name="coupled",
    )(
        tile_list,
        surf_map,
        coef_table,
        trace_start,
        surface_load,
        coef_index,
        vol_source,
        panel_tiles,
    )
    response = product + flux
    return middle - COUPLING_STEP * response, response


def solution(mesh):
    return jax.shard_map(
        local,
        mesh=mesh,
        in_specs=(
            P(None, ("col", "row")),
            P(None, ("col", "row")),
            P(("col", "row"), None, None),
            P(("col", "row")),
            P(),
            P(None, None, "row"),
            P(),
            P(None, None, "row"),
        ),
        out_specs=(P(None, ("col", "row")), P(None, ("col", "row"))),
        check_vma=False,
    )
```

```python
import functools

import jax
import jax.numpy as jnp
from jax import lax
from jax.experimental import pallas as pl
from jax.experimental.pallas import tpu as pltpu
from jax.sharding import PartitionSpec as P

ITERS = 2
SWEEPS = 4

COUPLING_STEP = 0.3
JACOBI_WEIGHT = 0.8
CELL_MASS = 0.05

LANES = 128
SUB = 8
CORES = 2
TURNED_BYTES = 36 * 1024 * 1024
F32 = jnp.float32
BF16 = jnp.bfloat16
I32 = jnp.int32


def quotient(x, n):
    return x >> (n.bit_length() - 1) if n & (n - 1) == 0 else lax.div(x, n)


def remainder(x, n):
    return x & (n - 1) if n & (n - 1) == 0 else lax.rem(x, n)


def kernel(
    cfg,
    list_hbm,
    surf_hbm,
    table_hbm,
    start_hbm,
    load_hbm,
    index_hbm,
    source_hbm,
    panel_hbm,
    middle_hbm,
    product_hbm,
    flux_hbm,
    middle_ref,
    product_ref,
    flux,
    list_ref,
    surf_ref,
    table_ref,
    panel,
    turned,
    traces_ref,
    load_ref,
    index_ref,
    source_ref,
    tab,
    order,
    near_band0,
    near_band1,
    far_band0,
    far_band1,
    near_window0,
    near_window1,
    far_window0,
    far_window1,
    edge_out,
    edge_left,
    edge_right,
    halo_index,
    halo_source,
    product,
    mix_out,
    mix_in,
    zone_own,
    zone_out,
    zone_in,
    total_own,
    total_out,
    total_in,
    pair_out,
    pair_in,
    row_own,
    row_out,
    row_in,
    index_ext,
    coef_ext,
    source_ext,
    weights,
    state,
    top,
    panel_sem,
    input_sem,
    output_sem,
    tab_sem,
    band_send,
    pass_send,
    near_recv,
    far_recv,
    win_send,
    win_pass,
    win_recv,
    win_far,
    edge_send,
    edge_recv,
    halo_send,
    halo_recv,
    mix_send,
    mix_recv,
    zone_send,
    zone_recv,
    total_send,
    total_recv,
    pair_send,
    pair_recv,
    row_send,
    row_recv,
):
    cols, rows, lines, per_shard, tile, slots, nodes, layers, rhs, levels, turns = cfg
    dense = cols - lines
    group = cols // lines
    shard = per_shard * tile
    half = per_shard // CORES
    chips = cols // CORES
    dense_chips = dense // CORES
    win_tiles = rows * per_shard
    band_tiles = cols * per_shard
    side = cols * rows * per_shard
    span = shard + 2 * LANES
    wide = tile // 2
    near_bands = (near_band0, near_band1)
    far_bands = (far_band0, far_band1)
    near_windows = (near_window0, near_window1)
    far_windows = (far_window0, far_window1)
    c = lax.axis_index("col")
    r = lax.axis_index("row")
    core = lax.rem(c, CORES)
    chip = lax.div(c, CORES)
    other = 1 - core
    partner = chip * CORES + other
    q = lax.div(c, group)
    m = lax.rem(c, group)
    is_dense = c < dense
    row_up = jnp.minimum(r + 1, rows - 1)
    row_down = jnp.maximum(r - 1, 0)
    first_of_tile = m == 0
    last_of_tile = m == group - 1
    cross_left = first_of_tile & (r > 0)
    cross_right = last_of_tile & (r < rows - 1)

    def copy(src, dst, send, recv, to_col, to_row):
        return pltpu.make_async_remote_copy(
            src_ref=src,
            dst_ref=dst,
            send_sem=send,
            recv_sem=recv,
            device_id=(to_col, to_row),
            device_id_type=pl.DeviceIdType.MESH,
        )

    stops = sorted({0, slots * 3 // 8, slots * 3 // 4, slots})

    def panel_copy(i):
        part = pl.ds(stops[i], stops[i + 1] - stops[i])
        return pltpu.make_async_copy(panel_hbm.at[part], panel.at[part], panel_sem.at[i])

    inputs = (
        (start_hbm, traces_ref),
        (index_hbm, index_ref),
        (source_hbm, source_ref),
        (load_hbm, load_ref),
        (list_hbm, list_ref),
        (surf_hbm, surf_ref),
        (table_hbm, table_ref),
    )

    def input_copy(i):
        return pltpu.make_async_copy(inputs[i][0], inputs[i][1], input_sem.at[i])

    outputs = ((middle_ref, middle_hbm), (product_ref, product_hbm), (flux, flux_hbm))

    def output_copy(i):
        return pltpu.make_async_copy(outputs[i][0], outputs[i][1], output_sem.at[i])

    barrier = pltpu.get_barrier_semaphore()

    def greet(to_col, to_row):
        pl.semaphore_signal(
            barrier, inc=1, device_id=(to_col, to_row), device_id_type=pl.DeviceIdType.MESH
        )

    input_copy(0).start()
    for k in range(1, rows):
        greet(c, lax.rem(r + k, rows))
    for k in range(1, cols):
        greet(lax.rem(c + k, cols), r)

    @pl.when(cross_right)
    def _():
        for z in range(lines):
            greet(z * group, row_up)

    @pl.when(cross_left)
    def _():
        for z in range(lines):
            greet(z * group + group - 1, row_down)

    for i in (1, 2, 4, 5, 6, 3):
        input_copy(i).start()

    @pl.when(is_dense)
    def _():
        for i in range(len(stops) - 1):
            panel_copy(i).start()


    padded_slots = -(-slots // SUB) * SUB
    lane = lax.broadcasted_iota(I32, (SUB, LANES), 1)

    def sort_slots():
        slot = lax.broadcasted_iota(I32, (padded_slots, LANES), 0)
        lanes = lax.broadcasted_iota(I32, (padded_slots, LANES), 1)
        row_key = jnp.full((padded_slots, LANES), band_tiles, I32)
        col_key = jnp.full((padded_slots, LANES), win_tiles, I32)
        keys = []
        for s in range(slots):
            name = list_ref[s]
            safe = jnp.maximum(name, 0)
            row = quotient(safe, side)
            row = quotient(quotient(row, per_shard), rows) * per_shard + remainder(row, per_shard)
            row = jnp.where(name >= 0, row, band_tiles)
            col = jnp.where(name >= 0, remainder(safe, side), win_tiles)
            keys.append((col, row))
            row_key = jnp.where(slot == s, row, row_key)
            col_key = jnp.where(slot == s, col, col_key)

        def fold(x):
            x = functools.reduce(jnp.add, [x[i : i + SUB] for i in range(0, padded_slots, SUB)])
            for shift in (4, 2, 1):
                x = x + pltpu.roll(x, shift, 0)
            return x

        for which, key, source, count in (
            (0, col_key, row_key, win_tiles),
            (1, row_key, col_key, band_tiles),
        ):
            rank = jnp.zeros((padded_slots, LANES), I32)
            upto = jnp.zeros((SUB, LANES), I32)
            equal = jnp.zeros((SUB, LANES), I32)
            for s in range(slots):
                value = keys[s][which]
                ahead = (key > value) | ((key == value) & (slot > s))
                rank = rank + jnp.where(ahead, 1, 0)
                upto = upto + jnp.where(lane >= value, 1, 0)
                equal = equal + jnp.where(lane == value, 1, 0)
            rank = jnp.where(slot < slots, rank, LANES)
            here = rank == lanes
            place = fold(jnp.where(here, slot, 0))
            origin = fold(jnp.where(here, jnp.where(key < count, source, 0), 0))
            value = fold(jnp.where(here, key, 0))
            keep = (value == pltpu.roll(value, 1, 1)) & (lane > 0)
            last = jnp.where(equal > 0, upto - 1, slots)
            for i, x in enumerate((place, origin, jnp.where(keep, 1, 0), last)):
                tab[4 * which + i : 4 * which + i + 1, :] = x[0:1, :]

    input_copy(0).wait()
    expected = (
        cols - 1 + rows - 1 + jnp.where(cross_right, lines, 0) + jnp.where(cross_left, lines, 0)
    )
    pl.semaphore_wait(barrier, expected)

    def settle(ref, sem):
        copy(ref, ref, sem, sem, partner, r).wait_recv()

    def settle_send(ref, sem):
        copy(ref, ref, sem, sem, partner, r).wait_send()


    def halo_copy(kind, side_of, arrival=False):
        ref = (index_ref, source_ref)[kind]
        dst = (halo_index, halo_source)[kind]
        at = nodes - LANES if side_of == 0 else 0
        to = row_up if (side_of == 0) != arrival else row_down
        return copy(
            ref.at[:, :, pl.ds(at, LANES)],
            dst.at[side_of],
            halo_send.at[side_of],
            halo_recv.at[side_of],
            c,
            to,
        )

    halo_sends = (first_of_tile & (r < rows - 1), last_of_tile & (r > 0))
    halo_receives = (cross_left, cross_right)


    def edge_near(it, side_of):
        dst = (edge_left, edge_right)[side_of]
        return copy(
            edge_out.at[it, side_of],
            dst.at[it, lines],
            edge_send.at[it, side_of],
            edge_recv.at[it, side_of],
            c + 1 if side_of == 0 else c - 1,
            r,
        )

    def edge_far(it, side_of, z):
        dst = (edge_left, edge_right)[side_of]
        to = (z * group, row_up) if side_of == 0 else (z * group + group - 1, row_down)
        return copy(
            edge_out.at[it, side_of],
            dst.at[it, q],
            edge_send.at[it, side_of],
            edge_recv.at[it, side_of],
            *to,
        )


    def shards(ref, col, count=1):
        return ref.at[pl.ds(col * per_shard, count * per_shard)]

    bits = chips.bit_length() - 1
    power = chips == 1 << bits
    near_first = sorted(range(1, chips), key=lambda k: k.bit_count() if power else k)
    beside = [k for k in near_first if power and k.bit_count() == 1]
    beyond = [k for k in near_first if k not in beside]

    def peer_chip(k):
        if not power:
            return lax.rem(chip + k, chips)
        digits = [remainder(quotient(chip, 1 << b), 2) for b in range(bits)]
        return sum((1 - d if k >> b & 1 else d) * (1 << b) for b, d in enumerate(digits))

    def band_copies(it, k):
        peer = peer_chip(k) * CORES
        send, recv = band_send.at[it], near_recv.at[it, chip]
        near, far = shards(near_bands[it], c), shards(far_bands[it], c)
        return copy(near, near, send, recv, peer + core, r), copy(far, near, send, recv, peer + other, r)

    def partner_copies(it):
        near, far = shards(near_bands[it], c), shards(far_bands[it], c)
        return (
            copy(far, near, band_send.at[it], near_recv.at[it, chip], partner, r),
            copy(near, far, pass_send.at[it], far_recv.at[it], partner, r),
        )

    def band_pass(it, peer):
        at = peer * CORES
        return copy(
            shards(near_bands[it], at, CORES),
            shards(far_bands[it], at, CORES),
            pass_send.at[it],
            far_recv.at[it],
            partner,
            r,
        )

    def to_rows(send):
        for d in range(rows - 1, 0, -1):

            @pl.when(r + d < rows)
            def _():
                send(r + d)

            @pl.when(r >= d)
            def _():
                send(r - d)

    def window_copy(it, peer):
        return copy(
            shards(near_bands[it], 0),
            shards(near_windows[it], r),
            win_send.at[it],
            win_recv.at[it, r],
            c,
            peer,
        )

    def window_pass(it, at):
        return copy(
            shards(near_windows[it], at),
            shards(far_windows[it], at),
            win_pass.at[it],
            win_far.at[it],
            partner,
            r,
        )

    def send_window(it):
        to_rows(lambda peer: window_copy(it, peer).start())


    def mix_copy(it, h):
        return copy(
            mix_out.at[it, h], mix_in.at[it, h], mix_send.at[it], mix_recv.at[it, h], partner, r
        )

    def zone_copy(it, h, peer):
        return copy(
            zone_out.at[it, h, peer],
            zone_in.at[it, h, r],
            zone_send.at[it],
            zone_recv.at[it],
            c,
            peer,
        )

    def total_copy(it):
        return copy(
            total_out.at[it], total_in.at[it, c], total_send.at[it], total_recv.at[it], 0, r
        )


    def pair_copy(it, h):
        return copy(
            pair_out.at[it, h],
            pair_in.at[it, h],
            pair_send.at[it],
            pair_recv.at[it, h],
            partner,
            r,
        )

    def row_copy(it, h, k):
        peer = peer_chip(k)
        return copy(
            row_out.at[it, h, peer],
            row_in.at[it, h, chip],
            row_send.at[it],
            row_recv.at[it],
            peer * CORES + core,
            r,
        )

    def prepare_volume():
        line = lax.div(surf_ref[r * lines + q], rows)
        for side_of, edge_of_tile in ((0, first_of_tile), (1, last_of_tile)):
            to = pl.ds(0 if side_of == 0 else LANES + shard, LANES)
            at = m * shard - LANES if side_of == 0 else m * shard + shard
            at = pl.multiple_of(jnp.clip(at, 0, nodes - LANES), LANES)
            receives = halo_receives[side_of]

            @pl.when(jnp.logical_not(edge_of_tile))
            def _():
                index_ext[:, to] = index_ref[line, :, pl.ds(at, LANES)]
                source_ext[:, to] = source_ref[line, :, pl.ds(at, LANES)]

            @pl.when(receives)
            def _():
                settle(halo_source, halo_recv.at[side_of])
                index_ext[:, to] = halo_index[side_of, line]
                source_ext[:, to] = halo_source[side_of, line]

            @pl.when(edge_of_tile & jnp.logical_not(receives))
            def _():
                index_ext[:, to] = jnp.full((layers, LANES), levels, I32)
                source_ext[:, to] = jnp.zeros((layers, LANES), F32)

        at = pl.multiple_of(m * shard, LANES)
        index_ext[:, LANES : LANES + shard] = index_ref[line, :, pl.ds(at, shard)]
        source_ext[:, LANES : LANES + shard] = source_ref[line, :, pl.ds(at, shard)]
        indices = index_ext[...]
        coefs = jnp.zeros((layers, span), F32)
        for level in range(levels):
            coefs = jnp.where(indices == level, table_ref[level], coefs)
        coef_ext[...] = coefs
        inside = index_ext[0:1, :] < levels
        for layer in range(layers):
            k = coef_ext[layer : layer + 1, :]
            left = 0.5 * (k + pltpu.roll(k, 1, 1))
            right = 0.5 * (k + pltpu.roll(k, span - 1, 1))
            up = 0.5 * (k + coef_ext[layer - 1 : layer, :]) if layer else k
            diagonal = left + right + up + CELL_MASS
            parts = [left, right, up]
            if layer < layers - 1:
                down = 0.5 * (k + coef_ext[layer + 1 : layer + 2, :])
                diagonal = diagonal + down
                parts.append(down)
            else:
                parts.append(None)
            parts.append(source_ext[layer : layer + 1, :])
            scale = jnp.where(inside, JACOBI_WEIGHT / diagonal, 0.0)
            for kind, part in enumerate(parts):
                if part is not None:
                    weights[kind, layer] = jnp.broadcast_to(part * scale, (SUB, span))

    def relax(now, g, first):
        at = pl.ds(g * SUB, SUB)
        for layer in range(layers):
            value = weights[4, layer]
            if first:
                if layer == 0:
                    value = value + weights[2, layer] * top[at, :]
            else:
                centre = state[now, layer, at, :]
                value = value + (1.0 - JACOBI_WEIGHT) * centre
                value = value + weights[0, layer] * pltpu.roll(centre, 1, 1)
                value = value + weights[1, layer] * pltpu.roll(centre, span - 1, 1)
                above = state[now, layer - 1, at, :] if layer else top[at, :]
                value = value + weights[2, layer] * above
                if layer < layers - 1:
                    value = value + weights[3, layer] * state[now, layer + 1, at, :]
            state[1 - now, layer, at, :] = value

    def gather_top(it):
        line = lax.div(surf_ref[r * lines + q], rows)
        for side_of, edge_of_tile in ((0, first_of_tile), (1, last_of_tile)):
            dst = (edge_left, edge_right)[side_of]
            to = slice(0, LANES) if side_of == 0 else slice(LANES + shard, span)
            base = row_down if side_of == 0 else row_up
            place = 0
            for z in range(lines):
                place = jnp.where(surf_ref[base * lines + z] == line * rows + base, z, place)
            receives = halo_receives[side_of]

            @pl.when(jnp.logical_not(edge_of_tile))
            def _():
                settle(dst.at[it, lines], edge_recv.at[it, side_of])
                top[:, to] = dst[it, lines].astype(F32)

            @pl.when(receives)
            def _():
                settle(dst.at[it, pl.ds(0, lines)], edge_recv.at[it, side_of])
                value = dst[it, 0]
                for z in range(1, lines):
                    value = jnp.where(place == z, dst[it, z], value)
                top[:, to] = value.astype(F32)

            @pl.when(edge_of_tile & jnp.logical_not(receives))
            def _():
                top[:, to] = jnp.zeros((rhs, LANES), F32)

    def relax_groups(it, begin, end):
        def rows_of(g, _):
            for i in range(SWEEPS):
                relax(i % 2, g, it == 0 and i == 0)
            at = pl.ds(g * SUB, SUB)
            k = jnp.broadcast_to(coef_ext[0:1, LANES : LANES + shard], (SUB, shard))
            flux[at, :] = k * (
                top[at, LANES : LANES + shard]
                - state[SWEEPS % 2, 0, at, LANES : LANES + shard]
            )
            return 0

        lax.fori_loop(begin, end, rows_of, 0)

    def lanes_of(h):
        return slice(h * wide, (h + 1) * wide)

    def segments(which, traces_of, part, h=None):
        at = slice(None) if h is None else lanes_of(h)
        part = pl.ds(pl.multiple_of(part * wide, wide), wide)
        acc = jnp.zeros((rhs, tile if h is None else wide), F32)
        for k in range(slots):
            s = order[4 * which, k]
            traces = traces_of[order[4 * which + 1, k]]
            keep = order[4 * which + 2, k].astype(F32)
            if which == 0:
                term = jnp.dot(traces, panel[s, part, at], preferred_element_type=F32)
            elif turns == slots or k < turns:
                block = turned[s if turns == slots else k, part, at]
                term = jnp.dot(traces, block, preferred_element_type=F32)
            else:
                block = panel[s, at, part]
                contract = (((1,), (1,)), ((), ()))
                term = lax.dot_general(traces, block, contract, preferred_element_type=F32)
            acc = acc * keep + term
            product[k, :, at] = acc if h is None else product[k, :, at] + acc

    def last_of(which, h, at):
        return product[order[4 * which + 3, at], :, lanes_of(h)]

    def send_mix(it, h):
        for z in range(rows):
            for p in range(half):
                value = last_of(0, h, z * per_shard + other * half + p)
                mix_out[it, h, z, p] = value.astype(BF16)
                zone_own[h, z, p] = last_of(0, h, z * per_shard + core * half + p)
        mix_copy(it, h).start()

    def send_zone(it, h):
        settle(mix_in.at[it, h], mix_recv.at[it, h])
        for z in range(rows):
            for p in range(half):
                value = zone_own[h, z, p] + mix_in[it, h, z, p].astype(F32)
                zone_own[h, z, p] = value
                zone_out[it, h, z, p] = value.astype(BF16)
        to_rows(lambda peer: zone_copy(it, h, peer).start())

    def send_pair(it, h):
        for k in range(chips):
            for p in range(per_shard):
                value = last_of(1, h, (k * CORES + other) * per_shard + p)
                pair_out[it, h, k, p] = value.astype(BF16)
                row_own[h, k, p] = last_of(1, h, (k * CORES + core) * per_shard + p)
        pair_copy(it, h).start()

    def send_rows(it, h):
        settle(pair_in.at[it, h], pair_recv.at[it, h])
        for k in range(chips):
            for p in range(per_shard):
                value = row_own[h, k, p] + pair_in[it, h, k, p].astype(F32)
                row_own[h, k, p] = value
                row_out[it, h, k, p] = value.astype(BF16)
        for k in near_first if h == 0 and it < ITERS - 1 else beside:
            row_copy(it, h, k).start()

    def wait_panel():
        for i in range(len(stops) - 1):
            panel_copy(i).wait()


    def turn(i):
        begin, end = min(stops[i], turns), min(stops[i + 1], turns)
        if turns == slots:
            panel_copy(i).wait()

        def one(k):
            turned[k] = panel[k if turns == slots else order[4, k]].T

        def two(j, _):
            one(begin + 2 * j)
            one(begin + 2 * j + 1)
            return 0

        lax.fori_loop(0, (end - begin) // 2, two, 0)
        if (end - begin) % 2:
            one(end - 1)

    def begin():
        input_copy(1).wait()
        input_copy(2).wait()
        for side_of in range(2):

            @pl.when(halo_sends[side_of])
            def _():
                for kind in range(2):
                    halo_copy(kind, side_of).start()

        input_copy(4).wait()
        input_copy(5).wait()
        input_copy(6).wait()

        @pl.when(is_dense)
        def _():
            sort_slots()
            pltpu.make_async_copy(tab, order, tab_sem).start()
            product[slots] = jnp.zeros((rhs, tile), F32)

    def dense_part(it):
        near_band, far_band = near_bands[it], far_bands[it]
        near_window, far_window = near_windows[it], far_windows[it]
        if it == 0:
            if turns < slots:
                pltpu.make_async_copy(tab, order, tab_sem).wait()
                wait_panel()
            for i in range(len(stops) - 2):
                turn(i)
            prepare_volume()
        settle(shards(near_band, partner), near_recv.at[it, chip])

        @pl.when(c == 1)
        def _():
            send_window(it)

        def pass_on(peer):
            settle(shards(near_band, peer * CORES, CORES), near_recv.at[it, peer])
            band_pass(it, peer).start()

        @pl.when(chip != 0)
        def _():
            settle(shards(near_band, 0, CORES), near_recv.at[it, 0])
            send_window(it)
            band_pass(it, 0).start()

        if it == 0:
            turn(len(stops) - 2)
        for k in near_first:
            peer = peer_chip(k)

            @pl.when(peer != 0)
            def _():
                pass_on(peer)

        if it == 0 and turns == slots:
            pltpu.make_async_copy(tab, order, tab_sem).wait()
        segments(0, near_band, core)
        settle(shards(far_band, 0, cols - 1), far_recv.at[it])
        near_window[pl.ds(r * per_shard, per_shard)] = near_band[0:per_shard]
        far_window[pl.ds(r * per_shard, per_shard)] = far_band[0:per_shard]
        segments(0, far_band, other, 0)
        send_mix(it, 0)
        segments(0, far_band, other, 1)
        send_mix(it, 1)
        send_zone(it, 0)
        if it > 0:
            send_zone(it, 1)
        for k in range(1, rows):
            at = lax.rem(r + k, rows)
            settle(shards(near_window, at), win_recv.at[it, at])
            window_pass(it, at).start()
        segments(1, near_window, core)
        if it == 0:
            send_zone(it, 1)
        settle(shards(far_window, 0, rows - 1), win_far.at[it])
        segments(1, far_window, other, 0)
        send_pair(it, 0)
        segments(1, far_window, other, 1)
        send_pair(it, 1)
        groups = rhs // SUB
        gather_top(it)
        relax_groups(it, 0, groups // 4)
        send_rows(it, 0)
        relax_groups(it, groups // 4, groups // 2)
        send_rows(it, 1)
        settle(zone_in.at[it, :, pl.ds(0, rows - 1)], zone_recv.at[it])
        for p in range(half):
            for h in range(2):
                value = zone_own[h, r, p]
                for k in range(1, rows):
                    value = value + zone_in[it, h, lax.rem(r + k, rows), p].astype(F32)
                total_own[p, :, lanes_of(h)] = value
                total_out[it, p, :, lanes_of(h)] = value.astype(BF16)

        @pl.when(c != 0)
        def _():
            total_copy(it).start()

        for h in range(0 if it == ITERS - 1 else 1, 2):
            for k in beyond:
                row_copy(it, h, k).start()
        relax_groups(it, groups // 2, groups)

    def drain(it):
        for side_of, near, far in (
            (0, jnp.logical_not(last_of_tile), cross_right),
            (1, jnp.logical_not(first_of_tile), cross_left),
        ):

            @pl.when(near)
            def _():
                settle_send(edge_left.at[it, 0], edge_send.at[it, side_of])

            @pl.when(far)
            def _():
                settle_send(edge_left.at[it, pl.ds(0, lines)], edge_send.at[it, side_of])

        if it == 0:
            for side_of in range(2):

                @pl.when(halo_sends[side_of])
                def _():
                    settle_send(halo_source, halo_send.at[side_of])

        @pl.when(jnp.logical_not(is_dense))
        def _():
            settle_send(shards(near_bands[it], 0, dense_chips * CORES), band_send.at[it])

        @pl.when(is_dense)
        def _():
            settle_send(shards(near_bands[it], 0, (dense_chips - 1) * CORES + 1), band_send.at[it])
            settle_send(shards(near_bands[it], 0, cols - 1), pass_send.at[it])
            settle_send(shards(near_windows[it], 0, rows - 1), win_send.at[it])
            settle_send(shards(near_windows[it], 0, rows - 1), win_pass.at[it])
            settle_send(mix_out.at[it], mix_send.at[it])
            settle_send(zone_out.at[it, :, pl.ds(0, rows - 1)], zone_send.at[it])
            settle_send(pair_out.at[it], pair_send.at[it])
            settle_send(row_out.at[it, :, pl.ds(0, chips - 1)], row_send.at[it])

            @pl.when(c != 0)
            def _():
                settle_send(total_out.at[it], total_send.at[it])

    for it in range(ITERS):
        for p in range(per_shard):
            rounded = traces_ref[:, p * tile : (p + 1) * tile].astype(BF16)
            low, high = rounded[:, :wide], rounded[:, wide:]
            near_bands[it][c * per_shard + p] = jnp.where(core == 0, low, high)
            far_bands[it][c * per_shard + p] = jnp.where(core == 0, high, low)
            top[:, LANES + p * tile : LANES + (p + 1) * tile] = rounded.astype(F32)
            if p == per_shard - 1:
                edge_out[it, 0] = rounded[:, tile - LANES :]
            if p == 0:
                edge_out[it, 1] = rounded[:, :LANES]

        @pl.when(jnp.logical_not(last_of_tile))
        def _():
            edge_near(it, 0).start()

        @pl.when(jnp.logical_not(first_of_tile))
        def _():
            edge_near(it, 1).start()

        @pl.when(cross_right)
        def _():
            for z in range(lines):
                edge_far(it, 0, z).start()

        @pl.when(cross_left)
        def _():
            for z in range(lines):
                edge_far(it, 1, z).start()

        for k in near_first:

            @pl.when(peer_chip(k) < dense_chips)
            def _():
                for part in band_copies(it, k):
                    part.start()

        @pl.when(is_dense)
        def _():
            for part in partner_copies(it):
                part.start()

        @pl.when(c == 0)
        def _():
            send_window(it)

        if it == 0:
            begin()

        @pl.when(is_dense)
        def _():
            dense_part(it)

        @pl.when(jnp.logical_not(is_dense))
        def _():
            if it == 0:
                prepare_volume()
            gather_top(it)
            relax_groups(it, 0, rhs // SUB)

        if it == 0:
            input_copy(3).wait()
        middle_ref[...] = traces_ref[...] + COUPLING_STEP * (load_ref[...] - traces_ref[...])
        if it == ITERS - 1:
            output_copy(0).start()
            output_copy(2).start()
            for done in range(ITERS):
                drain(done)

        def own(h, p):
            return slice(p * tile + h * wide, p * tile + (h + 1) * wide)

        @pl.when(is_dense)
        def _():
            for h in range(2):
                for p in range(per_shard):
                    product_ref[:, own(h, p)] = row_own[h, chip, p]

        @pl.when(jnp.logical_not(is_dense))
        def _():
            product_ref[...] = jnp.zeros((rhs, shard), F32)

        @pl.when(is_dense)
        def _():
            settle(row_in.at[it, :, pl.ds(0, dense_chips - 1)], row_recv.at[it])

        @pl.when(jnp.logical_not(is_dense))
        def _():
            settle(row_in.at[it, :, pl.ds(0, dense_chips)], row_recv.at[it])

        for src in range(dense_chips):

            @pl.when(src != chip)
            def _():
                for h in range(2):
                    for p in range(per_shard):
                        product_ref[:, own(h, p)] += row_in[it, h, src, p].astype(F32)

        @pl.when(c == 0)
        def _():
            settle(total_in.at[it, pl.ds(0, dense - 1)], total_recv.at[it])
            for p in range(half):
                at = slice(p * tile, (p + 1) * tile)
                product_ref[:, at] += total_own[p]
            for src in range(1, dense):
                for p in range(half):
                    at = (src % CORES) * half + p
                    at = slice(at * tile, (at + 1) * tile)
                    product_ref[:, at] += total_in[it, src, p].astype(F32)

        if it < ITERS - 1:
            change = COUPLING_STEP * (product_ref[...] + flux[...])
            traces_ref[...] = middle_ref[...] - change

    output_copy(1).start()
    for i in range(len(outputs)):
        output_copy(i).wait()


def local(
    trace_start, surface_load, panel_tiles, tile_list, surf_map, coef_index, coef_table, vol_source
):
    cols = lax.axis_size("col")
    rows = lax.axis_size("row")
    lines, layers, nodes = coef_index.shape
    slots, tile, _ = panel_tiles.shape
    rhs, shard = trace_start.shape
    per_shard = shard // tile
    levels = coef_table.shape[0]
    half = per_shard // CORES
    chips = cols // CORES
    span = shard + 2 * LANES
    turns = min(slots, TURNED_BYTES // (2 * tile * tile) - slots)
    cfg = (cols, rows, lines, per_shard, tile, slots, nodes, layers, rhs, levels, turns)
    hbm = pl.BlockSpec(memory_space=pl.ANY)
    block = (rhs, tile)
    piece = (rhs, tile // 2)
    dma = pltpu.SemaphoreType.DMA
    out = jax.ShapeDtypeStruct((rhs, shard), F32)
    middle, product, flux = pl.pallas_call(
        functools.partial(kernel, cfg),
        out_shape=(out,) * 3,
        in_specs=[hbm] * 8,
        out_specs=(hbm,) * 3,
        scratch_shapes=[
            pltpu.VMEM((rhs, shard), F32),
            pltpu.VMEM((rhs, shard), F32),
            pltpu.VMEM((rhs, shard), F32),
            pltpu.SMEM(tile_list.shape, I32),
            pltpu.SMEM(surf_map.shape, I32),
            pltpu.SMEM(coef_table.shape, F32),
            pltpu.VMEM((slots, tile, tile), BF16),
            pltpu.VMEM((turns, tile, tile), BF16),
            pltpu.VMEM((rhs, shard), F32),
            pltpu.VMEM((rhs, shard), F32),
            pltpu.VMEM((lines, layers, nodes), I32),
            pltpu.VMEM((lines, layers, nodes), F32),
            pltpu.VMEM((SUB, LANES), I32),
            pltpu.SMEM((SUB, LANES), I32),
            pltpu.VMEM((cols * per_shard,) + piece, BF16),
            pltpu.VMEM((cols * per_shard,) + piece, BF16),
            pltpu.VMEM((cols * per_shard,) + piece, BF16),
            pltpu.VMEM((cols * per_shard,) + piece, BF16),
            pltpu.VMEM((rows * per_shard,) + piece, BF16),
            pltpu.VMEM((rows * per_shard,) + piece, BF16),
            pltpu.VMEM((rows * per_shard,) + piece, BF16),
            pltpu.VMEM((rows * per_shard,) + piece, BF16),
            pltpu.VMEM((ITERS, 2, rhs, LANES), BF16),
            pltpu.VMEM((ITERS, lines + 1, rhs, LANES), BF16),
            pltpu.VMEM((ITERS, lines + 1, rhs, LANES), BF16),
            pltpu.VMEM((2, lines, layers, LANES), I32),
            pltpu.VMEM((2, lines, layers, LANES), F32),
            pltpu.VMEM((slots + 1,) + block, F32),
            pltpu.VMEM((ITERS, 2, rows, half) + piece, BF16),
            pltpu.VMEM((ITERS, 2, rows, half) + piece, BF16),
            pltpu.VMEM((2, rows, half) + piece, F32),
            pltpu.VMEM((ITERS, 2, rows, half) + piece, BF16),
            pltpu.VMEM((ITERS, 2, rows, half) + piece, BF16),
            pltpu.VMEM((half,) + block, F32),
            pltpu.VMEM((ITERS, half) + block, BF16),
            pltpu.VMEM((ITERS, cols, half) + block, BF16),
            pltpu.VMEM((ITERS, 2, chips, per_shard) + piece, BF16),
            pltpu.VMEM((ITERS, 2, chips, per_shard) + piece, BF16),
            pltpu.VMEM((2, chips, per_shard) + piece, F32),
            pltpu.VMEM((ITERS, 2, chips, per_shard) + piece, BF16),
            pltpu.VMEM((ITERS, 2, chips, per_shard) + piece, BF16),
            pltpu.VMEM((layers, span), I32),
            pltpu.VMEM((layers, span), F32),
            pltpu.VMEM((layers, span), F32),
            pltpu.VMEM((5, layers, SUB, span), F32),
            pltpu.VMEM((2, layers, rhs, span), F32),
            pltpu.VMEM((rhs, span), F32),
            dma((3,)),
            dma((7,)),
            dma((3,)),
            dma,
            dma((ITERS,)),
            dma((ITERS,)),
            dma((ITERS, chips)),
            dma((ITERS,)),
            dma((ITERS,)),
            dma((ITERS,)),
            dma((ITERS, rows)),
            dma((ITERS,)),
            dma((ITERS, 2)),
            dma((ITERS, 2)),
            dma((2,)),
            dma((2,)),
            dma((ITERS,)),
            dma((ITERS, 2)),
            dma((ITERS,)),
            dma((ITERS,)),
            dma((ITERS,)),
            dma((ITERS,)),
            dma((ITERS,)),
            dma((ITERS, 2)),
            dma((ITERS,)),
            dma((ITERS,)),
        ],
        compiler_params=pltpu.CompilerParams(
            collective_id=0, has_side_effects=True, vmem_limit_bytes=60 * 1024 * 1024
        ),
        name="coupled",
    )(
        tile_list,
        surf_map,
        coef_table,
        trace_start,
        surface_load,
        coef_index,
        vol_source,
        panel_tiles,
    )
    response = product + flux
    return middle - COUPLING_STEP * response, response


def solution(mesh):
    return jax.shard_map(
        local,
        mesh=mesh,
        in_specs=(
            P(None, ("col", "row")),
            P(None, ("col", "row")),
            P(("col", "row"), None, None),
            P(("col", "row")),
            P(),
            P(None, None, "row"),
            P(),
            P(None, None, "row"),
        ),
        out_specs=(P(None, ("col", "row")), P(None, ("col", "row"))),
        check_vma=False,
    )
```

```python
import functools

import jax
import jax.numpy as jnp
from jax import lax
from jax.experimental import pallas as pl
from jax.experimental.pallas import tpu as pltpu
from jax.sharding import PartitionSpec as P

ITERS = 2
SWEEPS = 4

COUPLING_STEP = 0.3
JACOBI_WEIGHT = 0.8
CELL_MASS = 0.05

LANES = 128
SUB = 8
CORES = 2
TURNED_BYTES = 36 * 1024 * 1024
F32 = jnp.float32
BF16 = jnp.bfloat16
I32 = jnp.int32


def quotient(x, n):
    return x >> (n.bit_length() - 1) if n & (n - 1) == 0 else lax.div(x, n)


def remainder(x, n):
    return x & (n - 1) if n & (n - 1) == 0 else lax.rem(x, n)


def kernel(
    cfg,
    list_hbm,
    surf_hbm,
    table_hbm,
    start_hbm,
    load_hbm,
    index_hbm,
    source_hbm,
    panel_hbm,
    middle_hbm,
    product_hbm,
    flux_hbm,
    middle_ref,
    product_ref,
    flux,
    list_ref,
    surf_ref,
    table_ref,
    panel,
    turned,
    traces_ref,
    load_ref,
    index_ref,
    source_ref,
    tab,
    order,
    near_band0,
    near_band1,
    far_band0,
    far_band1,
    near_window0,
    near_window1,
    far_window0,
    far_window1,
    edge_out,
    edge_left,
    edge_right,
    halo_index,
    halo_source,
    product,
    mix_out,
    mix_in,
    zone_own,
    zone_out,
    zone_in,
    total_own,
    total_out,
    total_in,
    pair_out,
    pair_in,
    row_own,
    row_out,
    row_in,
    index_ext,
    coef_ext,
    source_ext,
    weights,
    state,
    top,
    panel_sem,
    input_sem,
    output_sem,
    tab_sem,
    band_send,
    pass_send,
    near_recv,
    far_recv,
    win_send,
    win_pass,
    win_recv,
    win_far,
    edge_send,
    edge_recv,
    halo_send,
    halo_recv,
    mix_send,
    mix_recv,
    zone_send,
    zone_recv,
    total_send,
    total_recv,
    pair_send,
    pair_recv,
    row_send,
    row_recv,
):
    cols, rows, lines, per_shard, tile, slots, nodes, layers, rhs, levels, turns = cfg
    dense = cols - lines
    group = cols // lines
    shard = per_shard * tile
    half = per_shard // CORES
    chips = cols // CORES
    dense_chips = dense // CORES
    win_tiles = rows * per_shard
    band_tiles = cols * per_shard
    side = cols * rows * per_shard
    span = shard + 2 * LANES
    wide = tile // 2
    near_bands = (near_band0, near_band1)
    far_bands = (far_band0, far_band1)
    near_windows = (near_window0, near_window1)
    far_windows = (far_window0, far_window1)
    c = lax.axis_index("col")
    r = lax.axis_index("row")
    core = lax.rem(c, CORES)
    chip = lax.div(c, CORES)
    other = 1 - core
    partner = chip * CORES + other
    q = lax.div(c, group)
    m = lax.rem(c, group)
    is_dense = c < dense
    row_up = jnp.minimum(r + 1, rows - 1)
    row_down = jnp.maximum(r - 1, 0)
    first_of_tile = m == 0
    last_of_tile = m == group - 1
    cross_left = first_of_tile & (r > 0)
    cross_right = last_of_tile & (r < rows - 1)

    def copy(src, dst, send, recv, to_col, to_row):
        return pltpu.make_async_remote_copy(
            src_ref=src,
            dst_ref=dst,
            send_sem=send,
            recv_sem=recv,
            device_id=(to_col, to_row),
            device_id_type=pl.DeviceIdType.MESH,
        )

    stops = sorted({0, slots * 3 // 8, slots * 3 // 4, slots})

    def panel_copy(i):
        part = pl.ds(stops[i], stops[i + 1] - stops[i])
        return pltpu.make_async_copy(panel_hbm.at[part], panel.at[part], panel_sem.at[i])

    inputs = (
        (start_hbm, traces_ref),
        (index_hbm, index_ref),
        (source_hbm, source_ref),
        (load_hbm, load_ref),
        (list_hbm, list_ref),
        (surf_hbm, surf_ref),
        (table_hbm, table_ref),
    )

    def input_copy(i):
        return pltpu.make_async_copy(inputs[i][0], inputs[i][1], input_sem.at[i])

    outputs = ((middle_ref, middle_hbm), (product_ref, product_hbm), (flux, flux_hbm))

    def output_copy(i):
        return pltpu.make_async_copy(outputs[i][0], outputs[i][1], output_sem.at[i])

    barrier = pltpu.get_barrier_semaphore()

    def greet(to_col, to_row):
        pl.semaphore_signal(
            barrier, inc=1, device_id=(to_col, to_row), device_id_type=pl.DeviceIdType.MESH
        )

    input_copy(0).start()
    for k in range(1, rows):
        greet(c, lax.rem(r + k, rows))
    for k in range(1, cols):
        greet(lax.rem(c + k, cols), r)

    @pl.when(cross_right)
    def _():
        for z in range(lines):
            greet(z * group, row_up)

    @pl.when(cross_left)
    def _():
        for z in range(lines):
            greet(z * group + group - 1, row_down)

    for i in (1, 2, 4, 5, 6, 3):
        input_copy(i).start()

    @pl.when(is_dense)
    def _():
        for i in range(len(stops) - 1):
            panel_copy(i).start()


    padded_slots = -(-slots // SUB) * SUB
    lane = lax.broadcasted_iota(I32, (SUB, LANES), 1)

    def sort_slots():
        slot = lax.broadcasted_iota(I32, (padded_slots, LANES), 0)
        lanes = lax.broadcasted_iota(I32, (padded_slots, LANES), 1)
        row_key = jnp.full((padded_slots, LANES), band_tiles, I32)
        col_key = jnp.full((padded_slots, LANES), win_tiles, I32)
        keys = []
        for s in range(slots):
            name = list_ref[s]
            safe = jnp.maximum(name, 0)
            row = quotient(safe, side)
            row = quotient(quotient(row, per_shard), rows) * per_shard + remainder(row, per_shard)
            row = jnp.where(name >= 0, row, band_tiles)
            col = jnp.where(name >= 0, remainder(safe, side), win_tiles)
            keys.append((col, row))
            row_key = jnp.where(slot == s, row, row_key)
            col_key = jnp.where(slot == s, col, col_key)

        def fold(x):
            x = functools.reduce(jnp.add, [x[i : i + SUB] for i in range(0, padded_slots, SUB)])
            for shift in (4, 2, 1):
                x = x + pltpu.roll(x, shift, 0)
            return x

        for which, key, source, count in (
            (0, col_key, row_key, win_tiles),
            (1, row_key, col_key, band_tiles),
        ):
            rank = jnp.zeros((padded_slots, LANES), I32)
            upto = jnp.zeros((SUB, LANES), I32)
            equal = jnp.zeros((SUB, LANES), I32)
            for s in range(slots):
                value = keys[s][which]
                ahead = (key > value) | ((key == value) & (slot > s))
                rank = rank + jnp.where(ahead, 1, 0)
                upto = upto + jnp.where(lane >= value, 1, 0)
                equal = equal + jnp.where(lane == value, 1, 0)
            rank = jnp.where(slot < slots, rank, LANES)
            here = rank == lanes
            place = fold(jnp.where(here, slot, 0))
            origin = fold(jnp.where(here, jnp.where(key < count, source, 0), 0))
            value = fold(jnp.where(here, key, 0))
            keep = (value == pltpu.roll(value, 1, 1)) & (lane > 0)
            last = jnp.where(equal > 0, upto - 1, slots)
            for i, x in enumerate((place, origin, jnp.where(keep, 1, 0), last)):
                tab[4 * which + i : 4 * which + i + 1, :] = x[0:1, :]

    input_copy(0).wait()
    expected = (
        cols - 1 + rows - 1 + jnp.where(cross_right, lines, 0) + jnp.where(cross_left, lines, 0)
    )

    def settle(ref, sem):
        copy(ref, ref, sem, sem, partner, r).wait_recv()

    def settle_send(ref, sem):
        copy(ref, ref, sem, sem, partner, r).wait_send()


    def halo_copy(kind, side_of, arrival=False):
        ref = (index_ref, source_ref)[kind]
        dst = (halo_index, halo_source)[kind]
        at = nodes - LANES if side_of == 0 else 0
        to = row_up if (side_of == 0) != arrival else row_down
        return copy(
            ref.at[:, :, pl.ds(at, LANES)],
            dst.at[side_of],
            halo_send.at[side_of],
            halo_recv.at[side_of],
            c,
            to,
        )

    halo_sends = (first_of_tile & (r < rows - 1), last_of_tile & (r > 0))
    halo_receives = (cross_left, cross_right)


    def edge_near(it, side_of):
        dst = (edge_left, edge_right)[side_of]
        return copy(
            edge_out.at[it, side_of],
            dst.at[it, lines],
            edge_send.at[it, side_of],
            edge_recv.at[it, side_of],
            c + 1 if side_of == 0 else c - 1,
            r,
        )

    def edge_far(it, side_of, z):
        dst = (edge_left, edge_right)[side_of]
        to = (z * group, row_up) if side_of == 0 else (z * group + group - 1, row_down)
        return copy(
            edge_out.at[it, side_of],
            dst.at[it, q],
            edge_send.at[it, side_of],
            edge_recv.at[it, side_of],
            *to,
        )


    def shards(ref, col, count=1):
        return ref.at[pl.ds(col * per_shard, count * per_shard)]

    bits = chips.bit_length() - 1
    power = chips == 1 << bits
    near_first = sorted(range(1, chips), key=lambda k: k.bit_count() if power else k)
    beside = [k for k in near_first if power and k.bit_count() == 1]
    beyond = [k for k in near_first if k not in beside]

    def peer_chip(k):
        if not power:
            return lax.rem(chip + k, chips)
        digits = [remainder(quotient(chip, 1 << b), 2) for b in range(bits)]
        return sum((1 - d if k >> b & 1 else d) * (1 << b) for b, d in enumerate(digits))

    def band_copies(it, k):
        peer = peer_chip(k) * CORES
        send, recv = band_send.at[it], near_recv.at[it, chip]
        near, far = shards(near_bands[it], c), shards(far_bands[it], c)
        return copy(near, near, send, recv, peer + core, r), copy(far, near, send, recv, peer + other, r)

    def partner_copies(it):
        near, far = shards(near_bands[it], c), shards(far_bands[it], c)
        return (
            copy(far, near, band_send.at[it], near_recv.at[it, chip], partner, r),
            copy(near, far, pass_send.at[it], far_recv.at[it], partner, r),
        )

    def band_pass(it, peer):
        at = peer * CORES
        return copy(
            shards(near_bands[it], at, CORES),
            shards(far_bands[it], at, CORES),
            pass_send.at[it],
            far_recv.at[it],
            partner,
            r,
        )

    def to_rows(send):
        for d in range(rows - 1, 0, -1):

            @pl.when(r + d < rows)
            def _():
                send(r + d)

            @pl.when(r >= d)
            def _():
                send(r - d)

    def window_copy(it, peer):
        return copy(
            shards(near_bands[it], 0),
            shards(near_windows[it], r),
            win_send.at[it],
            win_recv.at[it, r],
            c,
            peer,
        )

    def window_pass(it, at):
        return copy(
            shards(near_windows[it], at),
            shards(far_windows[it], at),
            win_pass.at[it],
            win_far.at[it],
            partner,
            r,
        )

    def send_window(it):
        to_rows(lambda peer: window_copy(it, peer).start())


    def mix_copy(it, h):
        return copy(
            mix_out.at[it, h], mix_in.at[it, h], mix_send.at[it], mix_recv.at[it, h], partner, r
        )

    def zone_copy(it, h, peer):
        return copy(
            zone_out.at[it, h, peer],
            zone_in.at[it, h, r],
            zone_send.at[it],
            zone_recv.at[it, h],
            c,
            peer,
        )

    def total_copy(it, h):
        return copy(
            total_out.at[it, h],
            total_in.at[it, h, c],
            total_send.at[it],
            total_recv.at[it, h],
            0,
            r,
        )


    def pair_copy(it, h):
        return copy(
            pair_out.at[it, h],
            pair_in.at[it, h],
            pair_send.at[it],
            pair_recv.at[it, h],
            partner,
            r,
        )

    def row_copy(it, h, k):
        peer = peer_chip(k)
        return copy(
            row_out.at[it, h, peer],
            row_in.at[it, h, chip],
            row_send.at[it],
            row_recv.at[it, h],
            peer * CORES + core,
            r,
        )

    def prepare_volume():
        line = lax.div(surf_ref[r * lines + q], rows)
        for side_of, edge_of_tile in ((0, first_of_tile), (1, last_of_tile)):
            to = pl.ds(0 if side_of == 0 else LANES + shard, LANES)
            at = m * shard - LANES if side_of == 0 else m * shard + shard
            at = pl.multiple_of(jnp.clip(at, 0, nodes - LANES), LANES)
            receives = halo_receives[side_of]

            @pl.when(jnp.logical_not(edge_of_tile))
            def _():
                index_ext[:, to] = index_ref[line, :, pl.ds(at, LANES)]
                source_ext[:, to] = source_ref[line, :, pl.ds(at, LANES)]

            @pl.when(receives)
            def _():
                settle(halo_source, halo_recv.at[side_of])
                index_ext[:, to] = halo_index[side_of, line]
                source_ext[:, to] = halo_source[side_of, line]

            @pl.when(edge_of_tile & jnp.logical_not(receives))
            def _():
                index_ext[:, to] = jnp.full((layers, LANES), levels, I32)
                source_ext[:, to] = jnp.zeros((layers, LANES), F32)

        at = pl.multiple_of(m * shard, LANES)
        index_ext[:, LANES : LANES + shard] = index_ref[line, :, pl.ds(at, shard)]
        source_ext[:, LANES : LANES + shard] = source_ref[line, :, pl.ds(at, shard)]
        indices = index_ext[...]
        coefs = jnp.zeros((layers, span), F32)
        for level in range(levels):
            coefs = jnp.where(indices == level, table_ref[level], coefs)
        coef_ext[...] = coefs
        inside = index_ext[0:1, :] < levels
        for layer in range(layers):
            k = coef_ext[layer : layer + 1, :]
            left = 0.5 * (k + pltpu.roll(k, 1, 1))
            right = 0.5 * (k + pltpu.roll(k, span - 1, 1))
            up = 0.5 * (k + coef_ext[layer - 1 : layer, :]) if layer else k
            diagonal = left + right + up + CELL_MASS
            parts = [left, right, up]
            if layer < layers - 1:
                down = 0.5 * (k + coef_ext[layer + 1 : layer + 2, :])
                diagonal = diagonal + down
                parts.append(down)
            else:
                parts.append(None)
            parts.append(source_ext[layer : layer + 1, :])
            scale = jnp.where(inside, JACOBI_WEIGHT / diagonal, 0.0)
            for kind, part in enumerate(parts):
                if part is not None:
                    weights[kind, layer] = jnp.broadcast_to(part * scale, (SUB, span))

    def relax(now, g, first):
        at = pl.ds(g * SUB, SUB)
        for layer in range(layers):
            value = weights[4, layer]
            if first:
                if layer == 0:
                    value = value + weights[2, layer] * top[at, :]
            else:
                centre = state[now, layer, at, :]
                value = value + (1.0 - JACOBI_WEIGHT) * centre
                value = value + weights[0, layer] * pltpu.roll(centre, 1, 1)
                value = value + weights[1, layer] * pltpu.roll(centre, span - 1, 1)
                above = state[now, layer - 1, at, :] if layer else top[at, :]
                value = value + weights[2, layer] * above
                if layer < layers - 1:
                    value = value + weights[3, layer] * state[now, layer + 1, at, :]
            state[1 - now, layer, at, :] = value

    def gather_top(it):
        line = lax.div(surf_ref[r * lines + q], rows)
        for side_of, edge_of_tile in ((0, first_of_tile), (1, last_of_tile)):
            dst = (edge_left, edge_right)[side_of]
            to = slice(0, LANES) if side_of == 0 else slice(LANES + shard, span)
            base = row_down if side_of == 0 else row_up
            place = 0
            for z in range(lines):
                place = jnp.where(surf_ref[base * lines + z] == line * rows + base, z, place)
            receives = halo_receives[side_of]

            @pl.when(jnp.logical_not(edge_of_tile))
            def _():
                settle(dst.at[it, lines], edge_recv.at[it, side_of])
                top[:, to] = dst[it, lines].astype(F32)

            @pl.when(receives)
            def _():
                settle(dst.at[it, pl.ds(0, lines)], edge_recv.at[it, side_of])
                value = dst[it, 0]
                for z in range(1, lines):
                    value = jnp.where(place == z, dst[it, z], value)
                top[:, to] = value.astype(F32)

            @pl.when(edge_of_tile & jnp.logical_not(receives))
            def _():
                top[:, to] = jnp.zeros((rhs, LANES), F32)

    def relax_groups(it, begin, end):
        def rows_of(g, _):
            for i in range(SWEEPS):
                relax(i % 2, g, it == 0 and i == 0)
            at = pl.ds(g * SUB, SUB)
            k = jnp.broadcast_to(coef_ext[0:1, LANES : LANES + shard], (SUB, shard))
            flux[at, :] = k * (
                top[at, LANES : LANES + shard]
                - state[SWEEPS % 2, 0, at, LANES : LANES + shard]
            )
            return 0

        lax.fori_loop(begin, end, rows_of, 0)

    def lanes_of(h):
        return slice(h * wide, (h + 1) * wide)

    def segments(which, traces_of, part, h=None):
        at = slice(None) if h is None else lanes_of(h)
        part = pl.ds(pl.multiple_of(part * wide, wide), wide)
        acc = jnp.zeros((rhs, tile if h is None else wide), F32)
        for k in range(slots):
            s = order[4 * which, k]
            traces = traces_of[order[4 * which + 1, k]]
            keep = order[4 * which + 2, k].astype(F32)
            if which == 0:
                term = jnp.dot(traces, panel[s, part, at], preferred_element_type=F32)
            elif turns == slots or k < turns:
                block = turned[s if turns == slots else k, part, at]
                term = jnp.dot(traces, block, preferred_element_type=F32)
            else:
                block = panel[s, at, part]
                contract = (((1,), (1,)), ((), ()))
                term = lax.dot_general(traces, block, contract, preferred_element_type=F32)
            acc = acc * keep + term
            product[k, :, at] = acc if h is None else product[k, :, at] + acc

    def last_of(which, h, at):
        return product[order[4 * which + 3, at], :, lanes_of(h)]

    def send_mix(it, h):
        for z in range(rows):
            for p in range(half):
                value = last_of(0, h, z * per_shard + other * half + p)
                mix_out[it, h, z, p] = value.astype(BF16)
                zone_own[h, z, p] = last_of(0, h, z * per_shard + core * half + p)
        mix_copy(it, h).start()

    def send_zone(it, h):
        settle(mix_in.at[it, h], mix_recv.at[it, h])
        for z in range(rows):
            for p in range(half):
                value = zone_own[h, z, p] + mix_in[it, h, z, p].astype(F32)
                zone_own[h, z, p] = value
                zone_out[it, h, z, p] = value.astype(BF16)
        to_rows(lambda peer: zone_copy(it, h, peer).start())

    def send_pair(it, h):
        for k in range(chips):
            for p in range(per_shard):
                value = last_of(1, h, (k * CORES + other) * per_shard + p)
                pair_out[it, h, k, p] = value.astype(BF16)
                row_own[h, k, p] = last_of(1, h, (k * CORES + core) * per_shard + p)
        pair_copy(it, h).start()

    def send_rows(it, h):
        settle(pair_in.at[it, h], pair_recv.at[it, h])
        for k in range(chips):
            for p in range(per_shard):
                value = row_own[h, k, p] + pair_in[it, h, k, p].astype(F32)
                row_own[h, k, p] = value
                row_out[it, h, k, p] = value.astype(BF16)
        for k in near_first if h == 0 and it < ITERS - 1 else beside:
            row_copy(it, h, k).start()

    def wait_panel():
        for i in range(len(stops) - 1):
            panel_copy(i).wait()


    def turn(i):
        begin, end = min(stops[i], turns), min(stops[i + 1], turns)
        if turns == slots:
            panel_copy(i).wait()

        def one(k):
            turned[k] = panel[k if turns == slots else order[4, k]].T

        def two(j, _):
            one(begin + 2 * j)
            one(begin + 2 * j + 1)
            return 0

        lax.fori_loop(0, (end - begin) // 2, two, 0)
        if (end - begin) % 2:
            one(end - 1)

    def begin():
        input_copy(1).wait()
        input_copy(2).wait()
        for side_of in range(2):

            @pl.when(halo_sends[side_of])
            def _():
                for kind in range(2):
                    halo_copy(kind, side_of).start()

        input_copy(4).wait()
        input_copy(5).wait()
        input_copy(6).wait()

        @pl.when(is_dense)
        def _():
            sort_slots()
            pltpu.make_async_copy(tab, order, tab_sem).start()
            product[slots] = jnp.zeros((rhs, tile), F32)

    def send_total(it, h):
        settle(zone_in.at[it, h, pl.ds(0, rows - 1)], zone_recv.at[it, h])
        for p in range(half):
            value = zone_own[h, r, p]
            for k in range(1, rows):
                value = value + zone_in[it, h, lax.rem(r + k, rows), p].astype(F32)
            total_own[h, p] = value
            total_out[it, h, p] = value.astype(BF16)

        @pl.when(c != 0)
        def _():
            total_copy(it, h).start()

    def dense_part(it):
        near_band, far_band = near_bands[it], far_bands[it]
        near_window, far_window = near_windows[it], far_windows[it]
        if it == 0:
            if turns < slots:
                pltpu.make_async_copy(tab, order, tab_sem).wait()
                wait_panel()
            for i in range(len(stops) - 2):
                turn(i)
            prepare_volume()
        settle(shards(near_band, partner), near_recv.at[it, chip])

        @pl.when(c == 1)
        def _():
            send_window(it)

        def pass_on(peer):
            settle(shards(near_band, peer * CORES, CORES), near_recv.at[it, peer])
            band_pass(it, peer).start()

        @pl.when(chip != 0)
        def _():
            settle(shards(near_band, 0, CORES), near_recv.at[it, 0])
            send_window(it)
            band_pass(it, 0).start()

        if it == 0:
            turn(len(stops) - 2)
        for k in near_first:
            peer = peer_chip(k)

            @pl.when(peer != 0)
            def _():
                pass_on(peer)

        if it == 0 and turns == slots:
            pltpu.make_async_copy(tab, order, tab_sem).wait()
        segments(0, near_band, core)
        settle(shards(far_band, 0, cols - 1), far_recv.at[it])
        near_window[pl.ds(r * per_shard, per_shard)] = near_band[0:per_shard]
        far_window[pl.ds(r * per_shard, per_shard)] = far_band[0:per_shard]
        segments(0, far_band, other, 0)
        send_mix(it, 0)
        segments(0, far_band, other, 1)
        send_mix(it, 1)
        send_zone(it, 0)
        if it > 0:
            send_zone(it, 1)
        for k in range(1, rows):
            at = lax.rem(r + k, rows)
            settle(shards(near_window, at), win_recv.at[it, at])
            window_pass(it, at).start()
        segments(1, near_window, core)
        if it == 0:
            send_zone(it, 1)
        settle(shards(far_window, 0, rows - 1), win_far.at[it])
        segments(1, far_window, other, 0)
        send_pair(it, 0)
        segments(1, far_window, other, 1)
        send_pair(it, 1)
        groups = rhs // SUB
        gather_top(it)
        relax_groups(it, 0, groups // 4)
        send_rows(it, 0)
        relax_groups(it, groups // 4, groups // 2)
        send_rows(it, 1)
        for h in range(2):
            send_total(it, h)
        for h in range(0 if it == ITERS - 1 else 1, 2):
            for k in beyond:
                row_copy(it, h, k).start()
        relax_groups(it, groups // 2, groups)

    def drain(it):
        for side_of, near, far in (
            (0, jnp.logical_not(last_of_tile), cross_right),
            (1, jnp.logical_not(first_of_tile), cross_left),
        ):

            @pl.when(near)
            def _():
                settle_send(edge_left.at[it, 0], edge_send.at[it, side_of])

            @pl.when(far)
            def _():
                settle_send(edge_left.at[it, pl.ds(0, lines)], edge_send.at[it, side_of])

        if it == 0:
            for side_of in range(2):

                @pl.when(halo_sends[side_of])
                def _():
                    settle_send(halo_source, halo_send.at[side_of])

        @pl.when(jnp.logical_not(is_dense))
        def _():
            settle_send(shards(near_bands[it], 0, dense_chips * CORES), band_send.at[it])

        @pl.when(is_dense)
        def _():
            settle_send(shards(near_bands[it], 0, (dense_chips - 1) * CORES + 1), band_send.at[it])
            settle_send(shards(near_bands[it], 0, cols - 1), pass_send.at[it])
            settle_send(shards(near_windows[it], 0, rows - 1), win_send.at[it])
            settle_send(shards(near_windows[it], 0, rows - 1), win_pass.at[it])
            settle_send(mix_out.at[it], mix_send.at[it])
            settle_send(zone_out.at[it, :, pl.ds(0, rows - 1)], zone_send.at[it])
            settle_send(pair_out.at[it], pair_send.at[it])
            settle_send(row_out.at[it, :, pl.ds(0, chips - 1)], row_send.at[it])

            @pl.when(c != 0)
            def _():
                settle_send(total_out.at[it], total_send.at[it])

    def own(h, p):
        return slice(p * tile + h * wide, p * tile + (h + 1) * wide)

    def round_half(it, h):
        for p in range(per_shard):
            rounded = traces_ref[:, own(h, p)].astype(BF16)

            @pl.when(core == h)
            def _():
                near_bands[it][c * per_shard + p] = rounded

            @pl.when(core != h)
            def _():
                far_bands[it][c * per_shard + p] = rounded

            at = LANES + p * tile + h * wide
            top[:, at : at + wide] = rounded.astype(F32)
            if h == 1 and p == per_shard - 1:
                edge_out[it, 0] = rounded[:, wide - LANES :]
            if h == 0 and p == 0:
                edge_out[it, 1] = rounded[:, :LANES]

    def send_half(it, h):
        side_of = 1 - h
        inner, outer = ((last_of_tile, cross_right), (first_of_tile, cross_left))[side_of]

        @pl.when(jnp.logical_not(inner))
        def _():
            edge_near(it, side_of).start()

        @pl.when(outer)
        def _():
            for z in range(lines):
                edge_far(it, side_of, z).start()

        for k in near_first:
            same, cross = band_copies(it, k)

            @pl.when((peer_chip(k) < dense_chips) & (core == h))
            def _():
                same.start()

            @pl.when((peer_chip(k) < dense_chips) & (core != h))
            def _():
                cross.start()

        to_near, to_far = partner_copies(it)

        @pl.when(is_dense & (core == h))
        def _():
            to_far.start()

        @pl.when(is_dense & (core != h))
        def _():
            to_near.start()

        if h == 0:

            @pl.when(c == 0)
            def _():
                send_window(it)

    def finish_half(it, h):
        @pl.when(is_dense)
        def _():
            for p in range(per_shard):
                product_ref[:, own(h, p)] = row_own[h, chip, p]
            settle(row_in.at[it, h, pl.ds(0, dense_chips - 1)], row_recv.at[it, h])

        @pl.when(jnp.logical_not(is_dense))
        def _():
            for p in range(per_shard):
                product_ref[:, own(h, p)] = jnp.zeros((rhs, wide), F32)
            settle(row_in.at[it, h, pl.ds(0, dense_chips)], row_recv.at[it, h])

        for src in range(dense_chips):

            @pl.when(src != chip)
            def _():
                for p in range(per_shard):
                    product_ref[:, own(h, p)] += row_in[it, h, src, p].astype(F32)

        @pl.when(c == 0)
        def _():
            settle(total_in.at[it, h, pl.ds(0, dense - 1)], total_recv.at[it, h])
            for p in range(half):
                product_ref[:, own(h, p)] += total_own[h, p]
            for src in range(1, dense):
                for p in range(half):
                    at = own(h, (src % CORES) * half + p)
                    product_ref[:, at] += total_in[it, h, src, p].astype(F32)

    for h in range(2):
        round_half(0, h)
    pl.semaphore_wait(barrier, expected)
    for h in range(2):
        send_half(0, h)
    begin()
    for it in range(ITERS):

        @pl.when(is_dense)
        def _():
            dense_part(it)

        @pl.when(jnp.logical_not(is_dense))
        def _():
            if it == 0:
                prepare_volume()
            gather_top(it)
            relax_groups(it, 0, rhs // SUB)

        if it == 0:
            input_copy(3).wait()
        middle_ref[...] = traces_ref[...] + COUPLING_STEP * (load_ref[...] - traces_ref[...])
        if it == ITERS - 1:
            output_copy(0).start()
            output_copy(2).start()
            for done in range(ITERS):
                drain(done)
        for h in range(2):
            finish_half(it, h)
            if it < ITERS - 1:
                for p in range(per_shard):
                    at = own(h, p)
                    change = COUPLING_STEP * (product_ref[:, at] + flux[:, at])
                    traces_ref[:, at] = middle_ref[:, at] - change
                round_half(it + 1, h)
                send_half(it + 1, h)

    output_copy(1).start()
    for i in range(len(outputs)):
        output_copy(i).wait()


def local(
    trace_start, surface_load, panel_tiles, tile_list, surf_map, coef_index, coef_table, vol_source
):
    cols = lax.axis_size("col")
    rows = lax.axis_size("row")
    lines, layers, nodes = coef_index.shape
    slots, tile, _ = panel_tiles.shape
    rhs, shard = trace_start.shape
    per_shard = shard // tile
    levels = coef_table.shape[0]
    half = per_shard // CORES
    chips = cols // CORES
    span = shard + 2 * LANES
    turns = min(slots, TURNED_BYTES // (2 * tile * tile) - slots)
    cfg = (cols, rows, lines, per_shard, tile, slots, nodes, layers, rhs, levels, turns)
    hbm = pl.BlockSpec(memory_space=pl.ANY)
    block = (rhs, tile)
    piece = (rhs, tile // 2)
    dma = pltpu.SemaphoreType.DMA
    out = jax.ShapeDtypeStruct((rhs, shard), F32)
    middle, product, flux = pl.pallas_call(
        functools.partial(kernel, cfg),
        out_shape=(out,) * 3,
        in_specs=[hbm] * 8,
        out_specs=(hbm,) * 3,
        scratch_shapes=[
            pltpu.VMEM((rhs, shard), F32),
            pltpu.VMEM((rhs, shard), F32),
            pltpu.VMEM((rhs, shard), F32),
            pltpu.SMEM(tile_list.shape, I32),
            pltpu.SMEM(surf_map.shape, I32),
            pltpu.SMEM(coef_table.shape, F32),
            pltpu.VMEM((slots, tile, tile), BF16),
            pltpu.VMEM((turns, tile, tile), BF16),
            pltpu.VMEM((rhs, shard), F32),
            pltpu.VMEM((rhs, shard), F32),
            pltpu.VMEM((lines, layers, nodes), I32),
            pltpu.VMEM((lines, layers, nodes), F32),
            pltpu.VMEM((SUB, LANES), I32),
            pltpu.SMEM((SUB, LANES), I32),
            pltpu.VMEM((cols * per_shard,) + piece, BF16),
            pltpu.VMEM((cols * per_shard,) + piece, BF16),
            pltpu.VMEM((cols * per_shard,) + piece, BF16),
            pltpu.VMEM((cols * per_shard,) + piece, BF16),
            pltpu.VMEM((rows * per_shard,) + piece, BF16),
            pltpu.VMEM((rows * per_shard,) + piece, BF16),
            pltpu.VMEM((rows * per_shard,) + piece, BF16),
            pltpu.VMEM((rows * per_shard,) + piece, BF16),
            pltpu.VMEM((ITERS, 2, rhs, LANES), BF16),
            pltpu.VMEM((ITERS, lines + 1, rhs, LANES), BF16),
            pltpu.VMEM((ITERS, lines + 1, rhs, LANES), BF16),
            pltpu.VMEM((2, lines, layers, LANES), I32),
            pltpu.VMEM((2, lines, layers, LANES), F32),
            pltpu.VMEM((slots + 1,) + block, F32),
            pltpu.VMEM((ITERS, 2, rows, half) + piece, BF16),
            pltpu.VMEM((ITERS, 2, rows, half) + piece, BF16),
            pltpu.VMEM((2, rows, half) + piece, F32),
            pltpu.VMEM((ITERS, 2, rows, half) + piece, BF16),
            pltpu.VMEM((ITERS, 2, rows, half) + piece, BF16),
            pltpu.VMEM((2, half) + piece, F32),
            pltpu.VMEM((ITERS, 2, half) + piece, BF16),
            pltpu.VMEM((ITERS, 2, cols, half) + piece, BF16),
            pltpu.VMEM((ITERS, 2, chips, per_shard) + piece, BF16),
            pltpu.VMEM((ITERS, 2, chips, per_shard) + piece, BF16),
            pltpu.VMEM((2, chips, per_shard) + piece, F32),
            pltpu.VMEM((ITERS, 2, chips, per_shard) + piece, BF16),
            pltpu.VMEM((ITERS, 2, chips, per_shard) + piece, BF16),
            pltpu.VMEM((layers, span), I32),
            pltpu.VMEM((layers, span), F32),
            pltpu.VMEM((layers, span), F32),
            pltpu.VMEM((5, layers, SUB, span), F32),
            pltpu.VMEM((2, layers, rhs, span), F32),
            pltpu.VMEM((rhs, span), F32),
            dma((3,)),
            dma((7,)),
            dma((3,)),
            dma,
            dma((ITERS,)),
            dma((ITERS,)),
            dma((ITERS, chips)),
            dma((ITERS,)),
            dma((ITERS,)),
            dma((ITERS,)),
            dma((ITERS, rows)),
            dma((ITERS,)),
            dma((ITERS, 2)),
            dma((ITERS, 2)),
            dma((2,)),
            dma((2,)),
            dma((ITERS,)),
            dma((ITERS, 2)),
            dma((ITERS,)),
            dma((ITERS, 2)),
            dma((ITERS,)),
            dma((ITERS, 2)),
            dma((ITERS,)),
            dma((ITERS, 2)),
            dma((ITERS,)),
            dma((ITERS, 2)),
        ],
        compiler_params=pltpu.CompilerParams(
            collective_id=0, has_side_effects=True, vmem_limit_bytes=60 * 1024 * 1024
        ),
        name="coupled",
    )(
        tile_list,
        surf_map,
        coef_table,
        trace_start,
        surface_load,
        coef_index,
        vol_source,
        panel_tiles,
    )
    response = product + flux
    return middle - COUPLING_STEP * response, response


def solution(mesh):
    return jax.shard_map(
        local,
        mesh=mesh,
        in_specs=(
            P(None, ("col", "row")),
            P(None, ("col", "row")),
            P(("col", "row"), None, None),
            P(("col", "row")),
            P(),
            P(None, None, "row"),
            P(),
            P(None, None, "row"),
        ),
        out_specs=(P(None, ("col", "row")), P(None, ("col", "row"))),
        check_vma=False,
    )
```

```python
import functools

import jax
import jax.numpy as jnp
from jax import lax
from jax.experimental import pallas as pl
from jax.experimental.pallas import tpu as pltpu
from jax.sharding import PartitionSpec as P

ITERS = 2
SWEEPS = 4

COUPLING_STEP = 0.3
JACOBI_WEIGHT = 0.8
CELL_MASS = 0.05

LANES = 128
SUB = 8
CORES = 2
TURNED_BYTES = 36 * 1024 * 1024
F32 = jnp.float32
BF16 = jnp.bfloat16
I32 = jnp.int32


def quotient(x, n):
    return x >> (n.bit_length() - 1) if n & (n - 1) == 0 else lax.div(x, n)


def remainder(x, n):
    return x & (n - 1) if n & (n - 1) == 0 else lax.rem(x, n)


def kernel(
    cfg,
    list_hbm,
    surf_hbm,
    table_hbm,
    start_hbm,
    load_hbm,
    index_hbm,
    source_hbm,
    panel_hbm,
    middle_hbm,
    product_hbm,
    flux_hbm,
    middle_ref,
    product_ref,
    flux,
    list_ref,
    surf_ref,
    table_ref,
    panel,
    turned,
    traces_ref,
    load_ref,
    index_ref,
    source_ref,
    tab,
    order,
    near_band0,
    near_band1,
    far_band0,
    far_band1,
    near_window0,
    near_window1,
    far_window0,
    far_window1,
    edge_out,
    edge_left,
    edge_right,
    halo_index,
    halo_source,
    product,
    mix_out,
    mix_in,
    zone_own,
    zone_out,
    zone_in,
    total_own,
    total_out,
    total_in,
    pair_out,
    pair_in,
    row_own,
    row_out,
    row_in,
    index_ext,
    coef_ext,
    source_ext,
    weights,
    state,
    top,
    panel_sem,
    input_sem,
    output_sem,
    tab_sem,
    band_send,
    pass_send,
    near_recv,
    far_recv,
    win_send,
    win_recv,
    win_far,
    edge_send,
    edge_recv,
    halo_send,
    halo_recv,
    mix_send,
    mix_recv,
    zone_send,
    zone_recv,
    total_send,
    total_recv,
    pair_send,
    pair_recv,
    row_send,
    row_recv,
):
    cols, rows, lines, per_shard, tile, slots, nodes, layers, rhs, levels, turns = cfg
    dense = cols - lines
    group = cols // lines
    shard = per_shard * tile
    half = per_shard // CORES
    chips = cols // CORES
    dense_chips = dense // CORES
    win_tiles = rows * per_shard
    band_tiles = cols * per_shard
    side = cols * rows * per_shard
    span = shard + 2 * LANES
    wide = tile // 2
    near_bands = (near_band0, near_band1)
    far_bands = (far_band0, far_band1)
    near_windows = (near_window0, near_window1)
    far_windows = (far_window0, far_window1)
    c = lax.axis_index("col")
    r = lax.axis_index("row")
    core = lax.rem(c, CORES)
    chip = lax.div(c, CORES)
    other = 1 - core
    partner = chip * CORES + other
    q = lax.div(c, group)
    m = lax.rem(c, group)
    is_dense = c < dense
    row_up = jnp.minimum(r + 1, rows - 1)
    row_down = jnp.maximum(r - 1, 0)
    first_of_tile = m == 0
    last_of_tile = m == group - 1
    cross_left = first_of_tile & (r > 0)
    cross_right = last_of_tile & (r < rows - 1)

    def copy(src, dst, send, recv, to_col, to_row):
        return pltpu.make_async_remote_copy(
            src_ref=src,
            dst_ref=dst,
            send_sem=send,
            recv_sem=recv,
            device_id=(to_col, to_row),
            device_id_type=pl.DeviceIdType.MESH,
        )

    stops = sorted({0, slots * 3 // 8, slots * 3 // 4, slots})

    def panel_copy(i):
        part = pl.ds(stops[i], stops[i + 1] - stops[i])
        return pltpu.make_async_copy(panel_hbm.at[part], panel.at[part], panel_sem.at[i])

    inputs = (
        (start_hbm, traces_ref),
        (index_hbm, index_ref),
        (source_hbm, source_ref),
        (load_hbm, load_ref),
        (list_hbm, list_ref),
        (surf_hbm, surf_ref),
        (table_hbm, table_ref),
    )

    def input_copy(i):
        return pltpu.make_async_copy(inputs[i][0], inputs[i][1], input_sem.at[i])

    outputs = ((middle_ref, middle_hbm), (product_ref, product_hbm), (flux, flux_hbm))

    def output_copy(i):
        return pltpu.make_async_copy(outputs[i][0], outputs[i][1], output_sem.at[i])

    barrier = pltpu.get_barrier_semaphore()

    def greet(to_col, to_row):
        pl.semaphore_signal(
            barrier, inc=1, device_id=(to_col, to_row), device_id_type=pl.DeviceIdType.MESH
        )

    input_copy(0).start()
    for k in range(1, rows):
        greet(c, lax.rem(r + k, rows))
    for k in range(1, cols):
        greet(lax.rem(c + k, cols), r)

    @pl.when(cross_right)
    def _():
        for z in range(lines):
            greet(z * group, row_up)

    @pl.when(cross_left)
    def _():
        for z in range(lines):
            greet(z * group + group - 1, row_down)

    for i in (1, 2, 4, 5, 6, 3):
        input_copy(i).start()

    @pl.when(is_dense)
    def _():
        for i in range(len(stops) - 1):
            panel_copy(i).start()


    padded_slots = -(-slots // SUB) * SUB
    lane = lax.broadcasted_iota(I32, (SUB, LANES), 1)

    def sort_slots():
        slot = lax.broadcasted_iota(I32, (padded_slots, LANES), 0)
        lanes = lax.broadcasted_iota(I32, (padded_slots, LANES), 1)
        row_key = jnp.full((padded_slots, LANES), band_tiles, I32)
        col_key = jnp.full((padded_slots, LANES), win_tiles, I32)
        keys = []
        for s in range(slots):
            name = list_ref[s]
            safe = jnp.maximum(name, 0)
            row = quotient(safe, side)
            row = quotient(quotient(row, per_shard), rows) * per_shard + remainder(row, per_shard)
            row = jnp.where(name >= 0, row, band_tiles)
            col = jnp.where(name >= 0, remainder(safe, side), win_tiles)
            keys.append((col, row))
            row_key = jnp.where(slot == s, row, row_key)
            col_key = jnp.where(slot == s, col, col_key)

        def fold(x):
            x = functools.reduce(jnp.add, [x[i : i + SUB] for i in range(0, padded_slots, SUB)])
            for shift in (4, 2, 1):
                x = x + pltpu.roll(x, shift, 0)
            return x

        for which, key, source, count in (
            (0, col_key, row_key, win_tiles),
            (1, row_key, col_key, band_tiles),
        ):
            rank = jnp.zeros((padded_slots, LANES), I32)
            upto = jnp.zeros((SUB, LANES), I32)
            equal = jnp.zeros((SUB, LANES), I32)
            for s in range(slots):
                value = keys[s][which]
                ahead = (key > value) | ((key == value) & (slot > s))
                rank = rank + jnp.where(ahead, 1, 0)
                upto = upto + jnp.where(lane >= value, 1, 0)
                equal = equal + jnp.where(lane == value, 1, 0)
            rank = jnp.where(slot < slots, rank, LANES)
            here = rank == lanes
            place = fold(jnp.where(here, slot, 0))
            origin = fold(jnp.where(here, jnp.where(key < count, source, 0), 0))
            value = fold(jnp.where(here, key, 0))
            keep = (value == pltpu.roll(value, 1, 1)) & (lane > 0)
            last = jnp.where(equal > 0, upto - 1, slots)
            for i, x in enumerate((place, origin, jnp.where(keep, 1, 0), last)):
                tab[4 * which + i : 4 * which + i + 1, :] = x[0:1, :]

    input_copy(0).wait()
    expected = (
        cols - 1 + rows - 1 + jnp.where(cross_right, lines, 0) + jnp.where(cross_left, lines, 0)
    )

    def settle(ref, sem):
        copy(ref, ref, sem, sem, partner, r).wait_recv()

    def settle_send(ref, sem):
        copy(ref, ref, sem, sem, partner, r).wait_send()


    def halo_copy(kind, side_of, arrival=False):
        ref = (index_ref, source_ref)[kind]
        dst = (halo_index, halo_source)[kind]
        at = nodes - LANES if side_of == 0 else 0
        to = row_up if (side_of == 0) != arrival else row_down
        return copy(
            ref.at[:, :, pl.ds(at, LANES)],
            dst.at[side_of],
            halo_send.at[side_of],
            halo_recv.at[side_of],
            c,
            to,
        )

    halo_sends = (first_of_tile & (r < rows - 1), last_of_tile & (r > 0))
    halo_receives = (cross_left, cross_right)


    def edge_near(it, side_of):
        dst = (edge_left, edge_right)[side_of]
        return copy(
            edge_out.at[it, side_of],
            dst.at[it, lines],
            edge_send.at[it, side_of],
            edge_recv.at[it, side_of],
            c + 1 if side_of == 0 else c - 1,
            r,
        )

    def edge_far(it, side_of, z):
        dst = (edge_left, edge_right)[side_of]
        to = (z * group, row_up) if side_of == 0 else (z * group + group - 1, row_down)
        return copy(
            edge_out.at[it, side_of],
            dst.at[it, q],
            edge_send.at[it, side_of],
            edge_recv.at[it, side_of],
            *to,
        )


    def shards(ref, col, count=1):
        return ref.at[pl.ds(col * per_shard, count * per_shard)]

    bits = chips.bit_length() - 1
    power = chips == 1 << bits
    near_first = sorted(range(1, chips), key=lambda k: k.bit_count() if power else k)
    beside = [k for k in near_first if power and k.bit_count() == 1]
    beyond = [k for k in near_first if k not in beside]

    def peer_chip(k):
        if not power:
            return lax.rem(chip + k, chips)
        digits = [remainder(quotient(chip, 1 << b), 2) for b in range(bits)]
        return sum((1 - d if k >> b & 1 else d) * (1 << b) for b, d in enumerate(digits))

    def band_copies(it, k):
        peer = peer_chip(k) * CORES
        send, recv = band_send.at[it], near_recv.at[it, chip]
        near, far = shards(near_bands[it], c), shards(far_bands[it], c)
        return copy(near, near, send, recv, peer + core, r), copy(far, near, send, recv, peer + other, r)

    def partner_copies(it):
        near, far = shards(near_bands[it], c), shards(far_bands[it], c)
        return (
            copy(far, near, band_send.at[it], near_recv.at[it, chip], partner, r),
            copy(near, far, pass_send.at[it], far_recv.at[it], partner, r),
        )

    def band_pass(it, peer):
        at = peer * CORES
        return copy(
            shards(near_bands[it], at, CORES),
            shards(far_bands[it], at, CORES),
            pass_send.at[it],
            far_recv.at[it],
            partner,
            r,
        )

    def to_rows(send):
        for d in range(rows - 1, 0, -1):

            @pl.when(r + d < rows)
            def _():
                send(r + d)

            @pl.when(r >= d)
            def _():
                send(r - d)

    def window_copy(it, peer):
        return copy(
            shards(near_bands[it], 0),
            shards(near_windows[it], r),
            win_send.at[it],
            win_recv.at[it],
            c,
            peer,
        )

    def window_pass(it, at):
        return copy(
            shards(near_windows[it], at),
            shards(far_windows[it], at),
            win_send.at[it],
            win_far.at[it],
            partner,
            r,
        )

    def send_window(it):
        to_rows(lambda peer: window_copy(it, peer).start())


    def mix_copy(it, h):
        return copy(
            mix_out.at[it, h], mix_in.at[it, h], mix_send.at[it], mix_recv.at[it, h], partner, r
        )

    def zone_copy(it, h, peer):
        return copy(
            zone_out.at[it, h, peer],
            zone_in.at[it, h, r],
            zone_send.at[it],
            zone_recv.at[it, h],
            c,
            peer,
        )

    def total_copy(it, h):
        return copy(
            total_out.at[it, h],
            total_in.at[it, h, c],
            total_send.at[it],
            total_recv.at[it, h],
            0,
            r,
        )


    def pair_copy(it, h):
        return copy(
            pair_out.at[it, h],
            pair_in.at[it, h],
            pair_send.at[it],
            pair_recv.at[it, h],
            partner,
            r,
        )

    def row_copy(it, h, k):
        peer = peer_chip(k)
        return copy(
            row_out.at[it, h, peer],
            row_in.at[it, h, chip],
            row_send.at[it],
            row_recv.at[it, h],
            peer * CORES + core,
            r,
        )

    def prepare_volume():
        line = lax.div(surf_ref[r * lines + q], rows)
        for side_of, edge_of_tile in ((0, first_of_tile), (1, last_of_tile)):
            to = pl.ds(0 if side_of == 0 else LANES + shard, LANES)
            at = m * shard - LANES if side_of == 0 else m * shard + shard
            at = pl.multiple_of(jnp.clip(at, 0, nodes - LANES), LANES)
            receives = halo_receives[side_of]

            @pl.when(jnp.logical_not(edge_of_tile))
            def _():
                index_ext[:, to] = index_ref[line, :, pl.ds(at, LANES)]
                source_ext[:, to] = source_ref[line, :, pl.ds(at, LANES)]

            @pl.when(receives)
            def _():
                settle(halo_source, halo_recv.at[side_of])
                index_ext[:, to] = halo_index[side_of, line]
                source_ext[:, to] = halo_source[side_of, line]

            @pl.when(edge_of_tile & jnp.logical_not(receives))
            def _():
                index_ext[:, to] = jnp.full((layers, LANES), levels, I32)
                source_ext[:, to] = jnp.zeros((layers, LANES), F32)

        at = pl.multiple_of(m * shard, LANES)
        index_ext[:, LANES : LANES + shard] = index_ref[line, :, pl.ds(at, shard)]
        source_ext[:, LANES : LANES + shard] = source_ref[line, :, pl.ds(at, shard)]
        indices = index_ext[...]
        coefs = jnp.zeros((layers, span), F32)
        for level in range(levels):
            coefs = jnp.where(indices == level, table_ref[level], coefs)
        coef_ext[...] = coefs
        inside = index_ext[0:1, :] < levels
        for layer in range(layers):
            k = coef_ext[layer : layer + 1, :]
            left = 0.5 * (k + pltpu.roll(k, 1, 1))
            right = 0.5 * (k + pltpu.roll(k, span - 1, 1))
            up = 0.5 * (k + coef_ext[layer - 1 : layer, :]) if layer else k
            diagonal = left + right + up + CELL_MASS
            parts = [left, right, up]
            if layer < layers - 1:
                down = 0.5 * (k + coef_ext[layer + 1 : layer + 2, :])
                diagonal = diagonal + down
                parts.append(down)
            else:
                parts.append(None)
            parts.append(source_ext[layer : layer + 1, :])
            scale = jnp.where(inside, JACOBI_WEIGHT / diagonal, 0.0)
            for kind, part in enumerate(parts):
                if part is not None:
                    weights[kind, layer] = jnp.broadcast_to(part * scale, (SUB, span))

    def relax(now, g, first):
        at = pl.ds(g * SUB, SUB)
        for layer in range(layers):
            value = weights[4, layer]
            if first:
                if layer == 0:
                    value = value + weights[2, layer] * top[at, :]
            else:
                centre = state[now, layer, at, :]
                value = value + (1.0 - JACOBI_WEIGHT) * centre
                value = value + weights[0, layer] * pltpu.roll(centre, 1, 1)
                value = value + weights[1, layer] * pltpu.roll(centre, span - 1, 1)
                above = state[now, layer - 1, at, :] if layer else top[at, :]
                value = value + weights[2, layer] * above
                if layer < layers - 1:
                    value = value + weights[3, layer] * state[now, layer + 1, at, :]
            state[1 - now, layer, at, :] = value

    def gather_top(it):
        line = lax.div(surf_ref[r * lines + q], rows)
        for side_of, edge_of_tile in ((0, first_of_tile), (1, last_of_tile)):
            dst = (edge_left, edge_right)[side_of]
            to = slice(0, LANES) if side_of == 0 else slice(LANES + shard, span)
            base = row_down if side_of == 0 else row_up
            place = 0
            for z in range(lines):
                place = jnp.where(surf_ref[base * lines + z] == line * rows + base, z, place)
            receives = halo_receives[side_of]

            @pl.when(jnp.logical_not(edge_of_tile))
            def _():
                settle(dst.at[it, lines], edge_recv.at[it, side_of])
                top[:, to] = dst[it, lines].astype(F32)

            @pl.when(receives)
            def _():
                settle(dst.at[it, pl.ds(0, lines)], edge_recv.at[it, side_of])
                value = dst[it, 0]
                for z in range(1, lines):
                    value = jnp.where(place == z, dst[it, z], value)
                top[:, to] = value.astype(F32)

            @pl.when(edge_of_tile & jnp.logical_not(receives))
            def _():
                top[:, to] = jnp.zeros((rhs, LANES), F32)

    def relax_groups(it, begin, end):
        def rows_of(g, _):
            for i in range(SWEEPS):
                relax(i % 2, g, it == 0 and i == 0)
            at = pl.ds(g * SUB, SUB)
            k = jnp.broadcast_to(coef_ext[0:1, LANES : LANES + shard], (SUB, shard))
            flux[at, :] = k * (
                top[at, LANES : LANES + shard]
                - state[SWEEPS % 2, 0, at, LANES : LANES + shard]
            )
            return 0

        lax.fori_loop(begin, end, rows_of, 0)

    def lanes_of(h):
        return slice(h * wide, (h + 1) * wide)

    def segments(which, traces_of, part, h=None):
        at = slice(None) if h is None else lanes_of(h)
        part = pl.ds(pl.multiple_of(part * wide, wide), wide)
        acc = jnp.zeros((rhs, tile if h is None else wide), F32)
        for k in range(slots):
            s = order[4 * which, k]
            traces = traces_of[order[4 * which + 1, k]]
            keep = order[4 * which + 2, k].astype(F32)
            if which == 0:
                term = jnp.dot(traces, panel[s, part, at], preferred_element_type=F32)
            elif turns == slots or k < turns:
                block = turned[s if turns == slots else k, part, at]
                term = jnp.dot(traces, block, preferred_element_type=F32)
            else:
                block = panel[s, at, part]
                contract = (((1,), (1,)), ((), ()))
                term = lax.dot_general(traces, block, contract, preferred_element_type=F32)
            acc = acc * keep + term
            product[k, :, at] = acc if h is None else product[k, :, at] + acc

    def last_of(which, h, at):
        return product[order[4 * which + 3, at], :, lanes_of(h)]

    def send_mix(it, h):
        for z in range(rows):
            for p in range(half):
                value = last_of(0, h, z * per_shard + other * half + p)
                mix_out[it, h, z, p] = value.astype(BF16)
                zone_own[h, z, p] = last_of(0, h, z * per_shard + core * half + p)
        mix_copy(it, h).start()

    def send_zone(it, h):
        settle(mix_in.at[it, h], mix_recv.at[it, h])
        for z in range(rows):
            for p in range(half):
                value = zone_own[h, z, p] + mix_in[it, h, z, p].astype(F32)
                zone_own[h, z, p] = value
                zone_out[it, h, z, p] = value.astype(BF16)
        to_rows(lambda peer: zone_copy(it, h, peer).start())

    def send_pair(it, h):
        for k in range(chips):
            for p in range(per_shard):
                value = last_of(1, h, (k * CORES + other) * per_shard + p)
                pair_out[it, h, k, p] = value.astype(BF16)
                row_own[h, k, p] = last_of(1, h, (k * CORES + core) * per_shard + p)
        pair_copy(it, h).start()

    def send_rows(it, h):
        settle(pair_in.at[it, h], pair_recv.at[it, h])
        for k in range(chips):
            for p in range(per_shard):
                value = row_own[h, k, p] + pair_in[it, h, k, p].astype(F32)
                row_own[h, k, p] = value
                row_out[it, h, k, p] = value.astype(BF16)
        for k in near_first if h == 0 and it < ITERS - 1 else beside:
            row_copy(it, h, k).start()

    def wait_panel():
        for i in range(len(stops) - 1):
            panel_copy(i).wait()


    def turn(i):
        begin, end = min(stops[i], turns), min(stops[i + 1], turns)
        if turns == slots:
            panel_copy(i).wait()

        def one(k):
            turned[k] = panel[k if turns == slots else order[4, k]].T

        def two(j, _):
            one(begin + 2 * j)
            one(begin + 2 * j + 1)
            return 0

        lax.fori_loop(0, (end - begin) // 2, two, 0)
        if (end - begin) % 2:
            one(end - 1)

    def begin():
        input_copy(1).wait()
        input_copy(2).wait()
        for side_of in range(2):

            @pl.when(halo_sends[side_of])
            def _():
                for kind in range(2):
                    halo_copy(kind, side_of).start()

        input_copy(4).wait()
        input_copy(5).wait()
        input_copy(6).wait()

        @pl.when(is_dense)
        def _():
            sort_slots()
            pltpu.make_async_copy(tab, order, tab_sem).start()
            product[slots] = jnp.zeros((rhs, tile), F32)

    def send_total(it, h):
        settle(zone_in.at[it, h, pl.ds(0, rows - 1)], zone_recv.at[it, h])
        for p in range(half):
            value = zone_own[h, r, p]
            for k in range(1, rows):
                value = value + zone_in[it, h, lax.rem(r + k, rows), p].astype(F32)
            total_own[h, p] = value
            total_out[it, h, p] = value.astype(BF16)

        @pl.when(c != 0)
        def _():
            total_copy(it, h).start()

    def dense_part(it):
        near_band, far_band = near_bands[it], far_bands[it]
        near_window, far_window = near_windows[it], far_windows[it]
        if it == 0:
            if turns < slots:
                pltpu.make_async_copy(tab, order, tab_sem).wait()
                wait_panel()
            for i in range(len(stops) - 2):
                turn(i)
            prepare_volume()
        settle(shards(near_band, partner), near_recv.at[it, chip])

        @pl.when(c == 1)
        def _():
            send_window(it)

        def pass_on(peer):
            settle(shards(near_band, peer * CORES, CORES), near_recv.at[it, peer])
            band_pass(it, peer).start()

        @pl.when(chip != 0)
        def _():
            settle(shards(near_band, 0, CORES), near_recv.at[it, 0])
            send_window(it)
            band_pass(it, 0).start()

        if it == 0:
            turn(len(stops) - 2)
        for k in near_first:
            peer = peer_chip(k)

            @pl.when(peer != 0)
            def _():
                pass_on(peer)

        if it == 0 and turns == slots:
            pltpu.make_async_copy(tab, order, tab_sem).wait()
        segments(0, near_band, core)
        settle(shards(far_band, 0, cols - 1), far_recv.at[it])
        near_window[pl.ds(r * per_shard, per_shard)] = near_band[0:per_shard]
        far_window[pl.ds(r * per_shard, per_shard)] = far_band[0:per_shard]
        segments(0, far_band, other, 0)
        send_mix(it, 0)
        segments(0, far_band, other, 1)
        send_mix(it, 1)
        send_zone(it, 0)
        if it > 0:
            send_zone(it, 1)
        settle(shards(near_window, 0, rows - 1), win_recv.at[it])
        for k in range(1, rows):
            window_pass(it, lax.rem(r + k, rows)).start()
        segments(1, near_window, core)
        if it == 0:
            send_zone(it, 1)
        settle(shards(far_window, 0, rows - 1), win_far.at[it])
        segments(1, far_window, other, 0)
        send_pair(it, 0)
        segments(1, far_window, other, 1)
        send_pair(it, 1)
        groups = rhs // SUB
        gather_top(it)
        relax_groups(it, 0, groups // 4)
        send_rows(it, 0)
        relax_groups(it, groups // 4, groups // 2)
        send_rows(it, 1)
        for h in range(2):
            send_total(it, h)
        for h in range(0 if it == ITERS - 1 else 1, 2):
            for k in beyond:
                row_copy(it, h, k).start()
        relax_groups(it, groups // 2, groups)

    def drain(it):
        for side_of, near, far in (
            (0, jnp.logical_not(last_of_tile), cross_right),
            (1, jnp.logical_not(first_of_tile), cross_left),
        ):

            @pl.when(near)
            def _():
                settle_send(edge_left.at[it, 0], edge_send.at[it, side_of])

            @pl.when(far)
            def _():
                settle_send(edge_left.at[it, pl.ds(0, lines)], edge_send.at[it, side_of])

        if it == 0:
            for side_of in range(2):

                @pl.when(halo_sends[side_of])
                def _():
                    settle_send(halo_source, halo_send.at[side_of])

        @pl.when(jnp.logical_not(is_dense))
        def _():
            settle_send(shards(near_bands[it], 0, dense_chips * CORES), band_send.at[it])

        @pl.when(is_dense)
        def _():
            settle_send(shards(near_bands[it], 0, (dense_chips - 1) * CORES + 1), band_send.at[it])
            settle_send(shards(near_bands[it], 0, cols - 1), pass_send.at[it])
            settle_send(shards(near_bands[it], 0, 2 * (rows - 1)), win_send.at[it])
            settle_send(mix_out.at[it], mix_send.at[it])
            settle_send(zone_out.at[it, :, pl.ds(0, rows - 1)], zone_send.at[it])
            settle_send(pair_out.at[it], pair_send.at[it])
            settle_send(row_out.at[it, :, pl.ds(0, chips - 1)], row_send.at[it])

            @pl.when(c != 0)
            def _():
                settle_send(total_out.at[it], total_send.at[it])

    def own(h, p):
        return slice(p * tile + h * wide, p * tile + (h + 1) * wide)

    def round_half(it, h):
        for p in range(per_shard):
            rounded = traces_ref[:, own(h, p)].astype(BF16)

            @pl.when(core == h)
            def _():
                near_bands[it][c * per_shard + p] = rounded

            @pl.when(core != h)
            def _():
                far_bands[it][c * per_shard + p] = rounded

            at = LANES + p * tile + h * wide
            top[:, at : at + wide] = rounded.astype(F32)
            if h == 1 and p == per_shard - 1:
                edge_out[it, 0] = rounded[:, wide - LANES :]
            if h == 0 and p == 0:
                edge_out[it, 1] = rounded[:, :LANES]

    def send_half(it, h):
        side_of = 1 - h
        inner, outer = ((last_of_tile, cross_right), (first_of_tile, cross_left))[side_of]

        @pl.when(jnp.logical_not(inner))
        def _():
            edge_near(it, side_of).start()

        @pl.when(outer)
        def _():
            for z in range(lines):
                edge_far(it, side_of, z).start()

        for k in near_first:
            same, cross = band_copies(it, k)

            @pl.when((peer_chip(k) < dense_chips) & (core == h))
            def _():
                same.start()

            @pl.when((peer_chip(k) < dense_chips) & (core != h))
            def _():
                cross.start()

        to_near, to_far = partner_copies(it)

        @pl.when(is_dense & (core == h))
        def _():
            to_far.start()

        @pl.when(is_dense & (core != h))
        def _():
            to_near.start()

        if h == 0:

            @pl.when(c == 0)
            def _():
                send_window(it)

    def finish_half(it, h):
        @pl.when(is_dense)
        def _():
            for p in range(per_shard):
                product_ref[:, own(h, p)] = row_own[h, chip, p]
            settle(row_in.at[it, h, pl.ds(0, dense_chips - 1)], row_recv.at[it, h])

        @pl.when(jnp.logical_not(is_dense))
        def _():
            for p in range(per_shard):
                product_ref[:, own(h, p)] = jnp.zeros((rhs, wide), F32)
            settle(row_in.at[it, h, pl.ds(0, dense_chips)], row_recv.at[it, h])

        for src in range(dense_chips):

            @pl.when(src != chip)
            def _():
                for p in range(per_shard):
                    product_ref[:, own(h, p)] += row_in[it, h, src, p].astype(F32)

        @pl.when(c == 0)
        def _():
            settle(total_in.at[it, h, pl.ds(0, dense - 1)], total_recv.at[it, h])
            for p in range(half):
                product_ref[:, own(h, p)] += total_own[h, p]
            for src in range(1, dense):
                for p in range(half):
                    at = own(h, (src % CORES) * half + p)
                    product_ref[:, at] += total_in[it, h, src, p].astype(F32)

    for h in range(2):
        round_half(0, h)
    pl.semaphore_wait(barrier, expected)
    for h in range(2):
        send_half(0, h)
    begin()
    for it in range(ITERS):

        @pl.when(is_dense)
        def _():
            dense_part(it)

        @pl.when(jnp.logical_not(is_dense))
        def _():
            if it == 0:
                prepare_volume()
            gather_top(it)
            relax_groups(it, 0, rhs // SUB)

        if it == 0:
            input_copy(3).wait()
        middle_ref[...] = traces_ref[...] + COUPLING_STEP * (load_ref[...] - traces_ref[...])
        if it == ITERS - 1:
            output_copy(0).start()
            output_copy(2).start()
            for done in range(ITERS):
                drain(done)
        for h in range(2):
            finish_half(it, h)
            if it < ITERS - 1:
                for p in range(per_shard):
                    at = own(h, p)
                    change = COUPLING_STEP * (product_ref[:, at] + flux[:, at])
                    traces_ref[:, at] = middle_ref[:, at] - change
                round_half(it + 1, h)
                send_half(it + 1, h)

    output_copy(1).start()
    for i in range(len(outputs)):
        output_copy(i).wait()


def local(
    trace_start, surface_load, panel_tiles, tile_list, surf_map, coef_index, coef_table, vol_source
):
    cols = lax.axis_size("col")
    rows = lax.axis_size("row")
    lines, layers, nodes = coef_index.shape
    slots, tile, _ = panel_tiles.shape
    rhs, shard = trace_start.shape
    per_shard = shard // tile
    levels = coef_table.shape[0]
    half = per_shard // CORES
    chips = cols // CORES
    span = shard + 2 * LANES
    turns = min(slots, TURNED_BYTES // (2 * tile * tile) - slots)
    cfg = (cols, rows, lines, per_shard, tile, slots, nodes, layers, rhs, levels, turns)
    hbm = pl.BlockSpec(memory_space=pl.ANY)
    block = (rhs, tile)
    piece = (rhs, tile // 2)
    dma = pltpu.SemaphoreType.DMA
    out = jax.ShapeDtypeStruct((rhs, shard), F32)
    middle, product, flux = pl.pallas_call(
        functools.partial(kernel, cfg),
        out_shape=(out,) * 3,
        in_specs=[hbm] * 8,
        out_specs=(hbm,) * 3,
        scratch_shapes=[
            pltpu.VMEM((rhs, shard), F32),
            pltpu.VMEM((rhs, shard), F32),
            pltpu.VMEM((rhs, shard), F32),
            pltpu.SMEM(tile_list.shape, I32),
            pltpu.SMEM(surf_map.shape, I32),
            pltpu.SMEM(coef_table.shape, F32),
            pltpu.VMEM((slots, tile, tile), BF16),
            pltpu.VMEM((turns, tile, tile), BF16),
            pltpu.VMEM((rhs, shard), F32),
            pltpu.VMEM((rhs, shard), F32),
            pltpu.VMEM((lines, layers, nodes), I32),
            pltpu.VMEM((lines, layers, nodes), F32),
            pltpu.VMEM((SUB, LANES), I32),
            pltpu.SMEM((SUB, LANES), I32),
            pltpu.VMEM((cols * per_shard,) + piece, BF16),
            pltpu.VMEM((cols * per_shard,) + piece, BF16),
            pltpu.VMEM((cols * per_shard,) + piece, BF16),
            pltpu.VMEM((cols * per_shard,) + piece, BF16),
            pltpu.VMEM((rows * per_shard,) + piece, BF16),
            pltpu.VMEM((rows * per_shard,) + piece, BF16),
            pltpu.VMEM((rows * per_shard,) + piece, BF16),
            pltpu.VMEM((rows * per_shard,) + piece, BF16),
            pltpu.VMEM((ITERS, 2, rhs, LANES), BF16),
            pltpu.VMEM((ITERS, lines + 1, rhs, LANES), BF16),
            pltpu.VMEM((ITERS, lines + 1, rhs, LANES), BF16),
            pltpu.VMEM((2, lines, layers, LANES), I32),
            pltpu.VMEM((2, lines, layers, LANES), F32),
            pltpu.VMEM((slots + 1,) + block, F32),
            pltpu.VMEM((ITERS, 2, rows, half) + piece, BF16),
            pltpu.VMEM((ITERS, 2, rows, half) + piece, BF16),
            pltpu.VMEM((2, rows, half) + piece, F32),
            pltpu.VMEM((ITERS, 2, rows, half) + piece, BF16),
            pltpu.VMEM((ITERS, 2, rows, half) + piece, BF16),
            pltpu.VMEM((2, half) + piece, F32),
            pltpu.VMEM((ITERS, 2, half) + piece, BF16),
            pltpu.VMEM((ITERS, 2, cols, half) + piece, BF16),
            pltpu.VMEM((ITERS, 2, chips, per_shard) + piece, BF16),
            pltpu.VMEM((ITERS, 2, chips, per_shard) + piece, BF16),
            pltpu.VMEM((2, chips, per_shard) + piece, F32),
            pltpu.VMEM((ITERS, 2, chips, per_shard) + piece, BF16),
            pltpu.VMEM((ITERS, 2, chips, per_shard) + piece, BF16),
            pltpu.VMEM((layers, span), I32),
            pltpu.VMEM((layers, span), F32),
            pltpu.VMEM((layers, span), F32),
            pltpu.VMEM((5, layers, SUB, span), F32),
            pltpu.VMEM((2, layers, rhs, span), F32),
            pltpu.VMEM((rhs, span), F32),
            dma((3,)),
            dma((7,)),
            dma((3,)),
            dma,
            dma((ITERS,)),
            dma((ITERS,)),
            dma((ITERS, chips)),
            dma((ITERS,)),
            dma((ITERS,)),
            dma((ITERS,)),
            dma((ITERS,)),
            dma((ITERS, 2)),
            dma((ITERS, 2)),
            dma((2,)),
            dma((2,)),
            dma((ITERS,)),
            dma((ITERS, 2)),
            dma((ITERS,)),
            dma((ITERS, 2)),
            dma((ITERS,)),
            dma((ITERS, 2)),
            dma((ITERS,)),
            dma((ITERS, 2)),
            dma((ITERS,)),
            dma((ITERS, 2)),
        ],
        compiler_params=pltpu.CompilerParams(
            collective_id=0, has_side_effects=True, vmem_limit_bytes=60 * 1024 * 1024
        ),
        name="coupled",
    )(
        tile_list,
        surf_map,
        coef_table,
        trace_start,
        surface_load,
        coef_index,
        vol_source,
        panel_tiles,
    )
    response = product + flux
    return middle - COUPLING_STEP * response, response


def solution(mesh):
    return jax.shard_map(
        local,
        mesh=mesh,
        in_specs=(
            P(None, ("col", "row")),
            P(None, ("col", "row")),
            P(("col", "row"), None, None),
            P(("col", "row")),
            P(),
            P(None, None, "row"),
            P(),
            P(None, None, "row"),
        ),
        out_specs=(P(None, ("col", "row")), P(None, ("col", "row"))),
        check_vma=False,
    )
```

```python
import functools

import jax
import jax.numpy as jnp
from jax import lax
from jax.experimental import pallas as pl
from jax.experimental.pallas import tpu as pltpu
from jax.sharding import PartitionSpec as P

ITERS = 2
SWEEPS = 4

COUPLING_STEP = 0.3
JACOBI_WEIGHT = 0.8
CELL_MASS = 0.05

LANES = 128
SUB = 8
CORES = 2
TURNED_BYTES = 36 * 1024 * 1024
F32 = jnp.float32
BF16 = jnp.bfloat16
I32 = jnp.int32


def quotient(x, n):
    return x >> (n.bit_length() - 1) if n & (n - 1) == 0 else lax.div(x, n)


def remainder(x, n):
    return x & (n - 1) if n & (n - 1) == 0 else lax.rem(x, n)


def kernel(
    cfg,
    list_hbm,
    surf_hbm,
    table_hbm,
    start_hbm,
    load_hbm,
    index_hbm,
    source_hbm,
    panel_hbm,
    middle_hbm,
    product_hbm,
    flux_hbm,
    middle_ref,
    product_ref,
    flux,
    list_ref,
    surf_ref,
    table_ref,
    panel,
    turned,
    traces_ref,
    load_ref,
    index_ref,
    source_ref,
    tab,
    order,
    near_band0,
    near_band1,
    far_band0,
    far_band1,
    near_window0,
    near_window1,
    far_window0,
    far_window1,
    edge_out,
    edge_left,
    edge_right,
    halo_index,
    halo_source,
    product,
    mix_out,
    mix_in,
    zone_own,
    zone_out,
    zone_in,
    total_own,
    total_out,
    total_in,
    pair_out,
    pair_in,
    row_own,
    row_out,
    row_in,
    index_ext,
    coef_ext,
    source_ext,
    weights,
    state,
    top,
    panel_sem,
    input_sem,
    output_sem,
    tab_sem,
    band_send,
    pass_send,
    near_recv,
    far_recv,
    win_send,
    win_recv,
    win_far,
    edge_send,
    edge_recv,
    halo_send,
    halo_recv,
    sum_send,
    mix_recv,
    zone_send,
    zone_recv,
    total_recv,
    pair_recv,
    row_recv,
):
    cols, rows, lines, per_shard, tile, slots, nodes, layers, rhs, levels, turns = cfg
    dense = cols - lines
    group = cols // lines
    shard = per_shard * tile
    half = per_shard // CORES
    chips = cols // CORES
    dense_chips = dense // CORES
    win_tiles = rows * per_shard
    band_tiles = cols * per_shard
    side = cols * rows * per_shard
    span = shard + 2 * LANES
    wide = tile // 2
    near_bands = (near_band0, near_band1)
    far_bands = (far_band0, far_band1)
    near_windows = (near_window0, near_window1)
    far_windows = (far_window0, far_window1)
    c = lax.axis_index("col")
    r = lax.axis_index("row")
    core = lax.rem(c, CORES)
    chip = lax.div(c, CORES)
    other = 1 - core
    partner = chip * CORES + other
    q = lax.div(c, group)
    m = lax.rem(c, group)
    is_dense = c < dense
    row_up = jnp.minimum(r + 1, rows - 1)
    row_down = jnp.maximum(r - 1, 0)
    first_of_tile = m == 0
    last_of_tile = m == group - 1
    cross_left = first_of_tile & (r > 0)
    cross_right = last_of_tile & (r < rows - 1)

    def copy(src, dst, send, recv, to_col, to_row):
        return pltpu.make_async_remote_copy(
            src_ref=src,
            dst_ref=dst,
            send_sem=send,
            recv_sem=recv,
            device_id=(to_col, to_row),
            device_id_type=pl.DeviceIdType.MESH,
        )

    stops = sorted({0, slots * 3 // 8, slots * 3 // 4, slots})

    def panel_copy(i):
        part = pl.ds(stops[i], stops[i + 1] - stops[i])
        return pltpu.make_async_copy(panel_hbm.at[part], panel.at[part], panel_sem.at[i])

    inputs = (
        (start_hbm, traces_ref),
        (index_hbm, index_ref),
        (source_hbm, source_ref),
        (load_hbm, load_ref),
        (list_hbm, list_ref),
        (surf_hbm, surf_ref),
        (table_hbm, table_ref),
    )

    def input_copy(i):
        return pltpu.make_async_copy(inputs[i][0], inputs[i][1], input_sem.at[i])

    outputs = ((middle_ref, middle_hbm), (product_ref, product_hbm), (flux, flux_hbm))

    def output_copy(i):
        return pltpu.make_async_copy(outputs[i][0], outputs[i][1], output_sem)

    barrier = pltpu.get_barrier_semaphore()

    def greet(to_col, to_row):
        pl.semaphore_signal(
            barrier, inc=1, device_id=(to_col, to_row), device_id_type=pl.DeviceIdType.MESH
        )

    input_copy(0).start()
    for k in range(1, rows):
        greet(c, lax.rem(r + k, rows))
    for k in range(1, cols):
        greet(lax.rem(c + k, cols), r)

    @pl.when(cross_right)
    def _():
        for z in range(lines):
            greet(z * group, row_up)

    @pl.when(cross_left)
    def _():
        for z in range(lines):
            greet(z * group + group - 1, row_down)

    for i in (1, 2, 4, 5, 6, 3):
        input_copy(i).start()

    @pl.when(is_dense)
    def _():
        for i in range(len(stops) - 1):
            panel_copy(i).start()


    padded_slots = -(-slots // SUB) * SUB
    lane = lax.broadcasted_iota(I32, (SUB, LANES), 1)

    def sort_slots():
        slot = lax.broadcasted_iota(I32, (padded_slots, LANES), 0)
        lanes = lax.broadcasted_iota(I32, (padded_slots, LANES), 1)
        row_key = jnp.full((padded_slots, LANES), band_tiles, I32)
        col_key = jnp.full((padded_slots, LANES), win_tiles, I32)
        keys = []
        for s in range(slots):
            name = list_ref[s]
            safe = jnp.maximum(name, 0)
            row = quotient(safe, side)
            row = quotient(quotient(row, per_shard), rows) * per_shard + remainder(row, per_shard)
            row = jnp.where(name >= 0, row, band_tiles)
            col = jnp.where(name >= 0, remainder(safe, side), win_tiles)
            keys.append((col, row))
            row_key = jnp.where(slot == s, row, row_key)
            col_key = jnp.where(slot == s, col, col_key)

        def fold(x):
            x = functools.reduce(jnp.add, [x[i : i + SUB] for i in range(0, padded_slots, SUB)])
            for shift in (4, 2, 1):
                x = x + pltpu.roll(x, shift, 0)
            return x

        for which, key, source, count in (
            (0, col_key, row_key, win_tiles),
            (1, row_key, col_key, band_tiles),
        ):
            rank = jnp.zeros((padded_slots, LANES), I32)
            upto = jnp.zeros((SUB, LANES), I32)
            equal = jnp.zeros((SUB, LANES), I32)
            for s in range(slots):
                value = keys[s][which]
                ahead = (key > value) | ((key == value) & (slot > s))
                rank = rank + jnp.where(ahead, 1, 0)
                upto = upto + jnp.where(lane >= value, 1, 0)
                equal = equal + jnp.where(lane == value, 1, 0)
            rank = jnp.where(slot < slots, rank, LANES)
            here = rank == lanes
            place = fold(jnp.where(here, slot, 0))
            origin = fold(jnp.where(here, jnp.where(key < count, source, 0), 0))
            value = fold(jnp.where(here, key, 0))
            keep = (value == pltpu.roll(value, 1, 1)) & (lane > 0)
            last = jnp.where(equal > 0, upto - 1, slots)
            for i, x in enumerate((place, origin, jnp.where(keep, 1, 0), last)):
                tab[4 * which + i : 4 * which + i + 1, :] = x[0:1, :]

    input_copy(0).wait()
    expected = (
        cols - 1 + rows - 1 + jnp.where(cross_right, lines, 0) + jnp.where(cross_left, lines, 0)
    )

    def settle(ref, sem):
        copy(ref, ref, sem, sem, partner, r).wait_recv()

    def settle_send(ref, sem):
        copy(ref, ref, sem, sem, partner, r).wait_send()


    def halo_copy(kind, side_of, arrival=False):
        ref = (index_ref, source_ref)[kind]
        dst = (halo_index, halo_source)[kind]
        at = nodes - LANES if side_of == 0 else 0
        to = row_up if (side_of == 0) != arrival else row_down
        return copy(
            ref.at[:, :, pl.ds(at, LANES)],
            dst.at[side_of],
            halo_send.at[side_of],
            halo_recv.at[side_of],
            c,
            to,
        )

    halo_sends = (first_of_tile & (r < rows - 1), last_of_tile & (r > 0))
    halo_receives = (cross_left, cross_right)


    def edge_near(it, side_of):
        dst = (edge_left, edge_right)[side_of]
        return copy(
            edge_out.at[it, side_of],
            dst.at[it, lines],
            edge_send.at[it, side_of],
            edge_recv.at[it, side_of],
            c + 1 if side_of == 0 else c - 1,
            r,
        )

    def edge_far(it, side_of, z):
        dst = (edge_left, edge_right)[side_of]
        to = (z * group, row_up) if side_of == 0 else (z * group + group - 1, row_down)
        return copy(
            edge_out.at[it, side_of],
            dst.at[it, q],
            edge_send.at[it, side_of],
            edge_recv.at[it, side_of],
            *to,
        )


    def shards(ref, col, count=1):
        return ref.at[pl.ds(col * per_shard, count * per_shard)]

    bits = chips.bit_length() - 1
    power = chips == 1 << bits
    near_first = sorted(range(1, chips), key=lambda k: k.bit_count() if power else k)
    beside = [k for k in near_first if power and k.bit_count() == 1]
    beyond = [k for k in near_first if k not in beside]

    def peer_chip(k):
        if not power:
            return lax.rem(chip + k, chips)
        digits = [remainder(quotient(chip, 1 << b), 2) for b in range(bits)]
        return sum((1 - d if k >> b & 1 else d) * (1 << b) for b, d in enumerate(digits))

    def band_copies(it, k):
        peer = peer_chip(k) * CORES
        send, recv = band_send.at[it], near_recv.at[it, chip]
        near, far = shards(near_bands[it], c), shards(far_bands[it], c)
        return copy(near, near, send, recv, peer + core, r), copy(far, near, send, recv, peer + other, r)

    def partner_copies(it):
        near, far = shards(near_bands[it], c), shards(far_bands[it], c)
        return (
            copy(far, near, band_send.at[it], near_recv.at[it, chip], partner, r),
            copy(near, far, pass_send.at[it], far_recv.at[it], partner, r),
        )

    def band_pass(it, peer):
        at = peer * CORES
        return copy(
            shards(near_bands[it], at, CORES),
            shards(far_bands[it], at, CORES),
            pass_send.at[it],
            far_recv.at[it],
            partner,
            r,
        )

    def to_rows(send):
        for d in range(rows - 1, 0, -1):

            @pl.when(r + d < rows)
            def _():
                send(r + d)

            @pl.when(r >= d)
            def _():
                send(r - d)

    def window_copy(it, peer):
        return copy(
            shards(near_bands[it], 0),
            shards(near_windows[it], r),
            win_send.at[it],
            win_recv.at[it],
            c,
            peer,
        )

    def window_pass(it, at):
        return copy(
            shards(near_windows[it], at),
            shards(far_windows[it], at),
            win_send.at[it],
            win_far.at[it],
            partner,
            r,
        )

    def send_window(it):
        to_rows(lambda peer: window_copy(it, peer).start())


    def mix_copy(it, h):
        return copy(
            mix_out.at[it, h], mix_in.at[it, h], sum_send.at[it], mix_recv.at[it, h], partner, r
        )

    def zone_copy(it, h, peer):
        return copy(
            zone_out.at[it, h, peer],
            zone_in.at[it, h, r],
            zone_send.at[it],
            zone_recv.at[it, h],
            c,
            peer,
        )

    def total_copy(it, h):
        return copy(
            total_out.at[it, h],
            total_in.at[it, h, c],
            zone_send.at[it],
            total_recv.at[it, h],
            0,
            r,
        )


    def pair_copy(it, h):
        return copy(
            pair_out.at[it, h],
            pair_in.at[it, h],
            sum_send.at[it],
            pair_recv.at[it, h],
            partner,
            r,
        )

    def row_copy(it, h, k):
        peer = peer_chip(k)
        return copy(
            row_out.at[it, h, peer],
            row_in.at[it, h, chip],
            sum_send.at[it],
            row_recv.at[it, h],
            peer * CORES + core,
            r,
        )

    def prepare_volume():
        line = lax.div(surf_ref[r * lines + q], rows)
        for side_of, edge_of_tile in ((0, first_of_tile), (1, last_of_tile)):
            to = pl.ds(0 if side_of == 0 else LANES + shard, LANES)
            at = m * shard - LANES if side_of == 0 else m * shard + shard
            at = pl.multiple_of(jnp.clip(at, 0, nodes - LANES), LANES)
            receives = halo_receives[side_of]

            @pl.when(jnp.logical_not(edge_of_tile))
            def _():
                index_ext[:, to] = index_ref[line, :, pl.ds(at, LANES)]
                source_ext[:, to] = source_ref[line, :, pl.ds(at, LANES)]

            @pl.when(receives)
            def _():
                settle(halo_source, halo_recv.at[side_of])
                index_ext[:, to] = halo_index[side_of, line]
                source_ext[:, to] = halo_source[side_of, line]

            @pl.when(edge_of_tile & jnp.logical_not(receives))
            def _():
                index_ext[:, to] = jnp.full((layers, LANES), levels, I32)
                source_ext[:, to] = jnp.zeros((layers, LANES), F32)

        at = pl.multiple_of(m * shard, LANES)
        index_ext[:, LANES : LANES + shard] = index_ref[line, :, pl.ds(at, shard)]
        source_ext[:, LANES : LANES + shard] = source_ref[line, :, pl.ds(at, shard)]
        indices = index_ext[...]
        coefs = jnp.zeros((layers, span), F32)
        for level in range(levels):
            coefs = jnp.where(indices == level, table_ref[level], coefs)
        coef_ext[...] = coefs
        inside = index_ext[0:1, :] < levels
        for layer in range(layers):
            k = coef_ext[layer : layer + 1, :]
            left = 0.5 * (k + pltpu.roll(k, 1, 1))
            right = 0.5 * (k + pltpu.roll(k, span - 1, 1))
            up = 0.5 * (k + coef_ext[layer - 1 : layer, :]) if layer else k
            diagonal = left + right + up + CELL_MASS
            parts = [left, right, up]
            if layer < layers - 1:
                down = 0.5 * (k + coef_ext[layer + 1 : layer + 2, :])
                diagonal = diagonal + down
                parts.append(down)
            else:
                parts.append(None)
            parts.append(source_ext[layer : layer + 1, :])
            scale = jnp.where(inside, JACOBI_WEIGHT / diagonal, 0.0)
            for kind, part in enumerate(parts):
                if part is not None:
                    weights[kind, layer] = jnp.broadcast_to(part * scale, (SUB, span))

    def relax(now, g, first):
        at = pl.ds(g * SUB, SUB)
        for layer in range(layers):
            value = weights[4, layer]
            if first:
                if layer == 0:
                    value = value + weights[2, layer] * top[at, :]
            else:
                centre = state[now, layer, at, :]
                value = value + (1.0 - JACOBI_WEIGHT) * centre
                value = value + weights[0, layer] * pltpu.roll(centre, 1, 1)
                value = value + weights[1, layer] * pltpu.roll(centre, span - 1, 1)
                above = state[now, layer - 1, at, :] if layer else top[at, :]
                value = value + weights[2, layer] * above
                if layer < layers - 1:
                    value = value + weights[3, layer] * state[now, layer + 1, at, :]
            state[1 - now, layer, at, :] = value

    def gather_top(it):
        line = lax.div(surf_ref[r * lines + q], rows)
        for side_of, edge_of_tile in ((0, first_of_tile), (1, last_of_tile)):
            dst = (edge_left, edge_right)[side_of]
            to = slice(0, LANES) if side_of == 0 else slice(LANES + shard, span)
            base = row_down if side_of == 0 else row_up
            place = 0
            for z in range(lines):
                place = jnp.where(surf_ref[base * lines + z] == line * rows + base, z, place)
            receives = halo_receives[side_of]

            @pl.when(jnp.logical_not(edge_of_tile))
            def _():
                settle(dst.at[it, lines], edge_recv.at[it, side_of])
                top[:, to] = dst[it, lines].astype(F32)

            @pl.when(receives)
            def _():
                settle(dst.at[it, pl.ds(0, lines)], edge_recv.at[it, side_of])
                value = dst[it, 0]
                for z in range(1, lines):
                    value = jnp.where(place == z, dst[it, z], value)
                top[:, to] = value.astype(F32)

            @pl.when(edge_of_tile & jnp.logical_not(receives))
            def _():
                top[:, to] = jnp.zeros((rhs, LANES), F32)

    def relax_groups(it, begin, end):
        def rows_of(g, _):
            for i in range(SWEEPS):
                relax(i % 2, g, it == 0 and i == 0)
            at = pl.ds(g * SUB, SUB)
            k = jnp.broadcast_to(coef_ext[0:1, LANES : LANES + shard], (SUB, shard))
            flux[at, :] = k * (
                top[at, LANES : LANES + shard]
                - state[SWEEPS % 2, 0, at, LANES : LANES + shard]
            )
            return 0

        lax.fori_loop(begin, end, rows_of, 0)

    def lanes_of(h):
        return slice(h * wide, (h + 1) * wide)

    def segments(which, traces_of, part, h=None):
        at = slice(None) if h is None else lanes_of(h)
        part = pl.ds(pl.multiple_of(part * wide, wide), wide)
        acc = jnp.zeros((rhs, tile if h is None else wide), F32)
        for k in range(slots):
            s = order[4 * which, k]
            traces = traces_of[order[4 * which + 1, k]]
            keep = order[4 * which + 2, k].astype(F32)
            if which == 0:
                term = jnp.dot(traces, panel[s, part, at], preferred_element_type=F32)
            elif turns == slots or k < turns:
                block = turned[s if turns == slots else k, part, at]
                term = jnp.dot(traces, block, preferred_element_type=F32)
            else:
                block = panel[s, at, part]
                contract = (((1,), (1,)), ((), ()))
                term = lax.dot_general(traces, block, contract, preferred_element_type=F32)
            acc = acc * keep + term
            product[k, :, at] = acc if h is None else product[k, :, at] + acc

    def last_of(which, h, at):
        return product[order[4 * which + 3, at], :, lanes_of(h)]

    def send_mix(it, h):
        for z in range(rows):
            for p in range(half):
                value = last_of(0, h, z * per_shard + other * half + p)
                mix_out[it, h, z, p] = value.astype(BF16)
                zone_own[h, z, p] = last_of(0, h, z * per_shard + core * half + p)
        mix_copy(it, h).start()

    def send_zone(it, h):
        settle(mix_in.at[it, h], mix_recv.at[it, h])
        for z in range(rows):
            for p in range(half):
                value = zone_own[h, z, p] + mix_in[it, h, z, p].astype(F32)
                zone_own[h, z, p] = value
                zone_out[it, h, z, p] = value.astype(BF16)
        to_rows(lambda peer: zone_copy(it, h, peer).start())

    def send_pair(it, h):
        for k in range(chips):
            for p in range(per_shard):
                value = last_of(1, h, (k * CORES + other) * per_shard + p)
                pair_out[it, h, k, p] = value.astype(BF16)
                row_own[h, k, p] = last_of(1, h, (k * CORES + core) * per_shard + p)
        pair_copy(it, h).start()

    def send_rows(it, h):
        settle(pair_in.at[it, h], pair_recv.at[it, h])
        for k in range(chips):
            for p in range(per_shard):
                value = row_own[h, k, p] + pair_in[it, h, k, p].astype(F32)
                row_own[h, k, p] = value
                row_out[it, h, k, p] = value.astype(BF16)
        for k in near_first if h == 0 and it < ITERS - 1 else beside:
            row_copy(it, h, k).start()

    def wait_panel():
        for i in range(len(stops) - 1):
            panel_copy(i).wait()


    def turn(i):
        begin, end = min(stops[i], turns), min(stops[i + 1], turns)
        if turns == slots:
            panel_copy(i).wait()

        def one(k):
            turned[k] = panel[k if turns == slots else order[4, k]].T

        def two(j, _):
            one(begin + 2 * j)
            one(begin + 2 * j + 1)
            return 0

        lax.fori_loop(0, (end - begin) // 2, two, 0)
        if (end - begin) % 2:
            one(end - 1)

    def begin():
        input_copy(1).wait()
        input_copy(2).wait()
        for side_of in range(2):

            @pl.when(halo_sends[side_of])
            def _():
                for kind in range(2):
                    halo_copy(kind, side_of).start()

        input_copy(4).wait()
        input_copy(5).wait()
        input_copy(6).wait()

        @pl.when(is_dense)
        def _():
            sort_slots()
            pltpu.make_async_copy(tab, order, tab_sem).start()
            product[slots] = jnp.zeros((rhs, tile), F32)

    def send_total(it, h):
        settle(zone_in.at[it, h, pl.ds(0, rows - 1)], zone_recv.at[it, h])
        for p in range(half):
            value = zone_own[h, r, p]
            for k in range(1, rows):
                value = value + zone_in[it, h, lax.rem(r + k, rows), p].astype(F32)
            total_own[h, p] = value
            total_out[it, h, p] = value.astype(BF16)

        @pl.when(c != 0)
        def _():
            total_copy(it, h).start()

    def dense_part(it):
        near_band, far_band = near_bands[it], far_bands[it]
        near_window, far_window = near_windows[it], far_windows[it]
        if it == 0:
            if turns < slots:
                pltpu.make_async_copy(tab, order, tab_sem).wait()
                wait_panel()
            for i in range(len(stops) - 2):
                turn(i)
            prepare_volume()
        settle(shards(near_band, partner), near_recv.at[it, chip])

        @pl.when(c == 1)
        def _():
            send_window(it)

        def pass_on(peer):
            settle(shards(near_band, peer * CORES, CORES), near_recv.at[it, peer])
            band_pass(it, peer).start()

        @pl.when(chip != 0)
        def _():
            settle(shards(near_band, 0, CORES), near_recv.at[it, 0])
            send_window(it)
            band_pass(it, 0).start()

        if it == 0:
            turn(len(stops) - 2)
        for k in near_first:
            peer = peer_chip(k)

            @pl.when(peer != 0)
            def _():
                pass_on(peer)

        if it == 0 and turns == slots:
            pltpu.make_async_copy(tab, order, tab_sem).wait()
        segments(0, near_band, core)
        settle(shards(far_band, 0, cols - 1), far_recv.at[it])
        near_window[pl.ds(r * per_shard, per_shard)] = near_band[0:per_shard]
        far_window[pl.ds(r * per_shard, per_shard)] = far_band[0:per_shard]
        segments(0, far_band, other, 0)
        send_mix(it, 0)
        segments(0, far_band, other, 1)
        send_mix(it, 1)
        send_zone(it, 0)
        if it > 0:
            send_zone(it, 1)
        settle(shards(near_window, 0, rows - 1), win_recv.at[it])
        for k in range(1, rows):
            window_pass(it, lax.rem(r + k, rows)).start()
        segments(1, near_window, core)
        if it == 0:
            send_zone(it, 1)
        settle(shards(far_window, 0, rows - 1), win_far.at[it])
        segments(1, far_window, other, 0)
        send_pair(it, 0)
        segments(1, far_window, other, 1)
        send_pair(it, 1)
        groups = rhs // SUB
        gather_top(it)
        relax_groups(it, 0, groups // 4)
        send_rows(it, 0)
        relax_groups(it, groups // 4, groups // 2)
        send_rows(it, 1)
        for h in range(2):
            send_total(it, h)
        for h in range(0 if it == ITERS - 1 else 1, 2):
            for k in beyond:
                row_copy(it, h, k).start()
        relax_groups(it, groups // 2, groups)

    def drain(it):
        for side_of, near, far in (
            (0, jnp.logical_not(last_of_tile), cross_right),
            (1, jnp.logical_not(first_of_tile), cross_left),
        ):

            @pl.when(near)
            def _():
                settle_send(edge_left.at[it, 0], edge_send.at[it, side_of])

            @pl.when(far)
            def _():
                settle_send(edge_left.at[it, pl.ds(0, lines)], edge_send.at[it, side_of])

        if it == 0:
            for side_of in range(2):

                @pl.when(halo_sends[side_of])
                def _():
                    settle_send(halo_source, halo_send.at[side_of])

        @pl.when(jnp.logical_not(is_dense))
        def _():
            settle_send(shards(near_bands[it], 0, dense_chips * CORES), band_send.at[it])

        @pl.when(is_dense)
        def _():
            settle_send(shards(near_bands[it], 0, (dense_chips - 1) * CORES + 1), band_send.at[it])
            settle_send(shards(near_bands[it], 0, cols - 1), pass_send.at[it])
            settle_send(shards(near_bands[it], 0, 2 * (rows - 1)), win_send.at[it])
            pieces = 2 * (rows * half + (2 * chips - 1) * per_shard)
            settle_send(product.at[pl.ds(0, pieces // 4)], sum_send.at[it])

            @pl.when(c == 0)
            def _():
                settle_send(zone_out.at[it, :, pl.ds(0, rows - 1)], zone_send.at[it])

            @pl.when(c != 0)
            def _():
                settle_send(zone_out.at[it], zone_send.at[it])

    def own(h, p):
        return slice(p * tile + h * wide, p * tile + (h + 1) * wide)

    def round_half(it, h):
        for p in range(per_shard):
            rounded = traces_ref[:, own(h, p)].astype(BF16)

            @pl.when(core == h)
            def _():
                near_bands[it][c * per_shard + p] = rounded

            @pl.when(core != h)
            def _():
                far_bands[it][c * per_shard + p] = rounded

            at = LANES + p * tile + h * wide
            top[:, at : at + wide] = rounded.astype(F32)
            if h == 1 and p == per_shard - 1:
                edge_out[it, 0] = rounded[:, wide - LANES :]
            if h == 0 and p == 0:
                edge_out[it, 1] = rounded[:, :LANES]

    def send_half(it, h):
        side_of = 1 - h
        inner, outer = ((last_of_tile, cross_right), (first_of_tile, cross_left))[side_of]

        @pl.when(jnp.logical_not(inner))
        def _():
            edge_near(it, side_of).start()

        @pl.when(outer)
        def _():
            for z in range(lines):
                edge_far(it, side_of, z).start()

        for k in near_first:
            same, cross = band_copies(it, k)

            @pl.when((peer_chip(k) < dense_chips) & (core == h))
            def _():
                same.start()

            @pl.when((peer_chip(k) < dense_chips) & (core != h))
            def _():
                cross.start()

        to_near, to_far = partner_copies(it)

        @pl.when(is_dense & (core == h))
        def _():
            to_far.start()

        @pl.when(is_dense & (core != h))
        def _():
            to_near.start()

        if h == 0:

            @pl.when(c == 0)
            def _():
                send_window(it)

    def finish_half(it, h):
        @pl.when(is_dense)
        def _():
            for p in range(per_shard):
                product_ref[:, own(h, p)] = row_own[h, chip, p]
            settle(row_in.at[it, h, pl.ds(0, dense_chips - 1)], row_recv.at[it, h])

        @pl.when(jnp.logical_not(is_dense))
        def _():
            for p in range(per_shard):
                product_ref[:, own(h, p)] = jnp.zeros((rhs, wide), F32)
            settle(row_in.at[it, h, pl.ds(0, dense_chips)], row_recv.at[it, h])

        for src in range(dense_chips):

            @pl.when(src != chip)
            def _():
                for p in range(per_shard):
                    product_ref[:, own(h, p)] += row_in[it, h, src, p].astype(F32)

        @pl.when(c == 0)
        def _():
            settle(total_in.at[it, h, pl.ds(0, dense - 1)], total_recv.at[it, h])
            for p in range(half):
                product_ref[:, own(h, p)] += total_own[h, p]
            for src in range(1, dense):
                for p in range(half):
                    at = own(h, (src % CORES) * half + p)
                    product_ref[:, at] += total_in[it, h, src, p].astype(F32)

    for h in range(2):
        round_half(0, h)
    pl.semaphore_wait(barrier, expected)
    for h in range(2):
        send_half(0, h)
    begin()
    for it in range(ITERS):

        @pl.when(is_dense)
        def _():
            dense_part(it)

        @pl.when(jnp.logical_not(is_dense))
        def _():
            if it == 0:
                prepare_volume()
            gather_top(it)
            relax_groups(it, 0, rhs // SUB)

        if it == 0:
            input_copy(3).wait()
        middle_ref[...] = traces_ref[...] + COUPLING_STEP * (load_ref[...] - traces_ref[...])
        if it == ITERS - 1:
            output_copy(0).start()
            output_copy(2).start()
            for done in range(ITERS):
                drain(done)
        for h in range(2):
            finish_half(it, h)
            if it < ITERS - 1:
                for p in range(per_shard):
                    at = own(h, p)
                    change = COUPLING_STEP * (product_ref[:, at] + flux[:, at])
                    traces_ref[:, at] = middle_ref[:, at] - change
                round_half(it + 1, h)
                send_half(it + 1, h)

    output_copy(1).start()
    every = product.at[pl.ds(0, len(outputs) * per_shard)]
    pltpu.make_async_copy(every, every, output_sem).wait()


def local(
    trace_start, surface_load, panel_tiles, tile_list, surf_map, coef_index, coef_table, vol_source
):
    cols = lax.axis_size("col")
    rows = lax.axis_size("row")
    lines, layers, nodes = coef_index.shape
    slots, tile, _ = panel_tiles.shape
    rhs, shard = trace_start.shape
    per_shard = shard // tile
    levels = coef_table.shape[0]
    half = per_shard // CORES
    chips = cols // CORES
    span = shard + 2 * LANES
    assert (rows * half + (2 * chips - 1) * per_shard) % 2 == 0
    turns = min(slots, TURNED_BYTES // (2 * tile * tile) - slots)
    cfg = (cols, rows, lines, per_shard, tile, slots, nodes, layers, rhs, levels, turns)
    hbm = pl.BlockSpec(memory_space=pl.ANY)
    block = (rhs, tile)
    piece = (rhs, tile // 2)
    dma = pltpu.SemaphoreType.DMA
    out = jax.ShapeDtypeStruct((rhs, shard), F32)
    middle, product, flux = pl.pallas_call(
        functools.partial(kernel, cfg),
        out_shape=(out,) * 3,
        in_specs=[hbm] * 8,
        out_specs=(hbm,) * 3,
        scratch_shapes=[
            pltpu.VMEM((rhs, shard), F32),
            pltpu.VMEM((rhs, shard), F32),
            pltpu.VMEM((rhs, shard), F32),
            pltpu.SMEM(tile_list.shape, I32),
            pltpu.SMEM(surf_map.shape, I32),
            pltpu.SMEM(coef_table.shape, F32),
            pltpu.VMEM((slots, tile, tile), BF16),
            pltpu.VMEM((turns, tile, tile), BF16),
            pltpu.VMEM((rhs, shard), F32),
            pltpu.VMEM((rhs, shard), F32),
            pltpu.VMEM((lines, layers, nodes), I32),
            pltpu.VMEM((lines, layers, nodes), F32),
            pltpu.VMEM((SUB, LANES), I32),
            pltpu.SMEM((SUB, LANES), I32),
            pltpu.VMEM((cols * per_shard,) + piece, BF16),
            pltpu.VMEM((cols * per_shard,) + piece, BF16),
            pltpu.VMEM((cols * per_shard,) + piece, BF16),
            pltpu.VMEM((cols * per_shard,) + piece, BF16),
            pltpu.VMEM((rows * per_shard,) + piece, BF16),
            pltpu.VMEM((rows * per_shard,) + piece, BF16),
            pltpu.VMEM((rows * per_shard,) + piece, BF16),
            pltpu.VMEM((rows * per_shard,) + piece, BF16),
            pltpu.VMEM((ITERS, 2, rhs, LANES), BF16),
            pltpu.VMEM((ITERS, lines + 1, rhs, LANES), BF16),
            pltpu.VMEM((ITERS, lines + 1, rhs, LANES), BF16),
            pltpu.VMEM((2, lines, layers, LANES), I32),
            pltpu.VMEM((2, lines, layers, LANES), F32),
            pltpu.VMEM((slots + 1,) + block, F32),
            pltpu.VMEM((ITERS, 2, rows, half) + piece, BF16),
            pltpu.VMEM((ITERS, 2, rows, half) + piece, BF16),
            pltpu.VMEM((2, rows, half) + piece, F32),
            pltpu.VMEM((ITERS, 2, rows, half) + piece, BF16),
            pltpu.VMEM((ITERS, 2, rows, half) + piece, BF16),
            pltpu.VMEM((2, half) + piece, F32),
            pltpu.VMEM((ITERS, 2, half) + piece, BF16),
            pltpu.VMEM((ITERS, 2, cols, half) + piece, BF16),
            pltpu.VMEM((ITERS, 2, chips, per_shard) + piece, BF16),
            pltpu.VMEM((ITERS, 2, chips, per_shard) + piece, BF16),
            pltpu.VMEM((2, chips, per_shard) + piece, F32),
            pltpu.VMEM((ITERS, 2, chips, per_shard) + piece, BF16),
            pltpu.VMEM((ITERS, 2, chips, per_shard) + piece, BF16),
            pltpu.VMEM((layers, span), I32),
            pltpu.VMEM((layers, span), F32),
            pltpu.VMEM((layers, span), F32),
            pltpu.VMEM((5, layers, SUB, span), F32),
            pltpu.VMEM((2, layers, rhs, span), F32),
            pltpu.VMEM((rhs, span), F32),
            dma((3,)),
            dma((7,)),
            dma,
            dma,
            dma((ITERS,)),
            dma((ITERS,)),
            dma((ITERS, chips)),
            dma((ITERS,)),
            dma((ITERS,)),
            dma((ITERS,)),
            dma((ITERS,)),
            dma((ITERS, 2)),
            dma((ITERS, 2)),
            dma((2,)),
            dma((2,)),
            dma((ITERS,)),
            dma((ITERS, 2)),
            dma((ITERS,)),
            dma((ITERS, 2)),
            dma((ITERS, 2)),
            dma((ITERS, 2)),
            dma((ITERS, 2)),
        ],
        compiler_params=pltpu.CompilerParams(
            collective_id=0, has_side_effects=True, vmem_limit_bytes=60 * 1024 * 1024
        ),
        name="coupled",
    )(
        tile_list,
        surf_map,
        coef_table,
        trace_start,
        surface_load,
        coef_index,
        vol_source,
        panel_tiles,
    )
    response = product + flux
    return middle - COUPLING_STEP * response, response


def solution(mesh):
    return jax.shard_map(
        local,
        mesh=mesh,
        in_specs=(
            P(None, ("col", "row")),
            P(None, ("col", "row")),
            P(("col", "row"), None, None),
            P(("col", "row")),
            P(),
            P(None, None, "row"),
            P(),
            P(None, None, "row"),
        ),
        out_specs=(P(None, ("col", "row")), P(None, ("col", "row"))),
        check_vma=False,
    )
```
